128 devices in a mesh: blk: 16 (over x_hi, z, core), group: 8 (over x_lo, y).
Axes of the slice: x: 4 (x_hi: 2, x_lo: 2; x = x_hi * 2 + x_lo), y: 4, z: 4, core: 2. Of those that a mesh axis runs over, the one named last changes fastest.
Arguments:
- past_clicks_hidden: bfloat16 [4096, 24, 2048], P(('blk', 'group')), may hold values from -7.5 to 7.5
- candidate_hidden_state: bfloat16 [4096, 2048], P(('blk', 'group')), may hold values from -6 to 6
- customer_tower_projection: bfloat16 [2048, 768], replicated, may hold values from -0.125 to 0.125
- candidate_tower_projection: bfloat16 [2048, 768], replicated, may hold values from -0.125 to 0.125
- score_scaling_scalar: float32 [1], replicated, may hold values from 68 to 136
- score_shift_scalar: float32 [1], replicated, may hold values from -14 to -12
- upcoming_catalog_ident: int32 [4096], P(('blk', 'group')), may hold values from 0 to 1023
- correct_batch_slot: int32 [4096], P(('blk', 'group')), may hold values from 0 to 4095, each once
Outputs:
- mean_loss: float32 [1], replicated
- item_grad: float32 [4096, 768], P(('blk', 'group'))
- grad_user_weight: float32 [2048, 768], P(('blk', 'group'))
- grad_item_weight: float32 [2048, 768], P(('blk', 'group'))
The draws below stay inside these ranges and needn't reach their ends.
Inputs may be any that keep to these rules, and one draw needn't show every extreme that they name: `correct_batch_slot`: each row of the batch is the next item of exactly one user.
All inputs are finite; a program needn't handle non-finite values.
Results may differ from the reference program's by a relative error of at most 0.006.
Values may be sent and summed in bfloat16 or wider, within the bound.
A program may use at most 128 MiB of HBM per device.

```python
import math
import jax
import jax.numpy as jnp
import numpy as np
from jax import lax

D = 2048
E = 768
HIST = 24
TOTAL = 4096


def draw_past_clicks_hidden(key, part):
    folded = jax.random.fold_in(key, 17)
    shared_key, personal_key = jax.random.split(folded, 2)
    shared = 1.5 * jax.random.truncated_normal(shared_key, -3.0, 3.0, (TOTAL, 1, D), jnp.float32)
    personal = jax.random.truncated_normal(personal_key, -3.0, 3.0, (TOTAL, HIST, D), jnp.float32)
    return (shared + personal).astype(jnp.bfloat16)


def touch_ends(drawn, stream_key, low, largest):
    spot = [jax.random.randint(jax.random.fold_in(stream_key, axis), (), 0, length) for axis, length in enumerate(drawn.shape)]
    longest = drawn.shape.index(max(drawn.shape))
    next_to = spot[:longest] + [(spot[longest] + 1) % drawn.shape[longest]] + spot[longest + 1:]
    return drawn.at[tuple(spot)].set(low).at[tuple(next_to)].set(largest)


def shard_levels(key, extent, cuts, smallest, largest):
    factor_of = 1.0
    for axis_at, parts in cuts:
        heights = jax.random.uniform(jax.random.fold_in(jax.random.fold_in(key, 6), axis_at), (parts,), jnp.float32, smallest / len(cuts), largest / len(cuts))
        factor_of = factor_of * jnp.repeat(jnp.exp(heights), extent[axis_at] // parts).reshape((-1,) + (1,) * (len(extent) - 1 - axis_at))
    return factor_of


def rank_table(amount, slope):
    portions = [(1 << 20) // math.isqrt(standing ** slope) + 1 for standing in range(1, amount + 1)]
    deviation = 1 + sum(portions) // (1 << 30)
    return np.cumsum(np.array([max(1, weight // deviation) for weight in portions]))


def ranked(key, dims, count, skew):
    grid = rank_table(count, skew)
    ticket = jax.random.randint(jax.random.fold_in(key, 1), dims, 0, int(grid[count - 1]))
    grade = jnp.searchsorted(jnp.asarray(grid, jnp.int32), ticket, side="right")
    return jax.random.permutation(jax.random.fold_in(key, 2), count)[grade].astype(jnp.int32)


def scatter_about(rng, dims, width, limit, shards=(), kind=jnp.bfloat16):
    result = width * jax.random.normal(rng, dims, jnp.float32)
    if shards:
        result = result * shard_levels(rng, dims, shards, -0.22, 0.18)
    return jnp.clip(result, -limit, limit).astype(kind)


def setup_inputs(seed: int = 0) -> dict:
    streams_of = jax.random.split(jax.random.key(seed), 9)
    return {
        "past_clicks_hidden": draw_past_clicks_hidden(jax.random.fold_in(streams_of[8], 71), 0),
        "candidate_hidden_state": scatter_about(streams_of[1], (TOTAL, D), 1.0, 6.0, ((0, 128),)),
        "customer_tower_projection": scatter_about(streams_of[2], (D, E), D ** -0.5, 0.125),
        "candidate_tower_projection": scatter_about(streams_of[3], (D, E), D ** -0.5, 0.125),
        "score_scaling_scalar": jnp.clip(jax.random.uniform(streams_of[4], (1,), jnp.float32, 68.0, 136.0), 68.0, 136.0),
        "score_shift_scalar": jnp.clip(jax.random.uniform(streams_of[5], (1,), jnp.float32, -14.0, -12.0), -14.0, -12.0),
        "upcoming_catalog_ident": touch_ends(ranked(streams_of[6], (TOTAL,), TOTAL // 4, 2), jax.random.fold_in(streams_of[6], 3), 0, (TOTAL // 4) - 1).astype(jnp.int32),
        "correct_batch_slot": jax.random.permutation(streams_of[7], TOTAL).astype(jnp.int32),
    }


EPS = 1e-06

def user_tower(past_clicks_hidden, customer_tower_projection):
    batch_size, positions, feat_width = past_clicks_hidden.shape
    pre_act = jnp.dot(past_clicks_hidden.reshape(batch_size * positions, feat_width), customer_tower_projection, preferred_element_type=jnp.float32)
    pre_act = pre_act.reshape(batch_size, positions, -1)
    pooled = lax.optimization_barrier(jnp.mean(jax.nn.silu(pre_act), axis=1))
    length = jnp.sqrt(lax.optimization_barrier(jnp.sum(pooled * pooled, axis=1, keepdims=True)) + EPS)
    return (pre_act, length, pooled / length)

def item_tower(candidate_hidden_state, candidate_tower_projection):
    pre_act = jnp.dot(candidate_hidden_state, candidate_tower_projection, preferred_element_type=jnp.float32)
    length = jnp.sqrt(lax.optimization_barrier(jnp.sum(pre_act * pre_act, axis=1, keepdims=True)) + EPS)
    return (length, pre_act / length)

def sphere_back(normed, length, grad_normed):
    radial = lax.optimization_barrier(jnp.sum(normed * grad_normed, axis=1, keepdims=True))
    return (grad_normed - normed * radial) / length

def user_back(pre_act, length, normed, grad_normed):
    grad_pooled = sphere_back(normed, length, grad_normed) / pre_act.shape[1]
    sig_gate = jax.nn.sigmoid(pre_act)
    return (grad_pooled[:, None, :] * sig_gate * (1.0 + pre_act * (1.0 - sig_gate))).astype(jnp.bfloat16)

def pairwise_weight(user_embedding_rows, item_embedding_rows, per_user_target, item_label_matrix, smoothing_coefficient, column_offset):
    inner_product_matrix = lax.dot_general(user_embedding_rows, item_embedding_rows, (((1,), (1,)), ((), ())), preferred_element_type=jnp.float32)
    label_signs_matrix = jnp.where(per_user_target[:, None] == item_label_matrix[None, :], 1.0, -1.0).astype(jnp.float32)
    logit_offset_term = label_signs_matrix * (smoothing_coefficient * inner_product_matrix + column_offset)
    weight_matrix = (-smoothing_coefficient * label_signs_matrix * jax.nn.sigmoid(-logit_offset_term)).astype(jnp.bfloat16)
    return (weight_matrix, jnp.sum(jax.nn.softplus(-logit_offset_term)))

def transposed(first_op, second_op):
    return lax.dot_general(first_op, second_op, (((0,), (0,)), ((), ())), preferred_element_type=jnp.float32)

def reference(past_clicks_hidden, candidate_hidden_state, customer_tower_projection, candidate_tower_projection, score_scaling_scalar, score_shift_scalar, upcoming_catalog_ident, correct_batch_slot):
    smoothing_coefficient = score_scaling_scalar[0]
    column_offset = score_shift_scalar[0]
    pre_act, user_len, user_normed = user_tower(past_clicks_hidden, customer_tower_projection)
    user_embedding_rows = user_normed.astype(jnp.bfloat16)
    item_len, item_normed = item_tower(candidate_hidden_state, candidate_tower_projection)
    item_embedding_rows = item_normed.astype(jnp.bfloat16)
    target_matrix = jnp.take(upcoming_catalog_ident, correct_batch_slot)
    weight_matrix, loss_running_sum = pairwise_weight(user_embedding_rows, item_embedding_rows, target_matrix, upcoming_catalog_ident, smoothing_coefficient, column_offset)
    grad_users = jnp.dot(weight_matrix, item_embedding_rows, preferred_element_type=jnp.float32)
    item_grad = transposed(weight_matrix, user_embedding_rows)
    grad_pre_user = user_back(pre_act, user_len, user_normed, grad_users)
    grad_pre_item = sphere_back(item_normed, item_len, item_grad).astype(jnp.bfloat16)
    grad_user_weight = transposed(past_clicks_hidden.reshape(-1, D), grad_pre_user.reshape(-1, E))
    grad_item_weight = transposed(candidate_hidden_state, grad_pre_item)
    return ((loss_running_sum / TOTAL).reshape(1), item_grad, grad_user_weight, grad_item_weight)
```

```python
import functools

import jax
import jax.numpy as jnp
from jax import lax
from jax.experimental import pallas as pl
from jax.experimental.pallas import tpu as pltpu
from jax.sharding import PartitionSpec as P

EPS = 1e-06
MESH = pl.DeviceIdType.MESH
F32 = jnp.float32
BF16 = jnp.bfloat16
CORES = 2
COLOURS = 3


def dot(a, b):
    return jnp.dot(a, b, preferred_element_type=F32)


def dot_t(a, b):
    return lax.dot_general(a, b, (((0,), (0,)), ((), ())), preferred_element_type=F32)


def dot_nt(a, b):
    return lax.dot_general(a, b, (((1,), (1,)), ((), ())), preferred_element_type=F32)


def sigmoid(v):
    return 1.0 / (1.0 + jnp.exp(-v))


def tower_kernel(
    N, XL, TOTAL,
    x_hbm, ci_hbm, wu_hbm, wi_hbm, scale_ref, shift_ref, ids_ref, slot_ref,
    loss_ref, ig_ref, gu_ref, gi_ref,
    xv, xs, civ, cis, wuv, wiv, pre, pooled, gp, ulen, inorm, ilen,
    ua, ia, idbuf, slotbuf, tgtbuf, wt, pig, rig, pgu, rgu, g, gs, gi, gis,
    part, ra, sa, rb, sb, rc, losses, corelosses,
    lsem, xsem_s, xsem_r, id_s, id_r, slot_s, slot_r, tgt_s, tgt_r,
    ia_s, ia_r, ua_s, ua_r, ig_s, ig_r, ug_s, ug_r, g_s, g_r,
    rs_s, rs_r, lo_s, lo_r,
):
    USERS, E = pooled.shape
    HIST = xv.shape[0] // USERS
    FEAT = 128 if N == 4 else XL * N * 16
    QN = (N // XL) * N
    NU = N * CORES
    NI = N * N
    CW = 2 * E // COLOURS
    blk = lax.axis_index("blk")
    group = lax.axis_index("group")
    c = lax.rem(blk, CORES)
    z = lax.rem(blk // CORES, N)
    x = (blk // (CORES * N)) * XL + group // N
    y = lax.rem(group, N)

    def device(px, py, pz, pc):
        return (((px // XL) * N + pz) * CORES + pc, lax.rem(px, XL) * N + py)

    def plus(v, d, n):
        return v if d == 0 else lax.rem(v + d, n)

    def minus(v, d, n):
        return v if d == 0 else lax.rem(v + n - d, n)

    def send(src, dst, ssem, rsem, to):
        copy = pltpu.make_async_remote_copy(
            src_ref=src, dst_ref=dst, send_sem=ssem, recv_sem=rsem, device_id=to, device_id_type=MESH
        )
        copy.start()
        sent.append(copy)
        return copy

    sent = []
    sibling = device(x, y, z, 1 - c)
    user_peers = [(dy, dc) for dy in range(N) for dc in range(CORES) if (dy, dc) != (0, 0)]
    item_peers = [(dx, dz) for dx in range(N) for dz in range(N) if (dx, dz) != (0, 0)]

    def user_peer(dy, dc):
        return device(x, plus(y, dy, N), z, plus(c, dc, CORES))

    def user_slot(dy, dc):
        return plus(y, dy, N) * CORES + plus(c, dc, CORES)

    def item_peer(dx, dz):
        return device(plus(x, dx, N), y, plus(z, dz, N), c)

    load_ci = pltpu.make_async_copy(ci_hbm, civ, lsem.at[0])
    load_wi = pltpu.make_async_copy(wi_hbm, wiv, lsem.at[1])
    load_x = pltpu.make_async_copy(x_hbm, xv, lsem.at[2])
    load_wu = pltpu.make_async_copy(wu_hbm, wuv, lsem.at[3])
    for load in (load_ci, load_wi, load_x, load_wu):
        load.start()

    barrier = pltpu.get_barrier_semaphore()
    for d in user_peers:
        pl.semaphore_signal(barrier, inc=1, device_id=user_peer(*d), device_id_type=MESH)
    for d in item_peers:
        pl.semaphore_signal(barrier, inc=1, device_id=item_peer(*d), device_id_type=MESH)

    rows = lax.broadcasted_iota(jnp.int32, (USERS, USERS), 0)
    lanes = lax.broadcasted_iota(jnp.int32, (USERS, USERS), 1)
    id_col = jnp.sum(jnp.where(rows == lanes, ids_ref[...].astype(F32), 0.0), axis=1, keepdims=True)
    slot_col = jnp.sum(jnp.where(rows == lanes, slot_ref[...].astype(F32), 0.0), axis=1, keepdims=True)
    idbuf[0] = jnp.broadcast_to(id_col, (USERS, 128))
    my_user_slot = y * CORES + c
    wide_rows = lax.broadcasted_iota(jnp.int32, (USERS, NU * USERS), 0)
    wide_lanes = lax.broadcasted_iota(jnp.int32, (USERS, NU * USERS), 1)
    slot_row = jnp.sum(
        jnp.where(wide_lanes == wide_rows + my_user_slot * USERS, slot_col, 0.0), axis=0, keepdims=True
    )
    slotbuf[0] = jnp.broadcast_to(slot_row, (8, NU * USERS))

    pl.semaphore_wait(barrier, len(user_peers) + len(item_peers))

    id_recv, slot_recv = [], []
    for n, d in enumerate(user_peers):
        slot_recv.append(send(slotbuf.at[0], slotbuf.at[n + 1], slot_s.at[n], slot_r.at[n], user_peer(*d)))
    for n, (dx, dz) in enumerate(item_peers):
        s = dx * N + dz
        id_recv.append(send(idbuf.at[0], idbuf.at[s], id_s.at[n], id_r.at[n], item_peer(dx, dz)))

    load_ci.wait()
    load_wi.wait()
    item_pre = dot(civ[...], wiv[...])
    item_len = jnp.sqrt(jnp.sum(item_pre * item_pre, axis=1, keepdims=True) + EPS)
    item_normed = item_pre / item_len
    inorm[...] = item_normed
    ilen[...] = jnp.broadcast_to(item_len, (USERS, 128))
    ia[0] = item_normed.astype(BF16)
    ia_recv = []
    for n, (dx, dz) in enumerate(item_peers):
        s = dx * N + dz
        ia_recv.append(send(ia.at[0], ia.at[s], ia_s.at[n], ia_r.at[n], item_peer(dx, dz)))

    load_x.wait()
    x_recv = []
    for q in range(QN):
        cols = pl.ds(pl.multiple_of((q * CORES + 1 - c) * FEAT, FEAT), FEAT)
        x_recv.append(send(xv.at[:, cols], xs.at[q], xsem_s.at[q], xsem_r.at[q], sibling))
        x_recv.append(send(civ.at[:, cols], cis.at[q], xsem_s.at[QN + q], xsem_r.at[QN + q], sibling))
    load_wu.wait()

    def forward(n, _):
        cols = pl.ds(pl.multiple_of(n * 256, 256), 256)
        pre[:, cols] = dot(xv[...], wuv[:, cols])
        return 0

    lax.fori_loop(0, E // 256, forward, 0)

    def pool(n, _):
        u = n // (E // 128)
        j = lax.rem(n, E // 128)
        cols = pl.ds(pl.multiple_of(j * 128, 128), 128)
        v = pre[pl.ds(pl.multiple_of(u * 8 * HIST, 8 * HIST), 8 * HIST), cols]
        act = v * sigmoid(v)
        pooled[pl.ds(pl.multiple_of(u * 8, 8), 8), cols] = jnp.sum(act.reshape(8, HIST, 128), axis=1) / HIST
        return 0

    lax.fori_loop(0, (USERS // 8) * (E // 128), pool, 0)
    mean = pooled[...]
    user_len = jnp.sqrt(jnp.sum(mean * mean, axis=1, keepdims=True) + EPS)
    user_normed = mean / user_len
    ulen[...] = jnp.broadcast_to(user_len, (USERS, 128))
    pooled[...] = user_normed
    ua[my_user_slot] = user_normed.astype(BF16)
    ua_recv = []
    for n, d in enumerate(user_peers):
        ua_recv.append(send(ua.at[my_user_slot], ua.at[my_user_slot], ua_s.at[n], ua_r.at[n], user_peer(*d)))

    for copy in slot_recv + id_recv:
        copy.wait_recv()
    slots = slotbuf[0]
    for n in range(1, NU):
        slots = slots + slotbuf[n]
    slots = slots[0:1]
    found = jnp.zeros((1, NU * USERS), F32)
    item_rows = lax.broadcasted_iota(jnp.int32, (USERS, 128), 0)
    for dx in range(N):
        for dz in range(N):
            ox, oz = minus(x, dx, N), minus(z, dz, N)
            ob, og = device(ox, y, oz, c)
            at = (item_rows + (ob * (XL * N) + og) * USERS).astype(F32)
            ids = idbuf[dx * N + dz]
            wide = NU * USERS // 128
            hit = jnp.concatenate([at] * wide, axis=1) == slots
            found = found + jnp.sum(
                jnp.where(hit, jnp.concatenate([ids] * wide, axis=1), 0.0), axis=0, keepdims=True
            )
    tgtbuf[0] = jnp.broadcast_to(found, (8, NU * USERS))
    tgt_recv = []
    for n, d in enumerate(user_peers):
        tgt_recv.append(send(tgtbuf.at[0], tgtbuf.at[n + 1], tgt_s.at[n], tgt_r.at[n], user_peer(*d)))
    for copy in tgt_recv:
        copy.wait_recv()
    targets = tgtbuf[0]
    for n in range(1, NU):
        targets = targets + tgtbuf[n]
    targets = targets[0:1]

    for copy in ua_recv + ia_recv:
        copy.wait_recv()
    scale = scale_ref[0]
    shift = shift_ref[0]
    users = ua[...].reshape(NU * USERS, E)
    loss = jnp.zeros((8, 128), F32)
    ig_recv = []
    peer_at = {d: n for n, d in enumerate(item_peers)}
    for dx in range(N):
        items = ia[dx * N:(dx + 1) * N].reshape(N * USERS, E)
        scores = dot_nt(items, users)
        wide = NU * USERS // 128
        ids = idbuf[dx * N:(dx + 1) * N].reshape(N * USERS, 128)
        sign = jnp.where(jnp.concatenate([ids] * wide, axis=1) == targets, 1.0, -1.0)
        margin = sign * (scale * scores + shift)
        e = jnp.exp(-jnp.abs(margin))
        terms = jnp.log1p(e) + jnp.maximum(-margin, 0.0)
        gate = jnp.where(margin >= 0.0, e, 1.0) / (1.0 + e)
        weights = (-scale * sign * gate).astype(BF16)
        wt[dx * N * USERS:(dx + 1) * N * USERS, :] = weights
        terms = jnp.sum(terms.reshape(N * USERS // 8, 8, NU * USERS), axis=0)
        for j in range(wide):
            loss = loss + terms[:, j * 128:(j + 1) * 128]
        pig[dx * N:(dx + 1) * N] = dot(weights, users).astype(BF16).reshape(N, USERS, E)
        for dz in range(N):
            if (dx, dz) == (0, 0):
                continue
            n = peer_at[(dx, dz)]
            to = device(minus(x, dx, N), y, minus(z, dz, N), c)
            ig_recv.append(send(pig.at[dx * N + dz], rig.at[n], ig_s.at[n], ig_r.at[n], to))
    pgu[...] = dot_t(wt[...], ia[...].reshape(NI * USERS, E)).astype(BF16).reshape(NU, USERS, E)
    ug_recv = []
    for n, (dy, dc) in enumerate(user_peers):
        s = user_slot(dy, dc)
        ug_recv.append(send(pgu.at[s], rgu.at[n], ug_s.at[n], ug_r.at[n], user_peer(dy, dc)))

    def reduce_loss(value, step, pos):
        losses[step, pos] = value
        copies = []
        for d in range(1, N):
            at = [x, y, z]
            at[step] = plus(pos, d, N)
            copies.append(
                send(losses.at[step, pos], losses.at[step, pos], lo_s.at[step, d - 1], lo_r.at[step, d - 1],
                     device(at[0], at[1], at[2], c))
            )
        return copies

    def reduced_loss(step):
        total = losses[step, 0]
        for d in range(1, N):
            total = total + losses[step, d]
        return total

    loss_copies = reduce_loss(loss, 0, x)

    for copy in ig_recv:
        copy.wait_recv()
    item_grad = pig[0].astype(F32)
    for n in range(len(item_peers)):
        item_grad = item_grad + rig[n].astype(F32)
    ig_ref[...] = item_grad
    item_normed = inorm[...]
    radial = jnp.sum(item_normed * item_grad, axis=1, keepdims=True)
    gi[...] = ((item_grad - item_normed * radial) / ilen[:, 0:1]).astype(BF16)
    gi_copy = send(gi, gis, g_s.at[1], g_r.at[1], sibling)

    for copy in loss_copies:
        copy.wait_recv()
    loss_copies = reduce_loss(reduced_loss(0), 1, y)

    for copy in ug_recv:
        copy.wait_recv()
    grad_users = pgu[my_user_slot].astype(F32)
    for n in range(len(user_peers)):
        grad_users = grad_users + rgu[n].astype(F32)
    user_normed = pooled[...]
    radial = jnp.sum(user_normed * grad_users, axis=1, keepdims=True)
    gp[...] = (grad_users - user_normed * radial) / ulen[:, 0:1] / HIST

    def backward(n, _):
        u = n // (E // 128)
        j = lax.rem(n, E // 128)
        cols = pl.ds(pl.multiple_of(j * 128, 128), 128)
        at = pl.ds(pl.multiple_of(u * 8 * HIST, 8 * HIST), 8 * HIST)
        v = pre[at, cols]
        s = sigmoid(v)
        outer = jnp.broadcast_to(gp[pl.ds(pl.multiple_of(u * 8, 8), 8), cols][:, None, :], (8, HIST, 128))
        g[at, cols] = (outer.reshape(8 * HIST, 128) * s * (1.0 + v * (1.0 - s))).astype(BF16)
        return 0

    lax.fori_loop(0, (USERS // 8) * (E // 128), backward, 0)
    g_copy = send(g, gs, g_s.at[0], g_r.at[0], sibling)

    for copy in loss_copies:
        copy.wait_recv()
    loss_copies = reduce_loss(reduced_loss(1), 2, z)

    for copy in x_recv:
        copy.wait_recv()
    gi_copy.wait_recv()

    pos = (x, y, z)

    def put(k, q, r):
        r = r.astype(BF16)
        xh, qz = q // N, lax.rem(q, N)
        for xl in range(XL):
            for yy in range(N):
                at = (xh * XL + xl, yy, qz)
                i0, i1, i2 = at[k % 3], at[(k + 1) % 3], at[(k + 2) % 3]
                o = (xl * N + yy) * 16
                part[k, i0, i1, i2] = r[o:o + 16]

    def own_cols(q):
        return pl.ds(pl.multiple_of((q * CORES + c) * FEAT, FEAT), FEAT)

    def item_part(q, lo, hi):
        return dot_t(civ[:, own_cols(q)], gi[:, lo:hi]) + dot_t(cis[q], gis[:, lo:hi])

    def user_part(q, lo, hi):
        return dot_t(xv[:, own_cols(q)], g[:, lo:hi]) + dot_t(xs[q], gs[:, lo:hi])

    def colour2(q, _):
        put(2, q, item_part(q, 2 * CW - E, E))
        return 0

    def colour1(q, _):
        put(1, q, jnp.concatenate([user_part(q, CW, E), item_part(q, 0, 2 * CW - E)], axis=1))
        return 0

    def colour0(q, _):
        put(0, q, user_part(q, 0, CW))
        return 0

    def towards(axis, v):
        at = list(pos)
        at[axis] = v
        return device(at[0], at[1], at[2], c)

    def phase(k, ph, src, dst):
        axis = (k + ph) % 3
        copies = []
        for d in range(1, N):
            t = plus(pos[axis], d, N)
            copies.append(
                send(src.at[k, t], dst.at[k, d - 1], rs_s.at[k, ph, d - 1], rs_r.at[k, ph, d - 1], towards(axis, t))
            )
        return copies

    lax.fori_loop(0, QN, colour2, 0)
    flight = {2: phase(2, 0, part, ra)}
    for copy in loss_copies:
        copy.wait_recv()
    loss = reduced_loss(2)
    corelosses[c] = loss
    core_copy = send(corelosses.at[c], corelosses.at[c], lo_s.at[3, 0], lo_r.at[3, 0], sibling)
    g_copy.wait_recv()
    lax.fori_loop(0, QN, colour1, 0)
    flight[1] = phase(1, 0, part, ra)
    lax.fori_loop(0, QN, colour0, 0)
    flight[0] = phase(0, 0, part, ra)
    core_copy.wait_recv()
    loss_ref[0] = jnp.sum(corelosses[0] + corelosses[1]) / TOTAL

    order = (2, 1, 0)
    for k in order:
        for copy in flight[k]:
            copy.wait_recv()
        me = pos[k % 3]

        def add_a(n, _, k=k, me=me):
            i, j = n // N, lax.rem(n, N)
            total = part[k, me, i, j].astype(F32)
            for d in range(N - 1):
                total = total + ra[k, d, i, j].astype(F32)
            sa[k, i, j] = total.astype(BF16)
            return 0

        lax.fori_loop(0, N * N, add_a, 0)
        flight[k] = phase(k, 1, sa, rb)
    for k in order:
        for copy in flight[k]:
            copy.wait_recv()
        me = pos[(k + 1) % 3]
        for j in range(N):
            total = sa[k, me, j].astype(F32)
            for d in range(N - 1):
                total = total + rb[k, d, j].astype(F32)
            sb[k, j] = total.astype(BF16)
        flight[k] = phase(k, 2, sb, rc)
    for k in order:
        for copy in flight[k]:
            copy.wait_recv()
        me = pos[(k + 2) % 3]
        total = sb[k, me].astype(F32)
        for d in range(N - 1):
            total = total + rc[k, d].astype(F32)
        if k == 0:
            gu_ref[:, 0:CW] = total
        elif k == 1:
            gu_ref[:, CW:E] = total[:, 0:E - CW]
            gi_ref[:, 0:2 * CW - E] = total[:, E - CW:CW]
        else:
            gi_ref[:, 2 * CW - E:E] = total
    for copy in sent:
        copy.wait_send()


def shards(N, XL, past, cand, wu, wi, scale, shift, ids, slots):
    users, hist, depth = past.shape
    E = wu.shape[1]
    total = users * lax.axis_size("blk") * lax.axis_size("group")
    NU, NI, QN = N * CORES, N * N, (N // XL) * N
    feat = depth // (QN * CORES)
    hbm = pl.BlockSpec(memory_space=pl.ANY)
    smem = pl.BlockSpec(memory_space=pltpu.SMEM)
    vmem = pl.BlockSpec(memory_space=pltpu.VMEM)
    rows = depth // (NI * N * CORES)
    CW = 2 * E // COLOURS

    def dma(*shape):
        return pltpu.SemaphoreType.DMA(shape)

    V = pltpu.VMEM
    scratch = [
        V((users * hist, depth), BF16), V((QN, users * hist, feat), BF16),
        V((users, depth), BF16), V((QN, users, feat), BF16),
        V((depth, E), BF16), V((depth, E), BF16),
        V((users * hist, E), F32), V((users, E), F32), V((users, E), F32), V((users, 128), F32),
        V((users, E), F32), V((users, 128), F32),
        V((NU, users, E), BF16), V((NI, users, E), BF16), V((NI, users, 128), F32),
        V((NU, 8, NU * users), F32), V((NU, 8, NU * users), F32),
        V((NI * users, NU * users), BF16),
        V((NI, users, E), BF16), V((NI - 1, users, E), BF16),
        V((NU, users, E), BF16), V((NU - 1, users, E), BF16),
        V((users * hist, E), BF16), V((users * hist, E), BF16), V((users, E), BF16), V((users, E), BF16),
        V((COLOURS, N, N, N, rows, CW), BF16), V((COLOURS, N - 1, N, N, rows, CW), BF16),
        V((COLOURS, N, N, rows, CW), BF16), V((COLOURS, N - 1, N, rows, CW), BF16),
        V((COLOURS, N, rows, CW), BF16), V((COLOURS, N - 1, rows, CW), BF16),
        V((3, N, 8, 128), F32), V((CORES, 8, 128), F32),
        dma(4), dma(2 * QN), dma(2 * QN), dma(NI - 1), dma(NI - 1), dma(NU - 1), dma(NU - 1),
        dma(NU - 1), dma(NU - 1), dma(NI - 1), dma(NI - 1), dma(NU - 1), dma(NU - 1),
        dma(NI - 1), dma(NI - 1), dma(NU - 1), dma(NU - 1), dma(2), dma(2),
        dma(COLOURS, 3, N - 1), dma(COLOURS, 3, N - 1), dma(4, N - 1), dma(4, N - 1),
    ]
    return pl.pallas_call(
        functools.partial(tower_kernel, N, XL, total),
        name="two_tower",
        out_shape=(
            jax.ShapeDtypeStruct((1,), F32),
            jax.ShapeDtypeStruct((users, E), F32),
            jax.ShapeDtypeStruct((rows, E), F32),
            jax.ShapeDtypeStruct((rows, E), F32),
        ),
        in_specs=[hbm, hbm, hbm, hbm, smem, smem, vmem, vmem],
        out_specs=(smem, vmem, vmem, vmem),
        scratch_shapes=scratch,
        compiler_params=pltpu.CompilerParams(
            collective_id=0, has_side_effects=True, vmem_limit_bytes=60 * 1024 * 1024
        ),
    )(
        past.reshape(users * hist, depth), cand, wu, wi, scale, shift,
        ids.reshape(1, users), slots.reshape(1, users),
    )


def solution(mesh):
    group = mesh.shape["group"]
    n = {128: 4, 16: 2}[mesh.size]
    both = ("blk", "group")
    return jax.shard_map(
        functools.partial(shards, n, group // n),
        mesh=mesh,
        in_specs=(P(both, None, None), P(both, None), P(), P(), P(), P(), P(both), P(both)),
        out_specs=(P(), P(both, None), P(both, None), P(both, None)),
        check_vma=False,
    )
```

```python
import functools

import jax
import jax.numpy as jnp
from jax import lax
from jax.experimental import pallas as pl
from jax.experimental.pallas import tpu as pltpu
from jax.sharding import PartitionSpec as P

EPS = 1e-06
MESH = pl.DeviceIdType.MESH
F32 = jnp.float32
BF16 = jnp.bfloat16
CORES = 2
COLOURS = 3


def dot(a, b):
    return jnp.dot(a, b, preferred_element_type=F32)


def dot_t(a, b):
    return lax.dot_general(a, b, (((0,), (0,)), ((), ())), preferred_element_type=F32)


def dot_nt(a, b):
    return lax.dot_general(a, b, (((1,), (1,)), ((), ())), preferred_element_type=F32)


def sigmoid(v):
    return 1.0 / (1.0 + jnp.exp(-v))


def tower_kernel(
    N, XL, TOTAL,
    x_hbm, ci_hbm, wu_hbm, wi_hbm, scale_ref, shift_ref, ids_ref, slot_ref,
    loss_ref, ig_ref, gu_ref, gi_ref,
    xv, xs, civ, wuv, wiv, pre, pooled, gp, ulen, inorm, ilen,
    ua, ia, idbuf, slotbuf, tgtbuf, wt, pig, rig, pgu, rgu, g, gi, xi, xt,
    part, ra, sa, rb, sb, rc, parti, ri, losses, corelosses, scale_s, shift_s, idv, slotv,
    lsem, xsem_s, xsem_r, xi_s, xi_r, id_s, id_r, slot_s, slot_r, tgt_s, tgt_r,
    ia_s, ia_r, ua_s, ua_r, ig_s, ig_r, ug_s, ug_r, g_s, g_r, gi_s, gi_r,
    rs_s, rs_r, ri_s, ri_r, lo_s, lo_r,
):
    USERS, E = pooled.shape
    HIST = xv.shape[0] // USERS
    FEAT = 128 if N == 4 else XL * N * 16
    QN = (N // XL) * N
    NU = N * CORES
    NI = N * N
    CW = E // COLOURS
    XH = N // XL
    ROWS = USERS * HIST
    blk = lax.axis_index("blk")
    group = lax.axis_index("group")
    c = lax.rem(blk, CORES)
    z = lax.rem(blk // CORES, N)
    x = (blk // (CORES * N)) * XL + group // N
    y = lax.rem(group, N)

    def device(px, py, pz, pc):
        return (((px // XL) * N + pz) * CORES + pc, lax.rem(px, XL) * N + py)

    def plus(v, d, n):
        return v if d == 0 else lax.rem(v + d, n)

    def minus(v, d, n):
        return v if d == 0 else lax.rem(v + n - d, n)

    def send(src, dst, ssem, rsem, to):
        copy = pltpu.make_async_remote_copy(
            src_ref=src, dst_ref=dst, send_sem=ssem, recv_sem=rsem, device_id=to, device_id_type=MESH
        )
        copy.start()
        sent.append(copy)
        return copy

    sent = []
    sibling = device(x, y, z, 1 - c)
    user_peers = [(dy, dc) for dy in range(N) for dc in range(CORES) if (dy, dc) != (0, 0)]
    item_peers = [(dx, dz) for dx in range(N) for dz in range(N) if (dx, dz) != (0, 0)]
    feat_peers = [(dz, dc) for dz in range(N) for dc in range(CORES) if (dz, dc) != (0, 0)]
    row_peers = [(dx, dy) for dx in range(N) for dy in range(N) if (dx, dy) != (0, 0)]

    def user_peer(dy, dc):
        return device(x, plus(y, dy, N), z, plus(c, dc, CORES))

    def user_slot(dy, dc):
        return plus(y, dy, N) * CORES + plus(c, dc, CORES)

    def item_peer(dx, dz):
        return device(plus(x, dx, N), y, plus(z, dz, N), c)

    def feat_peer(dz, dc):
        return device(x, y, plus(z, dz, N), plus(c, dc, CORES))

    def row_peer(dx, dy):
        return device(plus(x, dx, N), plus(y, dy, N), z, c)

    small = [
        pltpu.make_async_copy(a, b, lsem.at[4 + n])
        for n, (a, b) in enumerate(((ids_ref, idv), (slot_ref, slotv), (scale_ref, scale_s), (shift_ref, shift_s)))
    ]
    for load in small:
        load.start()
    load_ci = pltpu.make_async_copy(ci_hbm, civ, lsem.at[0])
    load_wi = pltpu.make_async_copy(wi_hbm, wiv, lsem.at[1])
    load_x = pltpu.make_async_copy(x_hbm, xv, lsem.at[2])
    load_wu = pltpu.make_async_copy(wu_hbm, wuv, lsem.at[3])
    for load in (load_ci, load_wi, load_x, load_wu):
        load.start()

    barrier = pltpu.get_barrier_semaphore()
    for d in user_peers:
        pl.semaphore_signal(barrier, inc=1, device_id=user_peer(*d), device_id_type=MESH)
    for d in item_peers:
        pl.semaphore_signal(barrier, inc=1, device_id=item_peer(*d), device_id_type=MESH)
    far_feat = [d for d in feat_peers if d[0] and d[1]]
    far_row = [d for d in row_peers if d[0] and d[1]]
    for d in far_feat:
        pl.semaphore_signal(barrier, inc=1, device_id=feat_peer(*d), device_id_type=MESH)
    for d in far_row:
        pl.semaphore_signal(barrier, inc=1, device_id=row_peer(*d), device_id_type=MESH)
    for load in small:
        load.wait()

    rows = lax.broadcasted_iota(jnp.int32, (USERS, USERS), 0)
    lanes = lax.broadcasted_iota(jnp.int32, (USERS, USERS), 1)
    id_col = jnp.sum(jnp.where(rows == lanes, idv[...].astype(F32), 0.0), axis=1, keepdims=True)
    slot_col = jnp.sum(jnp.where(rows == lanes, slotv[...].astype(F32), 0.0), axis=1, keepdims=True)
    idbuf[0] = jnp.broadcast_to(id_col, (USERS, 128))
    my_user_slot = y * CORES + c
    wide_rows = lax.broadcasted_iota(jnp.int32, (USERS, NU * USERS), 0)
    wide_lanes = lax.broadcasted_iota(jnp.int32, (USERS, NU * USERS), 1)
    slot_row = jnp.sum(
        jnp.where(wide_lanes == wide_rows + my_user_slot * USERS, slot_col, 0.0), axis=0, keepdims=True
    )
    slotbuf[0] = jnp.broadcast_to(slot_row, (8, NU * USERS))

    pl.semaphore_wait(barrier, len(user_peers) + len(item_peers) + len(far_feat) + len(far_row))

    id_recv, slot_recv = [], []
    for n, d in enumerate(user_peers):
        slot_recv.append(send(slotbuf.at[0], slotbuf.at[n + 1], slot_s.at[n], slot_r.at[n], user_peer(*d)))
    for n, (dx, dz) in enumerate(item_peers):
        s = dx * N + dz
        id_recv.append(send(idbuf.at[0], idbuf.at[s], id_s.at[n], id_r.at[n], item_peer(dx, dz)))

    load_ci.wait()
    load_wi.wait()
    item_pre = dot(civ[...], wiv[...])
    item_len = jnp.sqrt(jnp.sum(item_pre * item_pre, axis=1, keepdims=True) + EPS)
    item_normed = item_pre / item_len
    inorm[...] = item_normed
    ilen[...] = jnp.broadcast_to(item_len, (USERS, 128))
    ia[0] = item_normed.astype(BF16)
    ia_recv = []
    for n, (dx, dz) in enumerate(item_peers):
        s = dx * N + dz
        ia_recv.append(send(ia.at[0], ia.at[s], ia_s.at[n], ia_r.at[n], item_peer(dx, dz)))

    load_x.wait()
    x_recv = []
    for q in range(QN):
        cols = pl.ds(pl.multiple_of((q * CORES + 1 - c) * FEAT, FEAT), FEAT)
        x_recv.append(send(xv.at[:, cols], xs.at[q], xsem_s.at[q], xsem_r.at[q], sibling))
    xi_recv = []
    for n, (dz, dc) in enumerate(feat_peers):
        pz, pc = plus(z, dz, N), plus(c, dc, CORES)
        for h in range(XH):
            cols = pl.ds(pl.multiple_of(((h * N + pz) * CORES + pc) * FEAT, FEAT), FEAT)
            xi_recv.append(
                send(civ.at[:, cols], xi.at[h, n + 1], xi_s.at[n, h], xi_r.at[n, h], feat_peer(dz, dc))
            )
    load_wu.wait()

    def forward(n, _):
        cols = pl.ds(pl.multiple_of(n * 256, 256), 256)
        pre[:, cols] = dot(xv[...], wuv[:, cols])
        return 0

    lax.fori_loop(0, E // 256, forward, 0)

    def pool(n, _):
        u = n // (E // 128)
        j = lax.rem(n, E // 128)
        cols = pl.ds(pl.multiple_of(j * 128, 128), 128)
        v = pre[pl.ds(pl.multiple_of(u * 8 * HIST, 8 * HIST), 8 * HIST), cols]
        act = v * sigmoid(v)
        pooled[pl.ds(pl.multiple_of(u * 8, 8), 8), cols] = jnp.sum(act.reshape(8, HIST, 128), axis=1) / HIST
        return 0

    lax.fori_loop(0, (USERS // 8) * (E // 128), pool, 0)
    mean = pooled[...]
    user_len = jnp.sqrt(jnp.sum(mean * mean, axis=1, keepdims=True) + EPS)
    user_normed = mean / user_len
    ulen[...] = jnp.broadcast_to(user_len, (USERS, 128))
    pooled[...] = user_normed
    ua[my_user_slot] = user_normed.astype(BF16)
    ua_recv = []
    for n, d in enumerate(user_peers):
        ua_recv.append(send(ua.at[my_user_slot], ua.at[my_user_slot], ua_s.at[n], ua_r.at[n], user_peer(*d)))

    for h in range(XH):
        xi[h, 0] = civ[:, pl.ds(pl.multiple_of(((h * N + z) * CORES + c) * FEAT, FEAT), FEAT)]
    for copy in x_recv:
        copy.wait_recv()

    def turn(q, _):
        cols = pl.ds(pl.multiple_of((q * CORES + c) * FEAT, FEAT), FEAT)
        to = pl.ds(pl.multiple_of(q * FEAT, FEAT), FEAT)
        xt[to, 0:ROWS] = xv[:, cols].T
        xt[to, ROWS:2 * ROWS] = xs[q].T
        return 0

    lax.fori_loop(0, QN, turn, 0)
    for copy in slot_recv + id_recv:
        copy.wait_recv()
    slots = slotbuf[0]
    for n in range(1, NU):
        slots = slots + slotbuf[n]
    slots = slots[0:1]
    found = jnp.zeros((1, NU * USERS), F32)
    item_rows = lax.broadcasted_iota(jnp.int32, (USERS, 128), 0)
    for dx in range(N):
        for dz in range(N):
            ox, oz = minus(x, dx, N), minus(z, dz, N)
            ob, og = device(ox, y, oz, c)
            at = (item_rows + (ob * (XL * N) + og) * USERS).astype(F32)
            ids = idbuf[dx * N + dz]
            wide = NU * USERS // 128
            hit = jnp.concatenate([at] * wide, axis=1) == slots
            found = found + jnp.sum(
                jnp.where(hit, jnp.concatenate([ids] * wide, axis=1), 0.0), axis=0, keepdims=True
            )
    tgtbuf[0] = jnp.broadcast_to(found, (8, NU * USERS))
    tgt_recv = []
    for n, d in enumerate(user_peers):
        tgt_recv.append(send(tgtbuf.at[0], tgtbuf.at[n + 1], tgt_s.at[n], tgt_r.at[n], user_peer(*d)))
    for copy in tgt_recv:
        copy.wait_recv()
    targets = tgtbuf[0]
    for n in range(1, NU):
        targets = targets + tgtbuf[n]
    targets = targets[0:1]

    for copy in ua_recv + ia_recv:
        copy.wait_recv()
    scale = scale_s[0]
    shift = shift_s[0]
    users = ua[...].reshape(NU * USERS, E)
    loss = jnp.zeros((8, 128), F32)
    wide = NU * USERS // 128
    for dx in range(N):
        items = ia[dx * N:(dx + 1) * N].reshape(N * USERS, E)
        scores = dot_nt(items, users)
        ids = idbuf[dx * N:(dx + 1) * N].reshape(N * USERS, 128)
        sign = jnp.where(jnp.concatenate([ids] * wide, axis=1) == targets, 1.0, -1.0)
        margin = sign * (scale * scores + shift)
        e = jnp.exp(-jnp.abs(margin))
        terms = jnp.log1p(e) + jnp.maximum(-margin, 0.0)
        gate = jnp.where(margin >= 0.0, e, 1.0) / (1.0 + e)
        wt[dx * N * USERS:(dx + 1) * N * USERS, :] = (-scale * sign * gate).astype(BF16)
        terms = jnp.sum(terms.reshape(N * USERS // 8, 8, NU * USERS), axis=0)
        for j in range(wide):
            loss = loss + terms[:, j * 128:(j + 1) * 128]
    pgu[...] = dot_t(wt[...], ia[...].reshape(NI * USERS, E)).astype(BF16).reshape(NU, USERS, E)
    ug_recv = []
    for n, (dy, dc) in enumerate(user_peers):
        s = user_slot(dy, dc)
        ug_recv.append(send(pgu.at[s], rgu.at[n], ug_s.at[n], ug_r.at[n], user_peer(dy, dc)))
    ig_recv = []
    peer_at = {d: n for n, d in enumerate(item_peers)}
    for dx in range(N):
        pig[dx * N:(dx + 1) * N] = (
            dot(wt[dx * N * USERS:(dx + 1) * N * USERS, :], users).astype(BF16).reshape(N, USERS, E)
        )
        for dz in range(N):
            if (dx, dz) == (0, 0):
                continue
            n = peer_at[(dx, dz)]
            to = device(minus(x, dx, N), y, minus(z, dz, N), c)
            ig_recv.append(send(pig.at[dx * N + dz], rig.at[n], ig_s.at[n], ig_r.at[n], to))

    def reduce_loss(value, step, pos):
        losses[step, pos] = value
        copies = []
        for d in range(1, N):
            at = [x, y, z]
            at[step] = plus(pos, d, N)
            copies.append(
                send(losses.at[step, pos], losses.at[step, pos], lo_s.at[step, d - 1], lo_r.at[step, d - 1],
                     device(at[0], at[1], at[2], c))
            )
        return copies

    def reduced_loss(step):
        total = losses[step, 0]
        for d in range(1, N):
            total = total + losses[step, d]
        return total

    loss_copies = reduce_loss(loss, 0, x)

    for copy in ug_recv:
        copy.wait_recv()
    grad_users = pgu[my_user_slot].astype(F32)
    for n in range(len(user_peers)):
        grad_users = grad_users + rgu[n].astype(F32)
    user_normed = pooled[...]
    radial = jnp.sum(user_normed * grad_users, axis=1, keepdims=True)
    gp[...] = (grad_users - user_normed * radial) / ulen[:, 0:1] / HIST

    pos = (x, y, z)

    def backward(k):
        def step(n, _):
            u = n // (CW // 128)
            j = lax.rem(n, CW // 128)
            cols = pl.ds(pl.multiple_of(k * CW + j * 128, 128), 128)
            at = pl.ds(pl.multiple_of(u * 8 * HIST, 8 * HIST), 8 * HIST)
            v = pre[at, cols]
            s = sigmoid(v)
            outer = jnp.broadcast_to(gp[pl.ds(pl.multiple_of(u * 8, 8), 8), cols][:, None, :], (8, HIST, 128))
            out = (outer.reshape(8 * HIST, 128) * s * (1.0 + v * (1.0 - s))).astype(BF16)
            g[k, at, pl.ds(pl.multiple_of(j * 128, 128), 128)] = out
            return 0

        lax.fori_loop(0, (USERS // 8) * (CW // 128), step, 0)
        return send(g.at[k, pl.ds(0, ROWS)], g.at[k, pl.ds(ROWS, ROWS)], g_s.at[k], g_r.at[k], sibling)

    def towards(axis, v):
        at = list(pos)
        at[axis] = v
        return device(at[0], at[1], at[2], c)

    def phase(k, ph, src, dst):
        axis = (k + ph) % 3
        copies = []
        for d in range(1, N):
            t = plus(pos[axis], d, N)
            copies.append(
                send(src.at[k, t], dst.at[k, d - 1], rs_s.at[k, ph, d - 1], rs_r.at[k, ph, d - 1], towards(axis, t))
            )
        return copies

    def weight_grad(k):
        r = dot(xt[...], g[k]).astype(BF16)
        for q in range(QN):
            for xl in range(XL):
                for yy in range(N):
                    at = ((q // N) * XL + xl, yy, q % N)
                    o = (q * XL * N + xl * N + yy) * 16
                    part[k, at[k % 3], at[(k + 1) % 3], at[(k + 2) % 3]] = r[o:o + 16]
        return phase(k, 0, part, ra)

    g_copies = [backward(0), backward(1)]
    g_copies[0].wait_recv()
    flight = {0: weight_grad(0)}
    g_copies.append(backward(2))
    g_copies[1].wait_recv()
    flight[1] = weight_grad(1)
    g_copies[2].wait_recv()
    flight[2] = weight_grad(2)

    for copy in ig_recv:
        copy.wait_recv()
    item_grad = pig[0].astype(F32)
    for n in range(len(item_peers)):
        item_grad = item_grad + rig[n].astype(F32)
    ig_ref[...] = item_grad
    item_normed = inorm[...]
    radial = jnp.sum(item_normed * item_grad, axis=1, keepdims=True)
    gi[0] = ((item_grad - item_normed * radial) / ilen[:, 0:1]).astype(BF16)
    gi_recv = []
    for n, d in enumerate(feat_peers):
        gi_recv.append(send(gi.at[0], gi.at[n + 1], gi_s.at[n], gi_r.at[n], feat_peer(*d)))

    for copy in loss_copies:
        copy.wait_recv()
    loss_copies = reduce_loss(reduced_loss(0), 1, y)

    def add_a(k):
        for copy in flight[k]:
            copy.wait_recv()
        me = pos[k % 3]

        def step(n, _):
            i, j = n // N, lax.rem(n, N)
            total = part[k, me, i, j].astype(F32)
            for d in range(N - 1):
                total = total + ra[k, d, i, j].astype(F32)
            sa[k, i, j] = total.astype(BF16)
            return 0

        lax.fori_loop(0, N * N, step, 0)
        flight[k] = phase(k, 1, sa, rb)

    def add_b(k):
        for copy in flight[k]:
            copy.wait_recv()
        me = pos[(k + 1) % 3]
        for j in range(N):
            total = sa[k, me, j].astype(F32)
            for d in range(N - 1):
                total = total + rb[k, d, j].astype(F32)
            sb[k, j] = total.astype(BF16)
        flight[k] = phase(k, 2, sb, rc)

    def add_c(k):
        for copy in flight[k]:
            copy.wait_recv()
        total = sb[k, pos[(k + 2) % 3]].astype(F32)
        for d in range(N - 1):
            total = total + rc[k, d].astype(F32)
        gu_ref[:, k * CW:(k + 1) * CW] = total

    add_a(0)
    for copy in loss_copies:
        copy.wait_recv()
    loss_copies = reduce_loss(reduced_loss(1), 2, z)
    add_a(1)

    for copy in xi_recv + gi_recv:
        copy.wait_recv()
    for h in range(XH):
        r = dot_t(
            xi[h].reshape(N * CORES * USERS, FEAT), gi[...].reshape(N * CORES * USERS, E)
        ).astype(BF16)
        for xl in range(XL):
            for yy in range(N):
                o = (xl * N + yy) * 16
                parti[h * XL + xl, yy] = r[o:o + 16]
    ri_recv = []
    for n, (dx, dy) in enumerate(row_peers):
        tx, ty = plus(x, dx, N), plus(y, dy, N)
        ri_recv.append(send(parti.at[tx, ty], ri.at[n], ri_s.at[n], ri_r.at[n], row_peer(dx, dy)))

    add_a(2)
    for copy in loss_copies:
        copy.wait_recv()
    corelosses[c] = reduced_loss(2)
    core_copy = send(corelosses.at[c], corelosses.at[c], lo_s.at[3, 0], lo_r.at[3, 0], sibling)
    add_b(0)
    add_b(1)
    add_b(2)
    core_copy.wait_recv()
    loss_ref[...] = jnp.broadcast_to(jnp.sum(corelosses[0] + corelosses[1], keepdims=True) / TOTAL, (8, 128))
    add_c(0)
    add_c(1)
    for copy in ri_recv:
        copy.wait_recv()
    total = parti[x, y].astype(F32)
    for n in range(len(row_peers)):
        total = total + ri[n].astype(F32)
    gi_ref[...] = total
    add_c(2)
    for copy in sent:
        copy.wait_send()


def hand_out(loss, ig, gu, gi, loss_out, ig_out, gu_out, gi_out):
    loss_out[0] = loss[0, 0]
    ig_out[...] = ig[...]
    gu_out[...] = gu[...]
    gi_out[...] = gi[...]


def shards(N, XL, past, cand, wu, wi, scale, shift, ids, slots):
    users, hist, depth = past.shape
    E = wu.shape[1]
    total = users * lax.axis_size("blk") * lax.axis_size("group")
    NU, NI, QN = N * CORES, N * N, (N // XL) * N
    feat = depth // (QN * CORES)
    hbm = pl.BlockSpec(memory_space=pl.ANY)
    smem = pl.BlockSpec(memory_space=pltpu.SMEM)
    vmem = pl.BlockSpec(memory_space=pltpu.VMEM)
    rows = depth // (NI * N * CORES)
    CW = E // COLOURS

    def dma(*shape):
        return pltpu.SemaphoreType.DMA(shape)

    V = pltpu.VMEM
    scratch = [
        V((users * hist, depth), BF16), V((QN, users * hist, feat), BF16),
        V((users, depth), BF16),
        V((depth, E), BF16), V((depth, E), BF16),
        V((users * hist, E), F32), V((users, E), F32), V((users, E), F32), V((users, 128), F32),
        V((users, E), F32), V((users, 128), F32),
        V((NU, users, E), BF16), V((NI, users, E), BF16), V((NI, users, 128), F32),
        V((NU, 8, NU * users), F32), V((NU, 8, NU * users), F32),
        V((NI * users, NU * users), BF16),
        V((NI, users, E), BF16), V((NI - 1, users, E), BF16),
        V((NU, users, E), BF16), V((NU - 1, users, E), BF16),
        V((COLOURS, 2 * users * hist, CW), BF16), V((NU, users, E), BF16),
        V((N // XL, NU, users, feat), BF16), V((QN * feat, 2 * users * hist), BF16),
        V((COLOURS, N, N, N, rows, CW), BF16), V((COLOURS, N - 1, N, N, rows, CW), BF16),
        V((COLOURS, N, N, rows, CW), BF16), V((COLOURS, N - 1, N, rows, CW), BF16),
        V((COLOURS, N, rows, CW), BF16), V((COLOURS, N - 1, rows, CW), BF16),
        V((N, N, rows, E), BF16), V((NI - 1, rows, E), BF16),
        V((3, N, 8, 128), F32), V((CORES, 8, 128), F32),
        pltpu.SMEM((1,), F32), pltpu.SMEM((1,), F32), V((1, users), jnp.int32), V((1, users), jnp.int32),
        dma(8), dma(QN), dma(QN), dma(NU - 1, N // XL), dma(NU - 1, N // XL),
        dma(NI - 1), dma(NI - 1), dma(NU - 1), dma(NU - 1),
        dma(NU - 1), dma(NU - 1), dma(NI - 1), dma(NI - 1), dma(NU - 1), dma(NU - 1),
        dma(NI - 1), dma(NI - 1), dma(NU - 1), dma(NU - 1), dma(COLOURS), dma(COLOURS), dma(NU - 1), dma(NU - 1),
        dma(COLOURS, 3, N - 1), dma(COLOURS, 3, N - 1), dma(NI - 1), dma(NI - 1), dma(4, N - 1), dma(4, N - 1),
    ]
    outs = pl.pallas_call(
        functools.partial(tower_kernel, N, XL, total),
        name="two_tower",
        out_shape=(
            jax.ShapeDtypeStruct((8, 128), F32),
            jax.ShapeDtypeStruct((users, E), F32),
            jax.ShapeDtypeStruct((rows, E), F32),
            jax.ShapeDtypeStruct((rows, E), F32),
        ),
        in_specs=[hbm] * 8,
        out_specs=(vmem,) * 4,
        scratch_shapes=scratch,
        compiler_params=pltpu.CompilerParams(
            collective_id=0, has_side_effects=True, vmem_limit_bytes=60 * 1024 * 1024
        ),
    )(
        past.reshape(users * hist, depth), cand, wu, wi, scale, shift,
        ids.reshape(1, users), slots.reshape(1, users),
    )
    return pl.pallas_call(
        hand_out,
        name="hand_out",
        out_shape=(
            jax.ShapeDtypeStruct((1,), F32),
            jax.ShapeDtypeStruct((users, E), F32),
            jax.ShapeDtypeStruct((rows, E), F32),
            jax.ShapeDtypeStruct((rows, E), F32),
        ),
        in_specs=[vmem] * 4,
        out_specs=(smem, vmem, vmem, vmem),
    )(*outs)


def solution(mesh):
    group = mesh.shape["group"]
    n = {128: 4, 16: 2}[mesh.size]
    both = ("blk", "group")
    return jax.shard_map(
        functools.partial(shards, n, group // n),
        mesh=mesh,
        in_specs=(P(both, None, None), P(both, None), P(), P(), P(), P(), P(both), P(both)),
        out_specs=(P(), P(both, None), P(both, None), P(both, None)),
        check_vma=False,
    )
```

```python
import functools

import jax
import jax.numpy as jnp
from jax import lax
from jax.experimental import pallas as pl
from jax.experimental.pallas import tpu as pltpu
from jax.sharding import PartitionSpec as P

EPS = 1e-06
MESH = pl.DeviceIdType.MESH
F32 = jnp.float32
BF16 = jnp.bfloat16
CORES = 2
COLOURS = 3


def dot(a, b):
    return jnp.dot(a, b, preferred_element_type=F32)


def dot_t(a, b):
    return lax.dot_general(a, b, (((0,), (0,)), ((), ())), preferred_element_type=F32)


def dot_nt(a, b):
    return lax.dot_general(a, b, (((1,), (1,)), ((), ())), preferred_element_type=F32)


def sigmoid(v):
    return 1.0 / (1.0 + jnp.exp(-v))


def tower_kernel(
    N, XL, TOTAL,
    x_hbm, ci_hbm, wu_hbm, wi_hbm, scale_ref, shift_ref, ids_ref, slot_ref,
    loss_ref, ig_ref, gu_ref, gi_ref,
    xv, xs, civ, wuv, wiv, pre, pooled, gp, ulen, inorm, ilen,
    ua, ia, idrow, idbuf, slotbuf, tgtbuf, wt, pig, pigf, rigc, rig, pgu, rgu, g, gi, xi, xt,
    part, ra, sa, rb, sb, rc, parti, ri, losses, corelosses, scale_s, shift_s, idv, slotv,
    lsem, xsem_s, xsem_r, xi_s, xi_r, id_s, id_r, slot_s, slot_r, tgt_s, tgt_r,
    ia_s, ia_r, ua_s, ua_r, ig_s, ig_r, ug_s, ug_r, g_s, g_r, gi_s, gi_r,
    ra_s, ra_r, rs_s, rs_r, ri_s, ri_r, lo_s, lo_r, hop_s, hop_r,
):
    USERS, E = pooled.shape
    HIST = xv.shape[0] // USERS
    FEAT = 128 if N == 4 else XL * N * 16
    QN = (N // XL) * N
    NU = XL * N
    NI = XL * N * CORES
    NS = XL * N
    CW = E // COLOURS
    XH = N // XL
    ROWS = USERS * HIST
    blk = lax.axis_index("blk")
    group = lax.axis_index("group")
    c = lax.rem(blk, CORES)
    z = lax.rem(blk // CORES, N)
    x = (blk // (CORES * N)) * XL + group // N
    y = lax.rem(group, N)
    odd = lax.rem(x, 2)
    pair_a = x + 1 - 2 * odd
    pair_b = lax.rem(x + N - 1 + 2 * odd, N)

    def device(px, py, pz, pc):
        return (((px // XL) * N + pz) * CORES + pc, lax.rem(px, XL) * N + py)

    def plus(v, d, n):
        return v if d == 0 else lax.rem(v + d, n)

    def minus(v, d, n):
        return v if d == 0 else lax.rem(v + n - d, n)

    def send(src, dst, ssem, rsem, to):
        copy = pltpu.make_async_remote_copy(
            src_ref=src, dst_ref=dst, send_sem=ssem, recv_sem=rsem, device_id=to, device_id_type=MESH
        )
        copy.start()
        sent.append(copy)
        return copy

    sent = []
    sibling = device(x, y, z, 1 - c)
    user_peers = [(da, dy) for da in range(2) for dy in range(N) if (da, dy) != (0, 0)]
    item_peers = [(db, dz, dc) for dc in range(CORES) for db in range(2) for dz in range(N) if (db, dz, dc) != (0, 0, 0)]
    near_items = [d for d in item_peers if d[2] == 0]
    feat_peers = [(dz, dc) for dc in range(CORES) for dz in range(N) if (dz, dc) != (0, 0)]
    row_peers = [(dx, dy) for dx in range(N) for dy in range(N) if (dx, dy) != (0, 0)]

    def user_peer(da, dy):
        return device(pair_a if da else x, plus(y, dy, N), z, c)

    def user_slot(da, dy):
        return (1 - odd if da else odd) * N + plus(y, dy, N)

    def item_slot(db, dz, dc):
        return dc * NS + db * N + dz

    def item_peer(db, dz, dc):
        return device(pair_b if db else x, y, plus(z, dz, N), plus(c, dc, CORES))

    def item_owner(db, dz, dc):
        return device(pair_b if db else x, y, minus(z, dz, N), plus(c, dc, CORES))

    def feat_peer(dz, dc):
        return device(x, y, plus(z, dz, N), plus(c, dc, CORES))

    def row_peer(dx, dy):
        return device(plus(x, dx, N), plus(y, dy, N), z, c)

    small = [
        pltpu.make_async_copy(a, b, lsem.at[4 + n])
        for n, (a, b) in enumerate(((ids_ref, idv), (slot_ref, slotv), (scale_ref, scale_s), (shift_ref, shift_s)))
    ]
    for load in small:
        load.start()
    load_ci = pltpu.make_async_copy(ci_hbm, civ, lsem.at[0])
    load_wi = pltpu.make_async_copy(wi_hbm, wiv, lsem.at[1])
    load_x = pltpu.make_async_copy(x_hbm, xv, lsem.at[2])
    load_wu = pltpu.make_async_copy(wu_hbm, wuv, lsem.at[3])
    for load in (load_ci, load_wi, load_x, load_wu):
        load.start()

    barrier = pltpu.get_barrier_semaphore()
    greeted = [row_peer(*d) for d in row_peers]
    greeted += [item_peer(*d) for d in item_peers if (d[1], d[2]) != (0, 0)]
    for to in greeted:
        pl.semaphore_signal(barrier, inc=1, device_id=to, device_id_type=MESH)
    for load in small:
        load.wait()
    my_user_slot = user_slot(0, 0)
    rows = lax.broadcasted_iota(jnp.int32, (USERS, USERS), 0)
    lanes = lax.broadcasted_iota(jnp.int32, (USERS, USERS), 1)
    id_col = jnp.sum(jnp.where(rows == lanes, idv[...].astype(F32), 0.0), axis=1, keepdims=True)
    slot_col = jnp.sum(jnp.where(rows == lanes, slotv[...].astype(F32), 0.0), axis=1, keepdims=True)
    tile_rows = lax.broadcasted_iota(jnp.int32, (USERS, 128), 0)
    tile_lanes = lax.broadcasted_iota(jnp.int32, (USERS, 128), 1)
    idrow[0] = jnp.sum(jnp.where(tile_rows == tile_lanes, id_col, 0.0), axis=0, keepdims=True)
    wide_rows = lax.broadcasted_iota(jnp.int32, (USERS, NU * USERS), 0)
    wide_lanes = lax.broadcasted_iota(jnp.int32, (USERS, NU * USERS), 1)
    slotbuf[0] = jnp.sum(
        jnp.where(wide_lanes == wide_rows + my_user_slot * USERS, slot_col, 0.0), axis=0, keepdims=True
    )
    load_ci.wait()
    load_wi.wait()
    item_pre = dot(civ[...], wiv[...])
    item_len = jnp.sqrt(jnp.sum(item_pre * item_pre, axis=1, keepdims=True) + EPS)
    item_normed = item_pre / item_len
    inorm[...] = item_normed
    ilen[...] = jnp.broadcast_to(item_len, (USERS, 128))
    ia[0, 0] = item_normed.astype(BF16)
    pl.semaphore_wait(barrier, len(greeted))
    id_recv, slot_recv = [], []
    for n, d in enumerate(user_peers):
        slot_recv.append(send(slotbuf.at[0], slotbuf.at[n + 1], slot_s.at[n], slot_r.at[n], user_peer(*d)))
    for n, d in enumerate(item_peers):
        id_recv.append(send(idrow.at[0], idrow.at[item_slot(*d)], id_s.at[n], id_r.at[n], item_peer(*d)))
    ia_recv = []
    for n, d in enumerate(near_items):
        ia_recv.append(send(ia.at[0, 0], ia.at[0, item_slot(*d)], ia_s.at[n], ia_r.at[n], item_peer(*d)))
    load_x.wait()
    x_recv = []
    for q in range(QN):
        cols = pl.ds(pl.multiple_of((q * CORES + 1 - c) * FEAT, FEAT), FEAT)
        x_recv.append(send(xv.at[:, cols], xs.at[q], xsem_s.at[q], xsem_r.at[q], sibling))
    load_wu.wait()

    def forward(n, _):
        cols = pl.ds(pl.multiple_of(n * 256, 256), 256)
        pre[:, cols] = dot(xv[...], wuv[:, cols])
        return 0

    lax.fori_loop(0, E // 256, forward, 0)

    for copy in slot_recv + id_recv:
        copy.wait_recv()
    slots = slotbuf[0]
    for n in range(1, NU):
        slots = slots + slotbuf[n]
    wide = NU * USERS // 128
    found = jnp.zeros((1, NU * USERS), F32)
    for dc in range(CORES):
        for db in range(2):
            for dz in range(N):
                s = item_slot(db, dz, dc)
                col = jnp.sum(jnp.where(tile_rows == tile_lanes, idrow[s], 0.0), axis=1, keepdims=True)
                ids = jnp.broadcast_to(col, (USERS, 128))
                idbuf[s] = ids
                ob, og = item_owner(db, dz, dc)
                at = (tile_rows + (ob * (XL * N) + og) * USERS).astype(F32)
                hit = jnp.concatenate([at] * wide, axis=1) == slots
                found = found + jnp.sum(
                    jnp.where(hit, jnp.concatenate([ids] * wide, axis=1), 0.0), axis=0, keepdims=True
                )
    tgtbuf[0] = found
    tgt_recv = []
    for n, d in enumerate(user_peers):
        tgt_recv.append(send(tgtbuf.at[0], tgtbuf.at[n + 1], tgt_s.at[n], tgt_r.at[n], user_peer(*d)))

    def pool(n, _):
        u = n // (E // 128)
        j = lax.rem(n, E // 128)
        cols = pl.ds(pl.multiple_of(j * 128, 128), 128)
        v = pre[pl.ds(pl.multiple_of(u * 8 * HIST, 8 * HIST), 8 * HIST), cols]
        act = v * sigmoid(v)
        pooled[pl.ds(pl.multiple_of(u * 8, 8), 8), cols] = jnp.sum(act.reshape(8, HIST, 128), axis=1) / HIST
        return 0

    lax.fori_loop(0, (USERS // 8) * (E // 128), pool, 0)
    mean = pooled[...]
    user_len = jnp.sqrt(jnp.sum(mean * mean, axis=1, keepdims=True) + EPS)
    user_normed = mean / user_len
    ulen[...] = jnp.broadcast_to(user_len, (USERS, 128))
    pooled[...] = user_normed
    ua[my_user_slot] = user_normed.astype(BF16)
    ua_recv = []
    for n, d in enumerate(user_peers):
        ua_recv.append(send(ua.at[my_user_slot], ua.at[my_user_slot], ua_s.at[n], ua_r.at[n], user_peer(*d)))

    xi_recv = []
    for n, (dz, dc) in enumerate(feat_peers):
        pz, pc = plus(z, dz, N), plus(c, dc, CORES)
        for h in range(XH):
            cols = pl.ds(pl.multiple_of(((h * N + pz) * CORES + pc) * FEAT, FEAT), FEAT)
            xi_recv.append(
                send(civ.at[:, cols], xi.at[h, dc * N + dz], xi_s.at[n, h], xi_r.at[n, h], feat_peer(dz, dc))
            )
    for h in range(XH):
        xi[h, 0] = civ[:, pl.ds(pl.multiple_of(((h * N + z) * CORES + c) * FEAT, FEAT), FEAT)]
    for copy in ia_recv:
        copy.wait_recv()
    ia_hop = send(ia.at[0], ia.at[1], hop_s.at[0], hop_r.at[0], sibling)
    for copy in x_recv:
        copy.wait_recv()

    def turn(q, _):
        cols = pl.ds(pl.multiple_of((q * CORES + c) * FEAT, FEAT), FEAT)
        to = pl.ds(pl.multiple_of(q * FEAT, FEAT), FEAT)
        xt[to, 0:ROWS] = xv[:, cols].T
        xt[to, ROWS:2 * ROWS] = xs[q].T
        return 0

    lax.fori_loop(0, QN, turn, 0)
    for copy in tgt_recv:
        copy.wait_recv()
    targets = tgtbuf[0]
    for n in range(1, NU):
        targets = targets + tgtbuf[n]

    for copy in ua_recv:
        copy.wait_recv()
    ia_hop.wait_recv()
    scale = scale_s[0]
    shift = shift_s[0]
    users = ua[...].reshape(NU * USERS, E)
    loss = jnp.zeros((8, 128), F32)
    for n in range(NI // N):
        items = ia[n // 2, (n % 2) * N:(n % 2 + 1) * N].reshape(N * USERS, E)
        scores = dot_nt(items, users)
        ids = idbuf[n * N:(n + 1) * N].reshape(N * USERS, 128)
        sign = jnp.where(jnp.concatenate([ids] * wide, axis=1) == targets, 1.0, -1.0)
        margin = sign * (scale * scores + shift)
        e = jnp.exp(-jnp.abs(margin))
        terms = jnp.log1p(e) + jnp.maximum(-margin, 0.0)
        gate = jnp.where(margin >= 0.0, e, 1.0) / (1.0 + e)
        wt[n * N * USERS:(n + 1) * N * USERS, :] = (-scale * sign * gate).astype(BF16)
        terms = jnp.sum(terms.reshape(N * USERS // 8, 8, NU * USERS), axis=0)
        for j in range(wide):
            loss = loss + terms[:, j * 128:(j + 1) * 128]
    def reduce_loss(value, step, pos):
        losses[step, pos] = value
        copies = []
        for d in range(1, N):
            at = [x, y, z]
            at[step] = plus(pos, d, N)
            copies.append(
                send(losses.at[step, pos], losses.at[step, pos], lo_s.at[step, d - 1], lo_r.at[step, d - 1],
                     device(at[0], at[1], at[2], c))
            )
        return copies

    def reduced_loss(step):
        total = losses[step, 0]
        for d in range(1, N):
            total = total + losses[step, d]
        return total

    loss_copies = reduce_loss(loss, 0, x)
    pgu[...] = dot_t(wt[...], ia[...].reshape(NI * USERS, E)).astype(BF16).reshape(NU, USERS, E)
    ug_recv = []
    for n, d in enumerate(user_peers):
        ug_recv.append(send(pgu.at[user_slot(*d)], rgu.at[n], ug_s.at[n], ug_r.at[n], user_peer(*d)))
    pig[1] = dot(wt[NS * USERS:2 * NS * USERS, :], users).astype(BF16).reshape(NS, USERS, E)
    ig_hop = send(pig.at[1], rigc, hop_s.at[1], hop_r.at[1], sibling)
    pigf[...] = dot(wt[0:NS * USERS, :], users).reshape(NS, USERS, E)
    ig_hop.wait_recv()
    ig_recv = []
    for s in range(NS):
        pigf[s] = pigf[s] + rigc[s].astype(F32)
        if s > 0:
            pig[0, s] = pigf[s].astype(BF16)
    for n, d in enumerate(near_items):
        ig_recv.append(send(pig.at[0, item_slot(*d)], rig.at[n], ig_s.at[n], ig_r.at[n], item_owner(*d)))

    for copy in ug_recv:
        copy.wait_recv()
    grad_users = pgu[my_user_slot].astype(F32)
    for n in range(len(user_peers)):
        grad_users = grad_users + rgu[n].astype(F32)
    user_normed = pooled[...]
    radial = jnp.sum(user_normed * grad_users, axis=1, keepdims=True)
    gp[...] = (grad_users - user_normed * radial) / ulen[:, 0:1] / HIST

    pos = (x, y, z)

    def backward(k):
        def step(n, _):
            u = n // (CW // 128)
            j = lax.rem(n, CW // 128)
            cols = pl.ds(pl.multiple_of(k * CW + j * 128, 128), 128)
            at = pl.ds(pl.multiple_of(u * 8 * HIST, 8 * HIST), 8 * HIST)
            v = pre[at, cols]
            s = sigmoid(v)
            outer = jnp.broadcast_to(gp[pl.ds(pl.multiple_of(u * 8, 8), 8), cols][:, None, :], (8, HIST, 128))
            out = (outer.reshape(8 * HIST, 128) * s * (1.0 + v * (1.0 - s))).astype(BF16)
            g[k, at, pl.ds(pl.multiple_of(j * 128, 128), 128)] = out
            return 0

        lax.fori_loop(0, (USERS // 8) * (CW // 128), step, 0)
        return send(g.at[k, pl.ds(0, ROWS)], g.at[k, pl.ds(ROWS, ROWS)], g_s.at[k], g_r.at[k], sibling)

    def towards(axis, v):
        at = list(pos)
        at[axis] = v
        return device(at[0], at[1], at[2], c)

    def phase(k, ph, src, dst):
        axis = (k + ph) % 3
        copies = []
        for d in range(1, N):
            t = plus(pos[axis], d, N)
            at = (k, ph - 1, d - 1)
            copies.append(send(src.at[k, t], dst.at[k, d - 1], rs_s.at[at], rs_r.at[at], towards(axis, t)))
        return copies

    def weight_grad(half, k):
        xh = x // XL if half else XH - 1 - x // XL
        depth = QN // XH * FEAT
        r = dot(xt[pl.ds(pl.multiple_of(xh * depth, depth), depth)], g[k]).astype(BF16)
        for qz in range(N):
            for xl in range(XL):
                for yy in range(N):
                    at = (xh * XL + xl, yy, qz)
                    o = ((qz * XL + xl) * N + yy) * 16
                    part[k, at[k % 3], at[(k + 1) % 3], at[(k + 2) % 3]] = r[o:o + 16]
        xs_here = pl.ds(xh * XL, XL)
        if k == 0:
            for t in ([pair_a] if half else [xh * XL + xl for xl in range(XL)]):
                d = lax.rem(t - x + N, N) - 1
                send(part.at[0, t], ra.at[0, d], ra_s.at[0, d, 0], ra_r.at[0, d, 0], towards(0, t))
            return
        for d in range(1, N):
            t = plus(pos[k], d, N)
            if k == 1:
                src, dst = part.at[1, t, :, xs_here], ra.at[1, d - 1, :, xs_here]
            else:
                src, dst = part.at[2, t, xs_here], ra.at[2, d - 1, xs_here]
            send(src, dst, ra_s.at[k, d - 1, half], ra_r.at[k, d - 1, half], towards(k, t))

    def wait_slabs(k):
        for d in range(N - 1):
            if k == 0:
                slabs = [ra.at[0, d]]
            elif k == 1:
                slabs = [ra.at[1, d, :, pl.ds(h * XL, XL)] for h in range(XH)]
            else:
                slabs = [ra.at[2, d, pl.ds(h * XL, XL)] for h in range(XH)]
            for h, slab in enumerate(slabs):
                pltpu.make_async_remote_copy(
                    src_ref=slab, dst_ref=slab, send_sem=ra_s.at[k, d, h], recv_sem=ra_r.at[k, d, h],
                    device_id=sibling, device_id_type=MESH,
                ).wait_recv()

    g_copies = [backward(0), backward(1)]
    for copy in loss_copies:
        copy.wait_recv()
    loss_copies = reduce_loss(reduced_loss(0), 1, y)
    g_copies[0].wait_recv()
    weight_grad(0, 0)
    g_copies.append(backward(2))
    g_copies[1].wait_recv()
    weight_grad(0, 1)
    g_copies[2].wait_recv()
    weight_grad(0, 2)

    for copy in ig_recv:
        copy.wait_recv()
    item_grad = pigf[0]
    for n in range(len(near_items)):
        item_grad = item_grad + rig[n].astype(F32)
    ig_ref[...] = item_grad
    item_normed = inorm[...]
    radial = jnp.sum(item_normed * item_grad, axis=1, keepdims=True)
    gi[0, 0] = ((item_grad - item_normed * radial) / ilen[:, 0:1]).astype(BF16)
    gi_recv = []
    for d in range(1, N):
        to = device(x, y, plus(z, d, N), c)
        gi_recv.append(send(gi.at[0, 0], gi.at[0, d], gi_s.at[d - 1], gi_r.at[d - 1], to))
    for k in range(COLOURS):
        weight_grad(1, k)
    for copy in loss_copies:
        copy.wait_recv()
    loss_copies = reduce_loss(reduced_loss(1), 2, z)
    for copy in gi_recv:
        copy.wait_recv()
    gi_hop = send(gi.at[0], gi.at[1], hop_s.at[2], hop_r.at[2], sibling)

    flight = {}

    def add_a(k):
        wait_slabs(k)
        me = pos[k % 3]

        def step(n, _):
            i, j = n // N, lax.rem(n, N)
            total = part[k, me, i, j].astype(F32)
            for d in range(N - 1):
                total = total + ra[k, d, i, j].astype(F32)
            sa[k, i, j] = total.astype(BF16)
            return 0

        lax.fori_loop(0, N * N, step, 0)
        flight[k] = phase(k, 1, sa, rb)

    def add_b(k):
        for copy in flight[k]:
            copy.wait_recv()
        me = pos[(k + 1) % 3]
        for j in range(N):
            total = sa[k, me, j].astype(F32)
            for d in range(N - 1):
                total = total + rb[k, d, j].astype(F32)
            sb[k, j] = total.astype(BF16)
        flight[k] = phase(k, 2, sb, rc)

    def add_c(k):
        for copy in flight[k]:
            copy.wait_recv()
        total = sb[k, pos[(k + 2) % 3]].astype(F32)
        for d in range(N - 1):
            total = total + rc[k, d].astype(F32)
        gu_ref[:, k * CW:(k + 1) * CW] = total

    add_a(0)
    add_a(1)
    add_a(2)
    for copy in loss_copies:
        copy.wait_recv()
    corelosses[c] = reduced_loss(2)
    core_copy = send(corelosses.at[c], corelosses.at[c], hop_s.at[3], hop_r.at[3], sibling)
    for copy in xi_recv:
        copy.wait_recv()
    gi_hop.wait_recv()
    for h in range(XH):
        r = dot_t(
            xi[h].reshape(N * CORES * USERS, FEAT), gi[...].reshape(N * CORES * USERS, E)
        ).astype(BF16)
        for xl in range(XL):
            for yy in range(N):
                o = (xl * N + yy) * 16
                parti[h * XL + xl, yy] = r[o:o + 16]
    ri_recv = []
    for n, (dx, dy) in enumerate(row_peers):
        tx, ty = plus(x, dx, N), plus(y, dy, N)
        ri_recv.append(send(parti.at[tx, ty], ri.at[n], ri_s.at[n], ri_r.at[n], row_peer(dx, dy)))
    add_b(0)
    add_b(1)
    add_b(2)
    core_copy.wait_recv()
    loss_ref[...] = jnp.broadcast_to(jnp.sum(corelosses[0] + corelosses[1], keepdims=True) / TOTAL, (8, 128))
    add_c(0)
    add_c(1)
    for copy in ri_recv:
        copy.wait_recv()
    total = parti[x, y].astype(F32)
    for n in range(len(row_peers)):
        total = total + ri[n].astype(F32)
    gi_ref[...] = total
    add_c(2)
    for copy in sent:
        copy.wait_send()


def hand_out(loss, ig, gu, gi, loss_out, ig_out, gu_out, gi_out):
    loss_out[0] = loss[0, 0]
    ig_out[...] = ig[...]
    gu_out[...] = gu[...]
    gi_out[...] = gi[...]


def shards(N, XL, past, cand, wu, wi, scale, shift, ids, slots):
    users, hist, depth = past.shape
    E = wu.shape[1]
    total = users * lax.axis_size("blk") * lax.axis_size("group")
    NU, NI, NS, QN = XL * N, XL * N * CORES, XL * N, (N // XL) * N
    feat = depth // (QN * CORES)
    hbm = pl.BlockSpec(memory_space=pl.ANY)
    smem = pl.BlockSpec(memory_space=pltpu.SMEM)
    vmem = pl.BlockSpec(memory_space=pltpu.VMEM)
    rows = depth // (N * N * N * CORES)
    CW = E // COLOURS

    def dma(*shape):
        return pltpu.SemaphoreType.DMA(shape)

    V = pltpu.VMEM
    scratch = [
        V((users * hist, depth), BF16), V((QN, users * hist, feat), BF16),
        V((users, depth), BF16),
        V((depth, E), BF16), V((depth, E), BF16),
        V((users * hist, E), F32), V((users, E), F32), V((users, E), F32), V((users, 128), F32),
        V((users, E), F32), V((users, 128), F32),
        V((NU, users, E), BF16), V((CORES, NS, users, E), BF16), V((NI, 1, 128), F32), V((NI, users, 128), F32),
        V((NU, 1, NU * users), F32), V((NU, 1, NU * users), F32),
        V((NI * users, NU * users), BF16),
        V((CORES, NS, users, E), BF16), V((NS, users, E), F32), V((NS, users, E), BF16),
        V((NS - 1, users, E), BF16),
        V((NU, users, E), BF16), V((NU - 1, users, E), BF16),
        V((COLOURS, 2 * users * hist, CW), BF16), V((CORES, N, users, E), BF16),
        V((N // XL, N * CORES, users, feat), BF16), V((QN * feat, 2 * users * hist), BF16),
        V((COLOURS, N, N, N, rows, CW), BF16), V((COLOURS, N - 1, N, N, rows, CW), BF16),
        V((COLOURS, N, N, rows, CW), BF16), V((COLOURS, N - 1, N, rows, CW), BF16),
        V((COLOURS, N, rows, CW), BF16), V((COLOURS, N - 1, rows, CW), BF16),
        V((N, N, rows, E), BF16), V((N * N - 1, rows, E), BF16),
        V((3, N, 8, 128), F32), V((CORES, 8, 128), F32),
        pltpu.SMEM((1,), F32), pltpu.SMEM((1,), F32), V((1, users), jnp.int32), V((1, users), jnp.int32),
        dma(8), dma(QN), dma(QN), dma(N * CORES - 1, N // XL), dma(N * CORES - 1, N // XL),
        dma(NI - 1), dma(NI - 1), dma(NU - 1), dma(NU - 1), dma(NU - 1), dma(NU - 1),
        dma(NS - 1), dma(NS - 1), dma(NU - 1), dma(NU - 1),
        dma(NS - 1), dma(NS - 1), dma(NU - 1), dma(NU - 1), dma(COLOURS), dma(COLOURS), dma(N - 1), dma(N - 1),
        dma(COLOURS, N - 1, 2), dma(COLOURS, N - 1, 2), dma(COLOURS, 2, N - 1), dma(COLOURS, 2, N - 1),
        dma(N * N - 1), dma(N * N - 1), dma(3, N - 1), dma(3, N - 1), dma(4), dma(4),
    ]
    outs = pl.pallas_call(
        functools.partial(tower_kernel, N, XL, total),
        name="two_tower",
        out_shape=(
            jax.ShapeDtypeStruct((8, 128), F32),
            jax.ShapeDtypeStruct((users, E), F32),
            jax.ShapeDtypeStruct((rows, E), F32),
            jax.ShapeDtypeStruct((rows, E), F32),
        ),
        in_specs=[hbm] * 8,
        out_specs=(vmem,) * 4,
        scratch_shapes=scratch,
        compiler_params=pltpu.CompilerParams(
            collective_id=0, has_side_effects=True, vmem_limit_bytes=60 * 1024 * 1024
        ),
    )(
        past.reshape(users * hist, depth), cand, wu, wi, scale, shift,
        ids.reshape(1, users), slots.reshape(1, users),
    )
    return pl.pallas_call(
        hand_out,
        name="hand_out",
        out_shape=(
            jax.ShapeDtypeStruct((1,), F32),
            jax.ShapeDtypeStruct((users, E), F32),
            jax.ShapeDtypeStruct((rows, E), F32),
            jax.ShapeDtypeStruct((rows, E), F32),
        ),
        in_specs=[vmem] * 4,
        out_specs=(smem, vmem, vmem, vmem),
    )(*outs)


def solution(mesh):
    group = mesh.shape["group"]
    n = {128: 4, 16: 2}[mesh.size]
    both = ("blk", "group")
    return jax.shard_map(
        functools.partial(shards, n, group // n),
        mesh=mesh,
        in_specs=(P(both, None, None), P(both, None), P(), P(), P(), P(), P(both), P(both)),
        out_specs=(P(), P(both, None), P(both, None), P(both, None)),
        check_vma=False,
    )
```

```python
import functools

import jax
import jax.numpy as jnp
from jax import lax
from jax.experimental import pallas as pl
from jax.experimental.pallas import tpu as pltpu
from jax.sharding import PartitionSpec as P

EPS = 1e-06
MESH = pl.DeviceIdType.MESH
F32 = jnp.float32
BF16 = jnp.bfloat16
CORES = 2
COLOURS = 3
HOME = 2


def dot(a, b):
    return jnp.dot(a, b, preferred_element_type=F32)


def dot_t(a, b):
    return lax.dot_general(a, b, (((0,), (0,)), ((), ())), preferred_element_type=F32)


def dot_nt(a, b):
    return lax.dot_general(a, b, (((1,), (1,)), ((), ())), preferred_element_type=F32)


def sigmoid(v):
    return 1.0 / (1.0 + jnp.exp(-v))


def tower_kernel(
    N, XL, TOTAL,
    x_hbm, ci_hbm, wu_hbm, wi_hbm, scale_ref, shift_ref, ids_ref, slot_ref,
    loss_ref, ig_ref, gu_ref, gi_ref,
    xv, xs, civ, wuv, wiv, pre, pooled, gp, ulen, inorm, ilen,
    ua, ia, idrow, idbuf, slotbuf, tgtbuf, wt, pig, pigf, rigc, rig, pgu, rgu, g, gi, xi, xt,
    part, ra0, ra1, ra2, sa, rb, parti, ri, losses, corelosses, scale_s, shift_s, idv, slotv,
    lsem, xsem_s, xsem_r, xi_s, xi_r, id_s, id_r, slot_s, slot_r, tgt_s, tgt_r,
    ia_s, ia_r, ua_s, ua_r, ig_s, ig_r, ug_s, ug_r, g_s, g_r, gi_s, gi_r,
    ra_s, ra_r, rs_s, rs_r, ri_s, ri_r, lo_s, lo_r, hop_s, hop_r,
):
    USERS, E = pooled.shape
    HIST = xv.shape[0] // USERS
    FEAT = 128 if N == 4 else XL * N * 16
    QN = (N // XL) * N
    NU = XL * N
    NI = XL * N * CORES
    NS = XL * N
    CW = E // COLOURS
    XH = N // XL
    ROWS = USERS * HIST
    blk = lax.axis_index("blk")
    group = lax.axis_index("group")
    c = lax.rem(blk, CORES)
    z = lax.rem(blk // CORES, N)
    x = (blk // (CORES * N)) * XL + group // N
    y = lax.rem(group, N)
    odd = lax.rem(x, 2)
    pair_a = x + 1 - 2 * odd
    pair_b = lax.rem(x + N - 1 + 2 * odd, N)

    def device(px, py, pz, pc):
        return (((px // XL) * N + pz) * CORES + pc, lax.rem(px, XL) * N + py)

    def plus(v, d, n):
        return v if d == 0 else lax.rem(v + d, n)

    def minus(v, d, n):
        return v if d == 0 else lax.rem(v + n - d, n)

    def send(src, dst, ssem, rsem, to):
        copy = pltpu.make_async_remote_copy(
            src_ref=src, dst_ref=dst, send_sem=ssem, recv_sem=rsem, device_id=to, device_id_type=MESH
        )
        copy.start()
        sent.append(copy)
        return copy

    def arrived(dst, sem):
        pltpu.make_async_remote_copy(
            src_ref=dst, dst_ref=dst, send_sem=sem, recv_sem=sem, device_id=sibling, device_id_type=MESH
        ).wait_recv()

    def left(src, sem):
        pltpu.make_async_remote_copy(
            src_ref=src, dst_ref=src, send_sem=sem, recv_sem=sem, device_id=sibling, device_id_type=MESH
        ).wait_send()

    sent = []
    sibling = device(x, y, z, 1 - c)
    def ring(d):
        return min(d, N - d)

    span = range(N)
    user_peers = [(da, dy) for da in range(2) for dy in span if (da, dy) != (0, 0)]
    user_peers.sort(key=lambda p: -p[0] - ring(p[1]))
    near_items = [(db, dz, 0) for db in range(2) for dz in span if (db, dz) != (0, 0)]
    near_items.sort(key=lambda p: -p[0] - ring(p[1]))
    item_peers = near_items + [(db, dz, 1) for db in range(2) for dz in span]
    planes = [(di, dj) for di in span for dj in span if (di, dj) != (0, 0)]
    planes.sort(key=lambda p: -ring(p[0]) - ring(p[1]))
    steps = sorted(range(1, N), key=lambda d: -ring(d))

    def user_peer(da, dy):
        return device(pair_a if da else x, plus(y, dy, N), z, c)

    def user_slot(da, dy):
        return (1 - odd if da else odd) * N + plus(y, dy, N)

    def item_slot(db, dz, dc):
        return dc * NS + db * N + dz

    def item_peer(db, dz, dc):
        return device(pair_b if db else x, y, plus(z, dz, N), plus(c, dc, CORES))

    def item_owner(db, dz, dc):
        return device(pair_b if db else x, y, minus(z, dz, N), plus(c, dc, CORES))

    def row_peer(dx, dy):
        return device(plus(x, dx, N), plus(y, dy, N), z, c)

    small = [
        pltpu.make_async_copy(a, b, lsem.at[4 + n])
        for n, (a, b) in enumerate(((ids_ref, idv), (slot_ref, slotv), (scale_ref, scale_s), (shift_ref, shift_s)))
    ]
    for load in small:
        load.start()
    load_ci = pltpu.make_async_copy(ci_hbm, civ, lsem.at[0])
    load_wi = pltpu.make_async_copy(wi_hbm, wiv, lsem.at[1])
    load_x = pltpu.make_async_copy(x_hbm, xv, lsem.at[2])
    load_wu = pltpu.make_async_copy(wu_hbm, wuv, lsem.at[3])
    for load in (load_ci, load_wi, load_x, load_wu):
        load.start()

    barrier = pltpu.get_barrier_semaphore()
    greeted = [row_peer(*d) for d in planes]
    greeted += [device(plus(x, dx, N), y, plus(z, dz, N), c) for dx in range(N) for dz in range(1, N)]
    greeted += [device(x, plus(y, dy, N), plus(z, dz, N), c) for dy in range(1, N) for dz in range(1, N)]
    greeted += [item_peer(*d) for d in item_peers if d[2]]
    for to in greeted:
        pl.semaphore_signal(barrier, inc=1, device_id=to, device_id_type=MESH)
    for load in small:
        load.wait()
    my_user_slot = user_slot(0, 0)
    rows = lax.broadcasted_iota(jnp.int32, (USERS, USERS), 0)
    lanes = lax.broadcasted_iota(jnp.int32, (USERS, USERS), 1)
    id_col = jnp.sum(jnp.where(rows == lanes, idv[...].astype(F32), 0.0), axis=1, keepdims=True)
    slot_col = jnp.sum(jnp.where(rows == lanes, slotv[...].astype(F32), 0.0), axis=1, keepdims=True)
    tile_rows = lax.broadcasted_iota(jnp.int32, (USERS, 128), 0)
    tile_lanes = lax.broadcasted_iota(jnp.int32, (USERS, 128), 1)
    idrow[0] = jnp.sum(jnp.where(tile_rows == tile_lanes, id_col, 0.0), axis=0, keepdims=True)
    wide_rows = lax.broadcasted_iota(jnp.int32, (USERS, NU * USERS), 0)
    wide_lanes = lax.broadcasted_iota(jnp.int32, (USERS, NU * USERS), 1)
    slotbuf[0] = jnp.sum(
        jnp.where(wide_lanes == wide_rows + my_user_slot * USERS, slot_col, 0.0), axis=0, keepdims=True
    )
    load_ci.wait()
    load_wi.wait()
    item_pre = dot(civ[...], wiv[...])
    item_len = jnp.sqrt(jnp.sum(item_pre * item_pre, axis=1, keepdims=True) + EPS)
    item_normed = item_pre / item_len
    inorm[...] = item_normed
    ilen[...] = jnp.broadcast_to(item_len, (USERS, 128))
    ia[0, 0] = item_normed.astype(BF16)
    pl.semaphore_wait(barrier, len(greeted))
    id_recv, slot_recv = [], []
    for n, d in enumerate(user_peers):
        slot_recv.append(send(slotbuf.at[0], slotbuf.at[n + 1], slot_s.at[n], slot_r.at[n], user_peer(*d)))
    for n, d in enumerate(item_peers):
        id_recv.append(send(idrow.at[0], idrow.at[item_slot(*d)], id_s.at[n], id_r.at[n], item_peer(*d)))
    ia_recv = []
    for n, d in enumerate(near_items):
        ia_recv.append(send(ia.at[0, 0], ia.at[0, item_slot(*d)], ia_s.at[n], ia_r.at[n], item_peer(*d)))
    load_x.wait()
    x_recv = []
    for q in range(QN):
        cols = pl.ds(pl.multiple_of((q * CORES + 1 - c) * FEAT, FEAT), FEAT)
        x_recv.append(send(xv.at[:, cols], xs.at[q], xsem_s.at[q], xsem_r.at[q], sibling))
    load_wu.wait()

    def forward(n, _):
        cols = pl.ds(pl.multiple_of(n * 256, 256), 256)
        pre[:, cols] = dot(xv[...], wuv[:, cols])
        return 0

    lax.fori_loop(0, E // 256, forward, 0)

    for copy in slot_recv + id_recv:
        copy.wait_recv()
    slots = slotbuf[0]
    for n in range(1, NU):
        slots = slots + slotbuf[n]
    wide = NU * USERS // 128
    found = jnp.zeros((1, NU * USERS), F32)
    for dc in range(CORES):
        for db in range(2):
            for dz in range(N):
                s = item_slot(db, dz, dc)
                col = jnp.sum(jnp.where(tile_rows == tile_lanes, idrow[s], 0.0), axis=1, keepdims=True)
                ids = jnp.broadcast_to(col, (USERS, 128))
                idbuf[s] = ids
                ob, og = item_owner(db, dz, dc)
                at = (tile_rows + (ob * (XL * N) + og) * USERS).astype(F32)
                hit = jnp.concatenate([at] * wide, axis=1) == slots
                found = found + jnp.sum(
                    jnp.where(hit, jnp.concatenate([ids] * wide, axis=1), 0.0), axis=0, keepdims=True
                )
    tgtbuf[0] = found
    tgt_recv = []
    for n, d in enumerate(user_peers):
        tgt_recv.append(send(tgtbuf.at[0], tgtbuf.at[n + 1], tgt_s.at[n], tgt_r.at[n], user_peer(*d)))

    def pool(n, _):
        u = n // COLOURS
        cols = pl.ds(pl.multiple_of(lax.rem(n, COLOURS) * CW, CW), CW)
        v = pre[pl.ds(pl.multiple_of(u * 8 * HIST, 8 * HIST), 8 * HIST), cols]
        act = v * sigmoid(v)
        pooled[pl.ds(pl.multiple_of(u * 8, 8), 8), cols] = jnp.sum(act.reshape(8, HIST, CW), axis=1) / HIST
        return 0

    lax.fori_loop(0, (USERS // 8) * COLOURS, pool, 0)
    mean = pooled[...]
    user_len = jnp.sqrt(jnp.sum(mean * mean, axis=1, keepdims=True) + EPS)
    user_normed = mean / user_len
    ulen[...] = jnp.broadcast_to(user_len, (USERS, 128))
    pooled[...] = user_normed
    ua[my_user_slot] = user_normed.astype(BF16)
    ua_recv = []
    for n, d in enumerate(user_peers):
        ua_recv.append(send(ua.at[my_user_slot], ua.at[my_user_slot], ua_s.at[n], ua_r.at[n], user_peer(*d)))

    xi_recv = []
    for n, (db, dz, dc) in enumerate(item_peers):
        px, pz, pc = pair_b if db else x, plus(z, dz, N), plus(c, dc, CORES)
        cols = pl.ds(pl.multiple_of(((px // XL * N + pz) * CORES + pc) * FEAT, FEAT), FEAT)
        xi_recv.append(
            send(civ.at[:, cols], xi.at[item_slot(db, dz, dc)], xi_s.at[n], xi_r.at[n], item_peer(db, dz, dc))
        )
    xi[0] = civ[:, pl.ds(pl.multiple_of(((x // XL * N + z) * CORES + c) * FEAT, FEAT), FEAT)]
    for copy in ia_recv:
        copy.wait_recv()
    ia_hop = send(ia.at[0], ia.at[1], hop_s.at[0], hop_r.at[0], sibling)
    for copy in x_recv:
        copy.wait_recv()

    def turn(q, _):
        cols = pl.ds(pl.multiple_of((q * CORES + c) * FEAT, FEAT), FEAT)
        to = pl.ds(pl.multiple_of(q * FEAT, FEAT), FEAT)
        xt[to, 0:ROWS] = xv[:, cols].T
        xt[to, ROWS:2 * ROWS] = xs[q].T
        return 0

    lax.fori_loop(0, QN, turn, 0)
    for copy in tgt_recv:
        copy.wait_recv()
    targets = tgtbuf[0]
    for n in range(1, NU):
        targets = targets + tgtbuf[n]

    for copy in ua_recv:
        copy.wait_recv()
    ia_hop.wait_recv()
    scale = scale_s[0]
    shift = shift_s[0]
    users = ua[...].reshape(NU * USERS, E)
    loss = jnp.zeros((8, 128), F32)
    for n in range(NI // N):
        items = ia[n // 2, (n % 2) * N:(n % 2 + 1) * N].reshape(N * USERS, E)
        scores = dot_nt(items, users)
        ids = idbuf[n * N:(n + 1) * N].reshape(N * USERS, 128)
        sign = jnp.where(jnp.concatenate([ids] * wide, axis=1) == targets, 1.0, -1.0)
        margin = sign * (scale * scores + shift)
        e = jnp.exp(-jnp.abs(margin))
        terms = jnp.log1p(e) + jnp.maximum(-margin, 0.0)
        gate = jnp.where(margin >= 0.0, e, 1.0) / (1.0 + e)
        wt[n * N * USERS:(n + 1) * N * USERS, :] = (-scale * sign * gate).astype(BF16)
        terms = jnp.sum(terms.reshape(N * USERS // 8, 8, NU * USERS), axis=0)
        for j in range(wide):
            loss = loss + terms[:, j * 128:(j + 1) * 128]
    def reduce_loss(value, step, pos):
        losses[step, pos] = value
        copies = []
        for d in range(1, N):
            at = [x, y, z]
            at[step] = plus(pos, d, N)
            copies.append(
                send(losses.at[step, pos], losses.at[step, pos], lo_s.at[step, d - 1], lo_r.at[step, d - 1],
                     device(at[0], at[1], at[2], c))
            )
        return copies

    def reduced_loss(step):
        total = losses[step, 0]
        for d in range(1, N):
            total = total + losses[step, d]
        return total

    loss_copies = reduce_loss(loss, 0, x)
    pgu[...] = dot_t(wt[...], ia[...].reshape(NI * USERS, E)).astype(BF16).reshape(NU, USERS, E)
    ug_recv = []
    for n, d in enumerate(user_peers):
        ug_recv.append(send(pgu.at[user_slot(*d)], rgu.at[n], ug_s.at[n], ug_r.at[n], user_peer(*d)))
    pig[1] = dot(wt[NS * USERS:2 * NS * USERS, :], users).astype(BF16).reshape(NS, USERS, E)
    ig_hop = send(pig.at[1], rigc, hop_s.at[1], hop_r.at[1], sibling)
    pigf[...] = dot(wt[0:NS * USERS, :], users).reshape(NS, USERS, E)
    ig_hop.wait_recv()
    ig_recv = []
    for s in range(NS):
        pigf[s] = pigf[s] + rigc[s].astype(F32)
        if s > 0:
            pig[0, s] = pigf[s].astype(BF16)
    for n, d in enumerate(near_items):
        ig_recv.append(send(pig.at[0, item_slot(*d)], rig.at[n], ig_s.at[n], ig_r.at[n], item_owner(*d)))

    for copy in ug_recv:
        copy.wait_recv()
    grad_users = pgu[my_user_slot].astype(F32)
    for n in range(len(user_peers)):
        grad_users = grad_users + rgu[n].astype(F32)
    user_normed = pooled[...]
    radial = jnp.sum(user_normed * grad_users, axis=1, keepdims=True)
    gp[...] = (grad_users - user_normed * radial) / ulen[:, 0:1] / HIST

    pos = (x, y, z)

    def backward(k, _):
        cols = pl.ds(pl.multiple_of(k * CW, CW), CW)

        def step(u, _):
            at = pl.ds(pl.multiple_of(u * 8 * HIST, 8 * HIST), 8 * HIST)
            v = pre[at, cols]
            s = sigmoid(v)
            outer = jnp.broadcast_to(gp[pl.ds(pl.multiple_of(u * 8, 8), 8), cols][:, None, :], (8, HIST, CW))
            g[k, at] = (outer.reshape(8 * HIST, CW) * s * (1.0 + v * (1.0 - s))).astype(BF16)
            return 0

        lax.fori_loop(0, USERS // 8, step, 0)
        pltpu.make_async_remote_copy(
            src_ref=g.at[k, pl.ds(0, ROWS)], dst_ref=g.at[k, pl.ds(ROWS, ROWS)], send_sem=g_s.at[k],
            recv_sem=g_r.at[k], device_id=sibling, device_id_type=MESH,
        ).start()
        return 0

    def towards(axis, v):
        at = list(pos)
        at[axis] = v
        return device(at[0], at[1], at[2], c)

    def item_home():
        for copy in ig_recv:
            copy.wait_recv()
        item_grad = pigf[0]
        for n in range(len(near_items)):
            item_grad = item_grad + rig[n].astype(F32)
        ig_ref[...] = item_grad
        item_normed = inorm[...]
        radial = jnp.sum(item_normed * item_grad, axis=1, keepdims=True)
        gi[0, 0] = ((item_grad - item_normed * radial) / ilen[:, 0:1]).astype(BF16)
        for n, d in enumerate(near_items):
            pltpu.make_async_remote_copy(
                src_ref=gi.at[0, 0], dst_ref=gi.at[0, item_slot(*d)], send_sem=gi_s.at[n], recv_sem=gi_r.at[n],
                device_id=item_peer(*d), device_id_type=MESH,
            ).start()

    depth = QN // XH * FEAT

    def weight_grad(m, _):
        half, k = m // COLOURS, lax.rem(m, COLOURS)
        xh = jnp.where(half == 0, XH - 1 - x // XL, x // XL)

        @pl.when(half == 0)
        def _():
            arrived(g.at[k, pl.ds(ROWS, ROWS)], g_r.at[k])

        pl.when(m == HOME)(item_home)
        r = dot(xt[pl.ds(pl.multiple_of(xh * depth, depth), depth)], g[k])
        part[k, xh] = r.astype(BF16).reshape(N, XL, N, 16, CW)

        def go(src, dst, sems, to):
            pltpu.make_async_remote_copy(
                src_ref=src, dst_ref=dst, send_sem=ra_s.at[sems], recv_sem=ra_r.at[sems], device_id=to,
                device_id_type=MESH,
            ).start()

        for xl in range(XL):
            t = xh * XL + xl
            d = lax.rem(t - x + N, N) - 1

            @pl.when((k == 0) & (t != x))
            def _(t=t, xl=xl, d=d):
                go(part.at[0, xh, :, xl], ra0.at[d], (0, d, 0), towards(0, t))

        @pl.when(k == 1)
        def _():
            for d in steps:
                t = plus(y, d, N)
                go(part.at[1, xh, :, :, t], ra1.at[d - 1, xh], (1, d - 1, half), towards(1, t))

        @pl.when(k == 2)
        def _():
            for d in steps:
                t = plus(z, d, N)
                go(part.at[2, xh, t], ra2.at[d - 1, xh], (2, d - 1, half), towards(2, t))

        return 0

    def slabs(k, d):
        if k == 0:
            return [ra0.at[d]]
        return [(ra1 if k == 1 else ra2).at[d, h] for h in range(XH)]

    lax.fori_loop(0, COLOURS, backward, 0)
    for copy in loss_copies:
        copy.wait_recv()
    loss_copies = reduce_loss(reduced_loss(0), 1, y)
    lax.fori_loop(0, 2 * COLOURS, weight_grad, 0)
    for copy in loss_copies:
        copy.wait_recv()
    loss_copies = reduce_loss(reduced_loss(1), 2, z)
    flight = {}

    def add_a(k):
        for d in range(N - 1):
            for h, slab in enumerate(slabs(k, d)):
                arrived(slab, ra_r.at[k, d, h])
        p1, p2 = pos[(k + 1) % 3], pos[(k + 2) % 3]

        def step(n, _):
            i, j = n // N, lax.rem(n, N)
            if k == 0:
                own, got = part.at[0, x // XL, j, lax.rem(x, XL), i], lambda d: ra0[d, j, i]
            elif k == 1:
                own, got = part.at[1, j // XL, i, lax.rem(j, XL), y], lambda d: ra1[d, j // XL, i, lax.rem(j, XL)]
            else:
                own, got = part.at[2, i // XL, z, lax.rem(i, XL), j], lambda d: ra2[d, i // XL, lax.rem(i, XL), j]
            total = own[...].astype(F32)
            for d in range(N - 1):
                total = total + got(d).astype(F32)
            sa[k, i, j] = total.astype(BF16)
            return 0

        lax.fori_loop(0, N * N, step, 0)
        flight[k] = []
        for n, (di, dj) in enumerate(planes):
            at = list(pos)
            i, j = plus(p1, di, N), plus(p2, dj, N)
            at[(k + 1) % 3], at[(k + 2) % 3] = i, j
            to = device(at[0], at[1], at[2], c)
            flight[k].append(send(sa.at[k, i, j], rb.at[k, n], rs_s.at[k, n], rs_r.at[k, n], to))

    def add_b(k):
        for copy in flight[k]:
            copy.wait_recv()
        total = sa[k, pos[(k + 1) % 3], pos[(k + 2) % 3]].astype(F32)
        for n in range(len(planes)):
            total = total + rb[k, n].astype(F32)
        gu_ref[:, k * CW:(k + 1) * CW] = total

    add_a(0)
    for n, d in enumerate(near_items):
        arrived(gi.at[0, item_slot(*d)], gi_r.at[n])
    gi_hop = send(gi.at[0], gi.at[1], hop_s.at[2], hop_r.at[2], sibling)
    add_a(1)
    for copy in xi_recv:
        copy.wait_recv()
    gi_hop.wait_recv()
    r = dot_t(xi[...].reshape(NI * USERS, FEAT), gi[...].reshape(NI * USERS, E)).astype(BF16)
    parti[...] = r.reshape(NU, 16, E)
    ri_recv = []
    for n, d in enumerate(user_peers):
        ri_recv.append(send(parti.at[user_slot(*d)], ri.at[n], ri_s.at[n], ri_r.at[n], user_peer(*d)))
    add_a(2)
    for copy in loss_copies:
        copy.wait_recv()
    corelosses[c] = reduced_loss(2)
    core_copy = send(corelosses.at[c], corelosses.at[c], hop_s.at[3], hop_r.at[3], sibling)
    add_b(0)
    add_b(1)
    core_copy.wait_recv()
    loss_ref[...] = jnp.broadcast_to(jnp.sum(corelosses[0] + corelosses[1], keepdims=True) / TOTAL, (8, 128))
    for copy in ri_recv:
        copy.wait_recv()
    total = parti[my_user_slot].astype(F32)
    for n in range(len(user_peers)):
        total = total + ri[n].astype(F32)
    gi_ref[...] = total
    add_b(2)
    for copy in sent:
        copy.wait_send()
    for k in range(COLOURS):
        left(g.at[k, pl.ds(0, ROWS)], g_s.at[k])
        for d in range(N - 1):
            for h, slab in enumerate(slabs(k, d)):
                left(slab, ra_s.at[k, d, h])
    for n in range(len(near_items)):
        left(gi.at[0, 0], gi_s.at[n])


def hand_out(loss, ig, gu, gi, loss_out, ig_out, gu_out, gi_out):
    loss_out[0] = loss[0, 0]
    ig_out[...] = ig[...]
    gu_out[...] = gu[...]
    gi_out[...] = gi[...]


def shards(N, XL, past, cand, wu, wi, scale, shift, ids, slots):
    users, hist, depth = past.shape
    E = wu.shape[1]
    total = users * lax.axis_size("blk") * lax.axis_size("group")
    NU, NI, NS, QN = XL * N, XL * N * CORES, XL * N, (N // XL) * N
    feat = depth // (QN * CORES)
    hbm = pl.BlockSpec(memory_space=pltpu.HBM)
    smem = pl.BlockSpec(memory_space=pltpu.SMEM)
    vmem = pl.BlockSpec(memory_space=pltpu.VMEM)
    rows = depth // (N * N * N * CORES)
    CW = E // COLOURS

    def dma(*shape):
        return pltpu.SemaphoreType.DMA(shape)

    V = pltpu.VMEM
    scratch = [
        V((users * hist, depth), BF16), V((QN, users * hist, feat), BF16),
        V((users, depth), BF16),
        V((depth, E), BF16), V((depth, E), BF16),
        V((users * hist, E), F32), V((users, E), F32), V((users, E), F32), V((users, 128), F32),
        V((users, E), F32), V((users, 128), F32),
        V((NU, users, E), BF16), V((CORES, NS, users, E), BF16), V((NI, 1, 128), F32), V((NI, users, 128), F32),
        V((NU, 1, NU * users), F32), V((NU, 1, NU * users), F32),
        V((NI * users, NU * users), BF16),
        V((CORES, NS, users, E), BF16), V((NS, users, E), F32), V((NS, users, E), BF16),
        V((NS - 1, users, E), BF16),
        V((NU, users, E), BF16), V((NU - 1, users, E), BF16),
        V((COLOURS, 2 * users * hist, CW), BF16), V((CORES, NS, users, E), BF16),
        V((NI, users, feat), BF16), V((QN * feat, 2 * users * hist), BF16),
        V((COLOURS, N // XL, N, XL, N, rows, CW), BF16), V((N - 1, N, N, rows, CW), BF16),
        V((N - 1, N // XL, N, XL, rows, CW), BF16), V((N - 1, N // XL, XL, N, rows, CW), BF16),
        V((COLOURS, N, N, rows, CW), BF16), V((COLOURS, N * N - 1, rows, CW), BF16),
        V((NU, rows, E), BF16), V((NU - 1, rows, E), BF16),
        V((3, N, 8, 128), F32), V((CORES, 8, 128), F32),
        pltpu.SMEM((1,), F32), pltpu.SMEM((1,), F32), V((1, users), jnp.int32), V((1, users), jnp.int32),
        dma(8), dma(QN), dma(QN), dma(NI - 1), dma(NI - 1),
        dma(NI - 1), dma(NI - 1), dma(NU - 1), dma(NU - 1), dma(NU - 1), dma(NU - 1),
        dma(NS - 1), dma(NS - 1), dma(NU - 1), dma(NU - 1),
        dma(NS - 1), dma(NS - 1), dma(NU - 1), dma(NU - 1), dma(COLOURS), dma(COLOURS), dma(NS - 1), dma(NS - 1),
        dma(COLOURS, N - 1, 2), dma(COLOURS, N - 1, 2), dma(COLOURS, N * N - 1), dma(COLOURS, N * N - 1),
        dma(NU - 1), dma(NU - 1), dma(3, N - 1), dma(3, N - 1), dma(4), dma(4),
    ]
    outs = pl.pallas_call(
        functools.partial(tower_kernel, N, XL, total),
        name="two_tower",
        out_shape=(
            pltpu.VMEM((8, 128), F32),
            pltpu.VMEM((users, E), F32),
            pltpu.VMEM((rows, E), F32),
            pltpu.VMEM((rows, E), F32),
        ),
        in_specs=[hbm] * 8,
        out_specs=(vmem,) * 4,
        scratch_shapes=scratch,
        compiler_params=pltpu.CompilerParams(
            collective_id=0, has_side_effects=True, vmem_limit_bytes=60 * 1024 * 1024
        ),
    )(
        past.reshape(users * hist, depth), cand, wu, wi, scale, shift,
        ids.reshape(1, users), slots.reshape(1, users),
    )
    return pl.pallas_call(
        hand_out,
        name="hand_out",
        out_shape=(
            jax.ShapeDtypeStruct((1,), F32),
            jax.ShapeDtypeStruct((users, E), F32),
            jax.ShapeDtypeStruct((rows, E), F32),
            jax.ShapeDtypeStruct((rows, E), F32),
        ),
        in_specs=[vmem] * 4,
        out_specs=(smem, vmem, vmem, vmem),
        compiler_params=pltpu.CompilerParams(vmem_limit_bytes=4 * 1024 * 1024),
    )(*outs)


def solution(mesh):
    group = mesh.shape["group"]
    n = {128: 4, 16: 2}[mesh.size]
    both = ("blk", "group")
    return jax.shard_map(
        functools.partial(shards, n, group // n),
        mesh=mesh,
        in_specs=(P(both, None, None), P(both, None), P(), P(), P(), P(), P(both), P(both)),
        out_specs=(P(), P(both, None), P(both, None), P(both, None)),
        check_vma=False,
    )
```

```python
import functools

import jax
import jax.numpy as jnp
from jax import lax
from jax.experimental import pallas as pl
from jax.experimental.pallas import tpu as pltpu
from jax.sharding import PartitionSpec as P

EPS = 1e-06
MESH = pl.DeviceIdType.MESH
F32 = jnp.float32
BF16 = jnp.bfloat16
CORES = 2
COLOURS = 3


def dot(a, b):
    return jnp.dot(a, b, preferred_element_type=F32)


def dot_t(a, b):
    return lax.dot_general(a, b, (((0,), (0,)), ((), ())), preferred_element_type=F32)


def dot_nt(a, b):
    return lax.dot_general(a, b, (((1,), (1,)), ((), ())), preferred_element_type=F32)


def sigmoid(v):
    return 1.0 / (1.0 + jnp.exp(-v))


def tower_kernel(
    N, XL, TOTAL,
    x_hbm, ci_hbm, wu_hbm, wi_hbm, scale_ref, shift_ref, ids_ref, slot_ref,
    loss_ref, ig_ref, gu_ref, gi_ref,
    xv, xs, civ, wuv, wiv, pre, pooled, gp, ulen, inorm, ilen,
    ua, ia, idrow, idbuf, slotbuf, tgtbuf, wt, pig, pigf, rigc, rig, pgu, rgu, g, gi, xi, xt,
    part, ra0, ra1, ra2, sa, rb, parti, ri, losses, corelosses, scale_s, shift_s, idv, slotv,
    lsem, xsem_s, xsem_r, xi_s, xi_r, id_s, id_r, slot_s, slot_r, tgt_s, tgt_r,
    ia_s, ia_r, ua_s, ua_r, ig_s, ig_r, ug_s, ug_r, g_s, g_r, gi_s, gi_r,
    ra_s, ra_r, rs_s, rs_r, ri_s, ri_r, lo_s, lo_r, hop_s, hop_r,
):
    USERS, E = pooled.shape
    HIST = xv.shape[0] // USERS
    FEAT = 128 if N == 4 else XL * N * 16
    QN = (N // XL) * N
    NU = XL * N
    NI = XL * N * CORES
    NS = XL * N
    CW = E // COLOURS
    XH = N // XL
    ROWS = USERS * HIST
    blk = lax.axis_index("blk")
    group = lax.axis_index("group")
    c = lax.rem(blk, CORES)
    z = lax.rem(blk // CORES, N)
    x = (blk // (CORES * N)) * XL + group // N
    y = lax.rem(group, N)
    odd = lax.rem(x, 2)
    pair_a = x + 1 - 2 * odd
    pair_b = lax.rem(x + N - 1 + 2 * odd, N)

    def device(px, py, pz, pc):
        return (((px // XL) * N + pz) * CORES + pc, lax.rem(px, XL) * N + py)

    def plus(v, d, n):
        return v if d == 0 else lax.rem(v + d, n)

    def minus(v, d, n):
        return v if d == 0 else lax.rem(v + n - d, n)

    def send(src, dst, ssem, rsem, to):
        copy = pltpu.make_async_remote_copy(
            src_ref=src, dst_ref=dst, send_sem=ssem, recv_sem=rsem, device_id=to, device_id_type=MESH
        )
        copy.start()
        sent.append(copy)
        return copy

    def arrived(dst, sem):
        pltpu.make_async_remote_copy(
            src_ref=dst, dst_ref=dst, send_sem=sem, recv_sem=sem, device_id=sibling, device_id_type=MESH
        ).wait_recv()

    def left(src, sem):
        pltpu.make_async_remote_copy(
            src_ref=src, dst_ref=src, send_sem=sem, recv_sem=sem, device_id=sibling, device_id_type=MESH
        ).wait_send()

    sent = []
    sibling = device(x, y, z, 1 - c)
    def ring(d):
        return min(d, N - d)

    span = range(N)
    user_peers = [(da, dy) for da in range(2) for dy in span if (da, dy) != (0, 0)]
    user_peers.sort(key=lambda p: -p[0] - ring(p[1]))
    near_items = [(db, dz, 0) for db in range(2) for dz in span if (db, dz) != (0, 0)]
    near_items.sort(key=lambda p: -p[0] - ring(p[1]))
    item_peers = near_items + [(db, dz, 1) for db in range(2) for dz in span]
    planes = [(di, dj) for di in span for dj in span if (di, dj) != (0, 0)]
    planes.sort(key=lambda p: -ring(p[0]) - ring(p[1]))
    steps = sorted(range(1, N), key=lambda d: -ring(d))

    def user_peer(da, dy):
        return device(pair_a if da else x, plus(y, dy, N), z, c)

    def user_slot(da, dy):
        return (1 - odd if da else odd) * N + plus(y, dy, N)

    def item_slot(db, dz, dc):
        return dc * NS + db * N + dz

    def item_peer(db, dz, dc):
        return device(pair_b if db else x, y, plus(z, dz, N), plus(c, dc, CORES))

    def item_owner(db, dz, dc):
        return device(pair_b if db else x, y, minus(z, dz, N), plus(c, dc, CORES))

    def row_peer(dx, dy):
        return device(plus(x, dx, N), plus(y, dy, N), z, c)

    small = [
        pltpu.make_async_copy(a, b, lsem.at[4 + n])
        for n, (a, b) in enumerate(((ids_ref, idv), (slot_ref, slotv), (scale_ref, scale_s), (shift_ref, shift_s)))
    ]
    for load in small:
        load.start()
    load_ci = pltpu.make_async_copy(ci_hbm, civ, lsem.at[0])
    load_wi = pltpu.make_async_copy(wi_hbm, wiv, lsem.at[1])
    load_x = pltpu.make_async_copy(x_hbm, xv, lsem.at[2])
    load_wu = pltpu.make_async_copy(wu_hbm, wuv, lsem.at[3])
    for load in (load_ci, load_wi, load_x, load_wu):
        load.start()

    barrier = pltpu.get_barrier_semaphore()
    greeted = [row_peer(*d) for d in planes]
    greeted += [device(plus(x, dx, N), y, plus(z, dz, N), c) for dx in range(N) for dz in range(1, N)]
    greeted += [device(x, plus(y, dy, N), plus(z, dz, N), c) for dy in range(1, N) for dz in range(1, N)]
    greeted += [item_peer(*d) for d in item_peers if d[2]]
    for to in greeted:
        pl.semaphore_signal(barrier, inc=1, device_id=to, device_id_type=MESH)
    for load in small:
        load.wait()
    my_user_slot = user_slot(0, 0)
    rows = lax.broadcasted_iota(jnp.int32, (USERS, USERS), 0)
    lanes = lax.broadcasted_iota(jnp.int32, (USERS, USERS), 1)
    id_col = jnp.sum(jnp.where(rows == lanes, idv[...].astype(F32), 0.0), axis=1, keepdims=True)
    slot_col = jnp.sum(jnp.where(rows == lanes, slotv[...].astype(F32), 0.0), axis=1, keepdims=True)
    tile_rows = lax.broadcasted_iota(jnp.int32, (USERS, 128), 0)
    tile_lanes = lax.broadcasted_iota(jnp.int32, (USERS, 128), 1)
    idrow[0] = jnp.sum(jnp.where(tile_rows == tile_lanes, id_col, 0.0), axis=0, keepdims=True)
    wide_rows = lax.broadcasted_iota(jnp.int32, (USERS, NU * USERS), 0)
    wide_lanes = lax.broadcasted_iota(jnp.int32, (USERS, NU * USERS), 1)
    slotbuf[0] = jnp.sum(
        jnp.where(wide_lanes == wide_rows + my_user_slot * USERS, slot_col, 0.0), axis=0, keepdims=True
    )
    load_ci.wait()
    load_wi.wait()
    item_pre = dot(civ[...], wiv[...])
    item_len = jnp.sqrt(jnp.sum(item_pre * item_pre, axis=1, keepdims=True) + EPS)
    item_normed = item_pre / item_len
    inorm[...] = item_normed
    ilen[...] = jnp.broadcast_to(item_len, (USERS, 128))
    ia[0, 0] = item_normed.astype(BF16)
    pl.semaphore_wait(barrier, len(greeted))
    id_recv, slot_recv = [], []
    for n, d in enumerate(user_peers):
        slot_recv.append(send(slotbuf.at[0], slotbuf.at[n + 1], slot_s.at[n], slot_r.at[n], user_peer(*d)))
    for n, d in enumerate(item_peers):
        id_recv.append(send(idrow.at[0], idrow.at[item_slot(*d)], id_s.at[n], id_r.at[n], item_peer(*d)))
    ia_recv = []
    for n, d in enumerate(near_items):
        ia_recv.append(send(ia.at[0, 0], ia.at[0, item_slot(*d)], ia_s.at[n], ia_r.at[n], item_peer(*d)))
    load_x.wait()
    x_recv = []
    for q in range(QN):
        cols = pl.ds(pl.multiple_of((q * CORES + 1 - c) * FEAT, FEAT), FEAT)
        x_recv.append(send(xv.at[:, cols], xs.at[q], xsem_s.at[q], xsem_r.at[q], sibling))
    load_wu.wait()

    def forward(n, _):
        cols = pl.ds(pl.multiple_of(n * 256, 256), 256)
        pre[:, cols] = dot(xv[...], wuv[:, cols])
        return 0

    lax.fori_loop(0, E // 256, forward, 0)

    for copy in slot_recv + id_recv:
        copy.wait_recv()
    slots = slotbuf[0]
    for n in range(1, NU):
        slots = slots + slotbuf[n]
    wide = NU * USERS // 128
    found = jnp.zeros((1, NU * USERS), F32)
    for dc in range(CORES):
        for db in range(2):
            for dz in range(N):
                s = item_slot(db, dz, dc)
                col = jnp.sum(jnp.where(tile_rows == tile_lanes, idrow[s], 0.0), axis=1, keepdims=True)
                ids = jnp.broadcast_to(col, (USERS, 128))
                idbuf[s] = ids
                ob, og = item_owner(db, dz, dc)
                at = (tile_rows + (ob * (XL * N) + og) * USERS).astype(F32)
                hit = jnp.concatenate([at] * wide, axis=1) == slots
                found = found + jnp.sum(
                    jnp.where(hit, jnp.concatenate([ids] * wide, axis=1), 0.0), axis=0, keepdims=True
                )
    tgtbuf[0] = found
    tgt_recv = []
    for n, d in enumerate(user_peers):
        tgt_recv.append(send(tgtbuf.at[0], tgtbuf.at[n + 1], tgt_s.at[n], tgt_r.at[n], user_peer(*d)))

    def pool(n, _):
        u = n // COLOURS
        cols = pl.ds(pl.multiple_of(lax.rem(n, COLOURS) * CW, CW), CW)
        v = pre[pl.ds(pl.multiple_of(u * 8 * HIST, 8 * HIST), 8 * HIST), cols]
        act = v * sigmoid(v)
        pooled[pl.ds(pl.multiple_of(u * 8, 8), 8), cols] = jnp.sum(act.reshape(8, HIST, CW), axis=1) / HIST
        return 0

    lax.fori_loop(0, (USERS // 8) * COLOURS, pool, 0)
    mean = pooled[...]
    user_len = jnp.sqrt(jnp.sum(mean * mean, axis=1, keepdims=True) + EPS)
    user_normed = mean / user_len
    ulen[...] = jnp.broadcast_to(user_len, (USERS, 128))
    pooled[...] = user_normed
    ua[my_user_slot] = user_normed.astype(BF16)
    ua_recv = []
    for n, d in enumerate(user_peers):
        ua_recv.append(send(ua.at[my_user_slot], ua.at[my_user_slot], ua_s.at[n], ua_r.at[n], user_peer(*d)))

    xi_recv = []
    for n, (db, dz, dc) in enumerate(item_peers):
        px, pz, pc = pair_b if db else x, plus(z, dz, N), plus(c, dc, CORES)
        cols = pl.ds(pl.multiple_of(((px // XL * N + pz) * CORES + pc) * FEAT, FEAT), FEAT)
        xi_recv.append(
            send(civ.at[:, cols], xi.at[item_slot(db, dz, dc)], xi_s.at[n], xi_r.at[n], item_peer(db, dz, dc))
        )
    xi[0] = civ[:, pl.ds(pl.multiple_of(((x // XL * N + z) * CORES + c) * FEAT, FEAT), FEAT)]
    for copy in ia_recv:
        copy.wait_recv()
    ia_hop = send(ia.at[0], ia.at[1], hop_s.at[0], hop_r.at[0], sibling)
    for copy in x_recv:
        copy.wait_recv()

    def turn(q, _):
        cols = pl.ds(pl.multiple_of((q * CORES + c) * FEAT, FEAT), FEAT)
        to = pl.ds(pl.multiple_of(q * FEAT, FEAT), FEAT)
        xt[to, 0:ROWS] = xv[:, cols].T
        xt[to, ROWS:2 * ROWS] = xs[q].T
        return 0

    lax.fori_loop(0, QN, turn, 0)
    for copy in tgt_recv:
        copy.wait_recv()
    targets = tgtbuf[0]
    for n in range(1, NU):
        targets = targets + tgtbuf[n]

    for copy in ua_recv:
        copy.wait_recv()
    ia_hop.wait_recv()
    scale = scale_s[0, 0]
    shift = shift_s[0, 0]
    users = ua[...].reshape(NU * USERS, E)
    loss = jnp.zeros((8, 128), F32)
    for n in range(NI // N):
        items = ia[n // 2, (n % 2) * N:(n % 2 + 1) * N].reshape(N * USERS, E)
        scores = dot_nt(items, users)
        ids = idbuf[n * N:(n + 1) * N].reshape(N * USERS, 128)
        sign = jnp.where(jnp.concatenate([ids] * wide, axis=1) == targets, 1.0, -1.0)
        margin = sign * (scale * scores + shift)
        e = jnp.exp(-jnp.abs(margin))
        terms = jnp.log1p(e) + jnp.maximum(-margin, 0.0)
        gate = jnp.where(margin >= 0.0, e, 1.0) / (1.0 + e)
        wt[n * N * USERS:(n + 1) * N * USERS, :] = (-scale * sign * gate).astype(BF16)
        terms = jnp.sum(terms.reshape(N * USERS // 8, 8, NU * USERS), axis=0)
        for j in range(wide):
            loss = loss + terms[:, j * 128:(j + 1) * 128]
    def reduce_loss(value, step, pos):
        losses[step, pos] = value
        copies = []
        for d in range(1, N):
            at = [x, y, z]
            at[step] = plus(pos, d, N)
            copies.append(
                send(losses.at[step, pos], losses.at[step, pos], lo_s.at[step, d - 1], lo_r.at[step, d - 1],
                     device(at[0], at[1], at[2], c))
            )
        return copies

    def reduced_loss(step):
        total = losses[step, 0]
        for d in range(1, N):
            total = total + losses[step, d]
        return total

    loss_copies = reduce_loss(loss, 0, x)
    pgu[...] = dot_t(wt[...], ia[...].reshape(NI * USERS, E)).astype(BF16).reshape(NU, USERS, E)
    ug_recv = []
    for n, d in enumerate(user_peers):
        ug_recv.append(send(pgu.at[user_slot(*d)], rgu.at[n], ug_s.at[n], ug_r.at[n], user_peer(*d)))
    pig[1] = dot(wt[NS * USERS:2 * NS * USERS, :], users).astype(BF16).reshape(NS, USERS, E)
    ig_hop = send(pig.at[1], rigc, hop_s.at[1], hop_r.at[1], sibling)
    pigf[...] = dot(wt[0:NS * USERS, :], users).reshape(NS, USERS, E)
    ig_hop.wait_recv()
    ig_recv = []
    for s in range(NS):
        pigf[s] = pigf[s] + rigc[s].astype(F32)
        if s > 0:
            pig[0, s] = pigf[s].astype(BF16)
    for n, d in enumerate(near_items):
        ig_recv.append(send(pig.at[0, item_slot(*d)], rig.at[n], ig_s.at[n], ig_r.at[n], item_owner(*d)))

    for copy in ug_recv:
        copy.wait_recv()
    grad_users = pgu[my_user_slot].astype(F32)
    for n in range(len(user_peers)):
        grad_users = grad_users + rgu[n].astype(F32)
    user_normed = pooled[...]
    radial = jnp.sum(user_normed * grad_users, axis=1, keepdims=True)
    gp[...] = (grad_users - user_normed * radial) / ulen[:, 0:1] / HIST

    pos = (x, y, z)

    def backward(m, _):
        k = jnp.where(m < 2, 1 - m, m)
        cols = pl.ds(pl.multiple_of(k * CW, CW), CW)

        def step(u, _):
            at = pl.ds(pl.multiple_of(u * 8 * HIST, 8 * HIST), 8 * HIST)
            v = pre[at, cols]
            s = sigmoid(v)
            outer = jnp.broadcast_to(gp[pl.ds(pl.multiple_of(u * 8, 8), 8), cols][:, None, :], (8, HIST, CW))
            g[k, at] = (outer.reshape(8 * HIST, CW) * s * (1.0 + v * (1.0 - s))).astype(BF16)
            return 0

        lax.fori_loop(0, USERS // 8, step, 0)
        pltpu.make_async_remote_copy(
            src_ref=g.at[k, pl.ds(0, ROWS)], dst_ref=g.at[k, pl.ds(ROWS, ROWS)], send_sem=g_s.at[k],
            recv_sem=g_r.at[k], device_id=sibling, device_id_type=MESH,
        ).start()
        return 0

    def towards(axis, v):
        at = list(pos)
        at[axis] = v
        return device(at[0], at[1], at[2], c)

    def item_home():
        for copy in ig_recv:
            copy.wait_recv()
        item_grad = pigf[0]
        for n in range(len(near_items)):
            item_grad = item_grad + rig[n].astype(F32)
        ig_ref[...] = item_grad
        item_normed = inorm[...]
        radial = jnp.sum(item_normed * item_grad, axis=1, keepdims=True)
        gi[0, 0] = ((item_grad - item_normed * radial) / ilen[:, 0:1]).astype(BF16)
        for n, d in enumerate(near_items):
            pltpu.make_async_remote_copy(
                src_ref=gi.at[0, 0], dst_ref=gi.at[0, item_slot(*d)], send_sem=gi_s.at[n], recv_sem=gi_r.at[n],
                device_id=item_peer(*d), device_id_type=MESH,
            ).start()

    def weight_grad(m, _):
        k = jnp.where(m < 2, 1 - m, m)
        pl.when(m == 1)(item_home)
        arrived(g.at[k, pl.ds(ROWS, ROWS)], g_r.at[k])
        part[k] = dot(xt[...], g[k]).astype(BF16).reshape(XH, N, XL, N, 16, CW)
        for axis in range(COLOURS):

            @pl.when(k == axis)
            def _(axis=axis):
                for d in steps:
                    t = plus(pos[axis], d, N)
                    pltpu.make_async_remote_copy(
                        src_ref=slab(axis, t), dst_ref=ra[axis].at[d - 1], send_sem=ra_s.at[axis, d - 1],
                        recv_sem=ra_r.at[axis, d - 1], device_id=towards(axis, t), device_id_type=MESH,
                    ).start()

        return 0

    ra = (ra0, ra1, ra2)

    def slab(axis, t):
        if axis == 0:
            return part.at[0, t // XL, :, lax.rem(t, XL)]
        if axis == 1:
            return part.at[1, :, :, :, t]
        return part.at[2, :, t]

    lax.fori_loop(0, COLOURS, backward, 0)
    for copy in loss_copies:
        copy.wait_recv()
    loss_copies = reduce_loss(reduced_loss(0), 1, y)
    lax.fori_loop(0, COLOURS, weight_grad, 0)
    for copy in loss_copies:
        copy.wait_recv()
    loss_copies = reduce_loss(reduced_loss(1), 2, z)
    flight = {}

    def add_a(k):
        for d in range(N - 1):
            arrived(ra[k].at[d], ra_r.at[k, d])
        p1, p2 = pos[(k + 1) % 3], pos[(k + 2) % 3]

        def step(n, _):
            i, j = n // N, lax.rem(n, N)
            if k == 0:
                own, got = part.at[0, x // XL, j, lax.rem(x, XL), i], lambda d: ra0[d, j, i]
            elif k == 1:
                own, got = part.at[1, j // XL, i, lax.rem(j, XL), y], lambda d: ra1[d, j // XL, i, lax.rem(j, XL)]
            else:
                own, got = part.at[2, i // XL, z, lax.rem(i, XL), j], lambda d: ra2[d, i // XL, lax.rem(i, XL), j]
            total = own[...].astype(F32)
            for d in range(N - 1):
                total = total + got(d).astype(F32)
            sa[k, i, j] = total.astype(BF16)
            return 0

        lax.fori_loop(0, N * N, step, 0)
        flight[k] = []
        for n, (di, dj) in enumerate(planes):
            at = list(pos)
            i, j = plus(p1, di, N), plus(p2, dj, N)
            at[(k + 1) % 3], at[(k + 2) % 3] = i, j
            to = device(at[0], at[1], at[2], c)
            flight[k].append(send(sa.at[k, i, j], rb.at[k, n], rs_s.at[k, n], rs_r.at[k, n], to))

    def add_b(k):
        for copy in flight[k]:
            copy.wait_recv()
        total = sa[k, pos[(k + 1) % 3], pos[(k + 2) % 3]].astype(F32)
        for n in range(len(planes)):
            total = total + rb[k, n].astype(F32)
        gu_ref[:, k * CW:(k + 1) * CW] = total

    for n, d in enumerate(near_items):
        arrived(gi.at[0, item_slot(*d)], gi_r.at[n])
    gi_hop = send(gi.at[0], gi.at[1], hop_s.at[2], hop_r.at[2], sibling)
    add_a(1)
    for copy in xi_recv:
        copy.wait_recv()
    gi_hop.wait_recv()
    r = dot_t(xi[...].reshape(NI * USERS, FEAT), gi[...].reshape(NI * USERS, E)).astype(BF16)
    parti[...] = r.reshape(NU, 16, E)
    ri_recv = []
    for n, d in enumerate(user_peers):
        ri_recv.append(send(parti.at[user_slot(*d)], ri.at[n], ri_s.at[n], ri_r.at[n], user_peer(*d)))
    add_a(0)
    add_a(2)
    for copy in loss_copies:
        copy.wait_recv()
    corelosses[c] = reduced_loss(2)
    core_copy = send(corelosses.at[c], corelosses.at[c], hop_s.at[3], hop_r.at[3], sibling)
    add_b(1)
    add_b(0)
    core_copy.wait_recv()
    loss_ref[...] = jnp.broadcast_to(jnp.sum(corelosses[0] + corelosses[1], keepdims=True) / TOTAL, (8, 128))
    for copy in ri_recv:
        copy.wait_recv()
    total = parti[my_user_slot].astype(F32)
    for n in range(len(user_peers)):
        total = total + ri[n].astype(F32)
    gi_ref[...] = total
    add_b(2)
    for copy in sent:
        copy.wait_send()
    for k in range(COLOURS):
        left(g.at[k, pl.ds(0, ROWS)], g_s.at[k])
        for d in range(N - 1):
            left(ra[k].at[d], ra_s.at[k, d])
    for n in range(len(near_items)):
        left(gi.at[0, 0], gi_s.at[n])


def hand_out(loss, ig, gu, gi, loss_out, ig_out, gu_out, gi_out):
    loss_out[0] = loss[0, 0]
    ig_out[...] = ig[...]
    gu_out[...] = gu[...]
    gi_out[...] = gi[...]


def shards(N, XL, past, cand, wu, wi, scale, shift, ids, slots):
    users, hist, depth = past.shape
    E = wu.shape[1]
    total = users * lax.axis_size("blk") * lax.axis_size("group")
    NU, NI, NS, QN = XL * N, XL * N * CORES, XL * N, (N // XL) * N
    feat = depth // (QN * CORES)
    hbm = pl.BlockSpec(memory_space=pltpu.HBM)
    smem = pl.BlockSpec(memory_space=pltpu.SMEM)
    vmem = pl.BlockSpec(memory_space=pltpu.VMEM)
    rows = depth // (N * N * N * CORES)
    CW = E // COLOURS

    def dma(*shape):
        return pltpu.SemaphoreType.DMA(shape)

    V = pltpu.VMEM
    scratch = [
        V((users * hist, depth), BF16), V((QN, users * hist, feat), BF16),
        V((users, depth), BF16),
        V((depth, E), BF16), V((depth, E), BF16),
        V((users * hist, E), F32), V((users, E), F32), V((users, E), F32), V((users, 128), F32),
        V((users, E), F32), V((users, 128), F32),
        V((NU, users, E), BF16), V((CORES, NS, users, E), BF16), V((NI, 1, 128), F32), V((NI, users, 128), F32),
        V((NU, 1, NU * users), F32), V((NU, 1, NU * users), F32),
        V((NI * users, NU * users), BF16),
        V((CORES, NS, users, E), BF16), V((NS, users, E), F32), V((NS, users, E), BF16),
        V((NS - 1, users, E), BF16),
        V((NU, users, E), BF16), V((NU - 1, users, E), BF16),
        V((COLOURS, 2 * users * hist, CW), BF16), V((CORES, NS, users, E), BF16),
        V((NI, users, feat), BF16), V((QN * feat, 2 * users * hist), BF16),
        V((COLOURS, N // XL, N, XL, N, rows, CW), BF16), V((N - 1, N, N, rows, CW), BF16),
        V((N - 1, N // XL, N, XL, rows, CW), BF16), V((N - 1, N // XL, XL, N, rows, CW), BF16),
        V((COLOURS, N, N, rows, CW), BF16), V((COLOURS, N * N - 1, rows, CW), BF16),
        V((NU, rows, E), BF16), V((NU - 1, rows, E), BF16),
        V((3, N, 8, 128), F32), V((CORES, 8, 128), F32),
        V((1, 1), F32), V((1, 1), F32), V((1, users), jnp.int32), V((1, users), jnp.int32),
        dma(8), dma(QN), dma(QN), dma(NI - 1), dma(NI - 1),
        dma(NI - 1), dma(NI - 1), dma(NU - 1), dma(NU - 1), dma(NU - 1), dma(NU - 1),
        dma(NS - 1), dma(NS - 1), dma(NU - 1), dma(NU - 1),
        dma(NS - 1), dma(NS - 1), dma(NU - 1), dma(NU - 1), dma(COLOURS), dma(COLOURS), dma(NS - 1), dma(NS - 1),
        dma(COLOURS, N - 1), dma(COLOURS, N - 1), dma(COLOURS, N * N - 1), dma(COLOURS, N * N - 1),
        dma(NU - 1), dma(NU - 1), dma(3, N - 1), dma(3, N - 1), dma(4), dma(4),
    ]
    outs = pl.pallas_call(
        functools.partial(tower_kernel, N, XL, total),
        name="two_tower",
        out_shape=(
            pltpu.VMEM((8, 128), F32),
            pltpu.VMEM((users, E), F32),
            pltpu.VMEM((rows, E), F32),
            pltpu.VMEM((rows, E), F32),
        ),
        in_specs=[hbm] * 8,
        out_specs=(vmem,) * 4,
        scratch_shapes=scratch,
        compiler_params=pltpu.CompilerParams(
            collective_id=0, has_side_effects=True, vmem_limit_bytes=60 * 1024 * 1024
        ),
    )(
        past.reshape(users * hist, depth), cand, wu, wi, scale.reshape(1, 1), shift.reshape(1, 1),
        ids.reshape(1, users), slots.reshape(1, users),
    )
    return pl.pallas_call(
        hand_out,
        name="hand_out",
        out_shape=(
            jax.ShapeDtypeStruct((1,), F32),
            jax.ShapeDtypeStruct((users, E), F32),
            jax.ShapeDtypeStruct((rows, E), F32),
            jax.ShapeDtypeStruct((rows, E), F32),
        ),
        in_specs=[vmem] * 4,
        out_specs=(smem, vmem, vmem, vmem),
        compiler_params=pltpu.CompilerParams(vmem_limit_bytes=4 * 1024 * 1024),
    )(*outs)


def solution(mesh):
    group = mesh.shape["group"]
    n = {128: 4, 16: 2}[mesh.size]
    both = ("blk", "group")
    return jax.shard_map(
        functools.partial(shards, n, group // n),
        mesh=mesh,
        in_specs=(P(both, None, None), P(both, None), P(), P(), P(), P(), P(both), P(both)),
        out_specs=(P(), P(both, None), P(both, None), P(both, None)),
        check_vma=False,
    )
```

```python
import functools

import jax
import jax.numpy as jnp
from jax import lax
from jax.experimental import pallas as pl
from jax.experimental.pallas import tpu as pltpu
from jax.sharding import PartitionSpec as P

EPS = 1e-06
MESH = pl.DeviceIdType.MESH
F32 = jnp.float32
BF16 = jnp.bfloat16
CORES = 2
COLOURS = 3


def dot(a, b):
    return jnp.dot(a, b, preferred_element_type=F32)


def dot_t(a, b):
    return lax.dot_general(a, b, (((0,), (0,)), ((), ())), preferred_element_type=F32)


def dot_nt(a, b):
    return lax.dot_general(a, b, (((1,), (1,)), ((), ())), preferred_element_type=F32)


def sigmoid(v):
    return 0.5 + 0.5 * jnp.tanh(0.5 * v)


def tower_kernel(
    N, XL, TOTAL,
    x_hbm, ci_hbm, wu_hbm, wi_hbm, scale_ref, shift_ref, ids_ref, slot_ref,
    loss_ref, ig_ref, gu_ref, gi_ref,
    xv, xs, civ, wuv, wiv, pre, pooled, gp, ulen, inorm, ilen,
    ua, ia, idrow, idbuf, slotbuf, tgtbuf, wt, pig, pigf, rigc, rig, pgu, rgu, g, gi, xi, xt,
    part, ra0, ra1, ra2, sa, rb, parti, ri, losses, corelosses, scale_s, shift_s, idv, slotv,
    lsem, xsem_s, xsem_r, xi_s, xi_r, id_s, id_r, slot_s, slot_r, tgt_s, tgt_r,
    ia_s, ia_r, ua_s, ua_r, ig_s, ig_r, ug_s, ug_r, g_s, g_r, gi_s, gi_r,
    ra_s, ra_r, rs_s, rs_r, ri_s, ri_r, lo_s, lo_r, hop_s, hop_r,
):
    USERS, E = pooled.shape
    HIST = xv.shape[0] // USERS
    FEAT = 128 if N == 4 else XL * N * 16
    QN = (N // XL) * N
    NU = XL * N
    NI = XL * N * CORES
    NS = XL * N
    CW = E // COLOURS
    XH = N // XL
    ROWS = USERS * HIST
    blk = lax.axis_index("blk")
    group = lax.axis_index("group")
    c = lax.rem(blk, CORES)
    z = lax.rem(blk // CORES, N)
    x = (blk // (CORES * N)) * XL + group // N
    y = lax.rem(group, N)
    odd = lax.rem(x, 2)
    pair_a = x + 1 - 2 * odd
    pair_b = lax.rem(x + N - 1 + 2 * odd, N)

    def device(px, py, pz, pc):
        return (((px // XL) * N + pz) * CORES + pc, lax.rem(px, XL) * N + py)

    def plus(v, d, n):
        return v if d == 0 else lax.rem(v + d, n)

    def minus(v, d, n):
        return v if d == 0 else lax.rem(v + n - d, n)

    def send(src, dst, ssem, rsem, to):
        copy = pltpu.make_async_remote_copy(
            src_ref=src, dst_ref=dst, send_sem=ssem, recv_sem=rsem, device_id=to, device_id_type=MESH
        )
        copy.start()
        sent.append(copy)
        return copy

    def arrived(dst, sem):
        pltpu.make_async_remote_copy(
            src_ref=dst, dst_ref=dst, send_sem=sem, recv_sem=sem, device_id=sibling, device_id_type=MESH
        ).wait_recv()

    def left(src, sem):
        pltpu.make_async_remote_copy(
            src_ref=src, dst_ref=src, send_sem=sem, recv_sem=sem, device_id=sibling, device_id_type=MESH
        ).wait_send()

    sent = []
    sibling = device(x, y, z, 1 - c)
    def ring(d):
        return min(d, N - d)

    span = range(N)
    user_peers = [(da, dy) for da in range(2) for dy in span if (da, dy) != (0, 0)]
    user_peers.sort(key=lambda p: -p[0] - ring(p[1]))
    near_items = [(db, dz, 0) for db in range(2) for dz in span if (db, dz) != (0, 0)]
    near_items.sort(key=lambda p: -p[0] - ring(p[1]))
    item_peers = near_items + [(db, dz, 1) for db in range(2) for dz in span]
    planes = [(di, dj) for di in span for dj in span if (di, dj) != (0, 0)]
    planes.sort(key=lambda p: -ring(p[0]) - ring(p[1]))
    steps = sorted(range(1, N), key=lambda d: -ring(d))

    def user_peer(da, dy):
        return device(pair_a if da else x, plus(y, dy, N), z, c)

    def user_slot(da, dy):
        return (1 - odd if da else odd) * N + plus(y, dy, N)

    def item_slot(db, dz, dc):
        return dc * NS + db * N + dz

    def item_peer(db, dz, dc):
        return device(pair_b if db else x, y, plus(z, dz, N), plus(c, dc, CORES))

    def item_owner(db, dz, dc):
        return device(pair_b if db else x, y, minus(z, dz, N), plus(c, dc, CORES))

    def row_peer(dx, dy):
        return device(plus(x, dx, N), plus(y, dy, N), z, c)

    small = [
        pltpu.make_async_copy(a, b, lsem.at[4 + n])
        for n, (a, b) in enumerate(((ids_ref, idv), (slot_ref, slotv), (scale_ref, scale_s), (shift_ref, shift_s)))
    ]
    for load in small:
        load.start()
    load_ci = pltpu.make_async_copy(ci_hbm, civ, lsem.at[0])
    load_wi = pltpu.make_async_copy(wi_hbm, wiv, lsem.at[1])
    load_x = pltpu.make_async_copy(x_hbm, xv, lsem.at[2])
    load_wu = pltpu.make_async_copy(wu_hbm, wuv, lsem.at[3])
    for load in (load_ci, load_wi, load_x, load_wu):
        load.start()

    barrier = pltpu.get_barrier_semaphore()
    greeted = [row_peer(*d) for d in planes]
    greeted += [device(plus(x, dx, N), y, plus(z, dz, N), c) for dx in range(N) for dz in range(1, N)]
    greeted += [device(x, plus(y, dy, N), plus(z, dz, N), c) for dy in range(1, N) for dz in range(1, N)]
    greeted += [item_peer(*d) for d in item_peers if d[2]]
    for to in greeted:
        pl.semaphore_signal(barrier, inc=1, device_id=to, device_id_type=MESH)
    for load in small:
        load.wait()
    my_user_slot = user_slot(0, 0)
    rows = lax.broadcasted_iota(jnp.int32, (USERS, USERS), 0)
    lanes = lax.broadcasted_iota(jnp.int32, (USERS, USERS), 1)
    id_col = jnp.sum(jnp.where(rows == lanes, idv[...].astype(F32), 0.0), axis=1, keepdims=True)
    slot_col = jnp.sum(jnp.where(rows == lanes, slotv[...].astype(F32), 0.0), axis=1, keepdims=True)
    tile_rows = lax.broadcasted_iota(jnp.int32, (USERS, 128), 0)
    tile_lanes = lax.broadcasted_iota(jnp.int32, (USERS, 128), 1)
    idrow[0] = jnp.sum(jnp.where(tile_rows == tile_lanes, id_col, 0.0), axis=0, keepdims=True)
    wide_rows = lax.broadcasted_iota(jnp.int32, (USERS, NU * USERS), 0)
    wide_lanes = lax.broadcasted_iota(jnp.int32, (USERS, NU * USERS), 1)
    slotbuf[0] = jnp.sum(
        jnp.where(wide_lanes == wide_rows + my_user_slot * USERS, slot_col, 0.0), axis=0, keepdims=True
    )
    load_ci.wait()
    load_wi.wait()
    item_pre = dot(civ[...], wiv[...])
    item_len = jnp.sqrt(jnp.sum(item_pre * item_pre, axis=1, keepdims=True) + EPS)
    item_normed = item_pre / item_len
    inorm[...] = item_normed
    ilen[...] = jnp.broadcast_to(item_len, (USERS, 128))
    ia[0, 0] = item_normed.astype(BF16)
    pl.semaphore_wait(barrier, len(greeted))
    id_recv, slot_recv = [], []
    for n, d in enumerate(user_peers):
        slot_recv.append(send(slotbuf.at[0], slotbuf.at[n + 1], slot_s.at[n], slot_r.at[n], user_peer(*d)))
    for n, d in enumerate(item_peers):
        id_recv.append(send(idrow.at[0], idrow.at[item_slot(*d)], id_s.at[n], id_r.at[n], item_peer(*d)))
    ia_recv = []
    for n, d in enumerate(near_items):
        ia_recv.append(send(ia.at[0, 0], ia.at[0, item_slot(*d)], ia_s.at[n], ia_r.at[n], item_peer(*d)))
    load_x.wait()
    x_recv = []
    for q in range(QN):
        cols = pl.ds(pl.multiple_of((q * CORES + 1 - c) * FEAT, FEAT), FEAT)
        x_recv.append(send(xv.at[:, cols], xs.at[q], xsem_s.at[q], xsem_r.at[q], sibling))
    load_wu.wait()

    def forward(n, _):
        cols = pl.ds(pl.multiple_of(n * 256, 256), 256)
        pre[:, cols] = dot(xv[...], wuv[:, cols])
        return 0

    lax.fori_loop(0, E // 256, forward, 0)

    for copy in slot_recv + id_recv:
        copy.wait_recv()
    slots = slotbuf[0]
    for n in range(1, NU):
        slots = slots + slotbuf[n]
    wide = NU * USERS // 128
    found = jnp.zeros((1, NU * USERS), F32)
    for dc in range(CORES):
        for db in range(2):
            for dz in range(N):
                s = item_slot(db, dz, dc)
                col = jnp.sum(jnp.where(tile_rows == tile_lanes, idrow[s], 0.0), axis=1, keepdims=True)
                ids = jnp.broadcast_to(col, (USERS, 128))
                idbuf[s] = ids
                ob, og = item_owner(db, dz, dc)
                at = (tile_rows + (ob * (XL * N) + og) * USERS).astype(F32)
                hit = jnp.concatenate([at] * wide, axis=1) == slots
                found = found + jnp.sum(
                    jnp.where(hit, jnp.concatenate([ids] * wide, axis=1), 0.0), axis=0, keepdims=True
                )
    tgtbuf[0] = found
    tgt_recv = []
    for n, d in enumerate(user_peers):
        tgt_recv.append(send(tgtbuf.at[0], tgtbuf.at[n + 1], tgt_s.at[n], tgt_r.at[n], user_peer(*d)))

    def pool(n, _):
        u = n // COLOURS
        cols = pl.ds(pl.multiple_of(lax.rem(n, COLOURS) * CW, CW), CW)
        v = pre[pl.ds(pl.multiple_of(u * 8 * HIST, 8 * HIST), 8 * HIST), cols]
        act = v * sigmoid(v)
        pooled[pl.ds(pl.multiple_of(u * 8, 8), 8), cols] = jnp.sum(act.reshape(8, HIST, CW), axis=1) / HIST
        return 0

    lax.fori_loop(0, (USERS // 8) * COLOURS, pool, 0)
    mean = pooled[...]
    user_len = jnp.sqrt(jnp.sum(mean * mean, axis=1, keepdims=True) + EPS)
    user_normed = mean / user_len
    ulen[...] = jnp.broadcast_to(user_len, (USERS, 128))
    pooled[...] = user_normed
    ua[my_user_slot] = user_normed.astype(BF16)
    ua_recv = []
    for n, d in enumerate(user_peers):
        ua_recv.append(send(ua.at[my_user_slot], ua.at[my_user_slot], ua_s.at[n], ua_r.at[n], user_peer(*d)))

    xi_recv = []
    for n, (db, dz, dc) in enumerate(item_peers):
        px, pz, pc = pair_b if db else x, plus(z, dz, N), plus(c, dc, CORES)
        cols = pl.ds(pl.multiple_of(((px // XL * N + pz) * CORES + pc) * FEAT, FEAT), FEAT)
        xi_recv.append(
            send(civ.at[:, cols], xi.at[item_slot(db, dz, dc)], xi_s.at[n], xi_r.at[n], item_peer(db, dz, dc))
        )
    xi[0] = civ[:, pl.ds(pl.multiple_of(((x // XL * N + z) * CORES + c) * FEAT, FEAT), FEAT)]
    for copy in ia_recv:
        copy.wait_recv()
    ia_hop = send(ia.at[0], ia.at[1], hop_s.at[0], hop_r.at[0], sibling)
    for copy in x_recv:
        copy.wait_recv()

    def turn(q, _):
        cols = pl.ds(pl.multiple_of((q * CORES + c) * FEAT, FEAT), FEAT)
        to = pl.ds(pl.multiple_of(q * FEAT, FEAT), FEAT)
        xt[to, 0:ROWS] = xv[:, cols].T
        xt[to, ROWS:2 * ROWS] = xs[q].T
        return 0

    lax.fori_loop(0, QN, turn, 0)
    for copy in tgt_recv:
        copy.wait_recv()
    targets = tgtbuf[0]
    for n in range(1, NU):
        targets = targets + tgtbuf[n]

    for copy in ua_recv:
        copy.wait_recv()
    ia_hop.wait_recv()
    scale = scale_s[0, 0]
    shift = shift_s[0, 0]
    users = ua[...].reshape(NU * USERS, E)
    loss = jnp.zeros((8, 128), F32)
    for n in range(NI // N):
        items = ia[n // 2, (n % 2) * N:(n % 2 + 1) * N].reshape(N * USERS, E)
        scores = dot_nt(items, users)
        ids = idbuf[n * N:(n + 1) * N].reshape(N * USERS, 128)
        sign = jnp.where(jnp.concatenate([ids] * wide, axis=1) == targets, 1.0, -1.0)
        margin = sign * (scale * scores + shift)
        e = jnp.exp(-jnp.abs(margin))
        terms = jnp.log1p(e) + jnp.maximum(-margin, 0.0)
        gate = jnp.where(margin >= 0.0, e, 1.0) / (1.0 + e)
        wt[n * N * USERS:(n + 1) * N * USERS, :] = (-scale * sign * gate).astype(BF16)
        terms = jnp.sum(terms.reshape(N * USERS // 8, 8, NU * USERS), axis=0)
        for j in range(wide):
            loss = loss + terms[:, j * 128:(j + 1) * 128]
    def reduce_loss(value, step, pos):
        losses[step, pos] = value
        copies = []
        for d in range(1, N):
            at = [x, y, z]
            at[step] = plus(pos, d, N)
            copies.append(
                send(losses.at[step, pos], losses.at[step, pos], lo_s.at[step, d - 1], lo_r.at[step, d - 1],
                     device(at[0], at[1], at[2], c))
            )
        return copies

    def reduced_loss(step):
        total = losses[step, 0]
        for d in range(1, N):
            total = total + losses[step, d]
        return total

    loss_copies = reduce_loss(loss, 0, x)
    pgu[...] = dot_t(wt[...], ia[...].reshape(NI * USERS, E)).astype(BF16).reshape(NU, USERS, E)
    ug_recv = []
    for n, d in enumerate(user_peers):
        ug_recv.append(send(pgu.at[user_slot(*d)], rgu.at[n], ug_s.at[n], ug_r.at[n], user_peer(*d)))
    pig[1] = dot(wt[NS * USERS:2 * NS * USERS, :], users).astype(BF16).reshape(NS, USERS, E)
    ig_hop = send(pig.at[1], rigc, hop_s.at[1], hop_r.at[1], sibling)
    pigf[...] = dot(wt[0:NS * USERS, :], users).reshape(NS, USERS, E)
    ig_hop.wait_recv()
    ig_recv = []
    for s in range(NS):
        pigf[s] = pigf[s] + rigc[s].astype(F32)
        if s > 0:
            pig[0, s] = pigf[s].astype(BF16)
    for n, d in enumerate(near_items):
        ig_recv.append(send(pig.at[0, item_slot(*d)], rig.at[n], ig_s.at[n], ig_r.at[n], item_owner(*d)))

    for copy in ug_recv:
        copy.wait_recv()
    grad_users = pgu[my_user_slot].astype(F32)
    for n in range(len(user_peers)):
        grad_users = grad_users + rgu[n].astype(F32)
    user_normed = pooled[...]
    radial = jnp.sum(user_normed * grad_users, axis=1, keepdims=True)
    gp[...] = (grad_users - user_normed * radial) / ulen[:, 0:1] / HIST

    pos = (x, y, z)

    def backward(m, _):
        k = jnp.where(m < 2, 1 - m, m)
        cols = pl.ds(pl.multiple_of(k * CW, CW), CW)

        def step(u, _):
            at = pl.ds(pl.multiple_of(u * 8 * HIST, 8 * HIST), 8 * HIST)
            v = pre[at, cols]
            s = sigmoid(v)
            outer = jnp.broadcast_to(gp[pl.ds(pl.multiple_of(u * 8, 8), 8), cols][:, None, :], (8, HIST, CW))
            g[k, at] = (outer.reshape(8 * HIST, CW) * s * (1.0 + v * (1.0 - s))).astype(BF16)
            return 0

        lax.fori_loop(0, USERS // 8, step, 0)
        pltpu.make_async_remote_copy(
            src_ref=g.at[k, pl.ds(0, ROWS)], dst_ref=g.at[k, pl.ds(ROWS, ROWS)], send_sem=g_s.at[k],
            recv_sem=g_r.at[k], device_id=sibling, device_id_type=MESH,
        ).start()
        return 0

    def towards(axis, v):
        at = list(pos)
        at[axis] = v
        return device(at[0], at[1], at[2], c)

    def item_home():
        for copy in ig_recv:
            copy.wait_recv()
        item_grad = pigf[0]
        for n in range(len(near_items)):
            item_grad = item_grad + rig[n].astype(F32)
        ig_ref[...] = item_grad
        item_normed = inorm[...]
        radial = jnp.sum(item_normed * item_grad, axis=1, keepdims=True)
        gi[0, 0] = ((item_grad - item_normed * radial) / ilen[:, 0:1]).astype(BF16)
        for n, d in enumerate(near_items):
            pltpu.make_async_remote_copy(
                src_ref=gi.at[0, 0], dst_ref=gi.at[0, item_slot(*d)], send_sem=gi_s.at[n], recv_sem=gi_r.at[n],
                device_id=item_peer(*d), device_id_type=MESH,
            ).start()

    def weight_grad(m, _):
        k = jnp.where(m < 2, 1 - m, m)
        pl.when(m == 1)(item_home)
        arrived(g.at[k, pl.ds(ROWS, ROWS)], g_r.at[k])
        part[k] = dot(xt[...], g[k]).astype(BF16).reshape(XH, N, XL, N, 16, CW)
        for axis in range(COLOURS):

            @pl.when(k == axis)
            def _(axis=axis):
                for d in steps:
                    t = plus(pos[axis], d, N)
                    pltpu.make_async_remote_copy(
                        src_ref=slab(axis, t), dst_ref=ra[axis].at[d - 1], send_sem=ra_s.at[axis, d - 1],
                        recv_sem=ra_r.at[axis, d - 1], device_id=towards(axis, t), device_id_type=MESH,
                    ).start()

        return 0

    ra = (ra0, ra1, ra2)

    def slab(axis, t):
        if axis == 0:
            return part.at[0, t // XL, :, lax.rem(t, XL)]
        if axis == 1:
            return part.at[1, :, :, :, t]
        return part.at[2, :, t]

    lax.fori_loop(0, COLOURS, backward, 0)
    for copy in loss_copies:
        copy.wait_recv()
    loss_copies = reduce_loss(reduced_loss(0), 1, y)
    lax.fori_loop(0, COLOURS, weight_grad, 0)
    for copy in loss_copies:
        copy.wait_recv()
    loss_copies = reduce_loss(reduced_loss(1), 2, z)
    flight = {}

    def add_a(k):
        for d in range(N - 1):
            arrived(ra[k].at[d], ra_r.at[k, d])
        p1, p2 = pos[(k + 1) % 3], pos[(k + 2) % 3]
        flight[k] = []
        for n, (di, dj) in enumerate(planes + [(0, 0)]):
            i, j = plus(p1, di, N), plus(p2, dj, N)
            if k == 0:
                own, got = part.at[0, x // XL, j, lax.rem(x, XL), i], lambda d: ra0[d, j, i]
            elif k == 1:
                own, got = part.at[1, j // XL, i, lax.rem(j, XL), y], lambda d: ra1[d, j // XL, i, lax.rem(j, XL)]
            else:
                own, got = part.at[2, i // XL, z, lax.rem(i, XL), j], lambda d: ra2[d, i // XL, lax.rem(i, XL), j]
            total = own[...].astype(F32)
            for d in range(N - 1):
                total = total + got(d).astype(F32)
            sa[k, n] = total.astype(BF16)
            if (di, dj) != (0, 0):
                at = list(pos)
                at[(k + 1) % 3], at[(k + 2) % 3] = i, j
                to = device(at[0], at[1], at[2], c)
                flight[k].append(send(sa.at[k, n], rb.at[k, n], rs_s.at[k, n], rs_r.at[k, n], to))

    def add_b(k):
        for copy in flight[k]:
            copy.wait_recv()
        total = sa[k, len(planes)].astype(F32)
        for n in range(len(planes)):
            total = total + rb[k, n].astype(F32)
        gu_ref[:, k * CW:(k + 1) * CW] = total

    add_a(1)
    for n, d in enumerate(near_items):
        arrived(gi.at[0, item_slot(*d)], gi_r.at[n])
    gi_hop = send(gi.at[0], gi.at[1], hop_s.at[2], hop_r.at[2], sibling)
    for copy in xi_recv:
        copy.wait_recv()
    gi_hop.wait_recv()
    r = dot_t(xi[...].reshape(NI * USERS, FEAT), gi[...].reshape(NI * USERS, E)).astype(BF16)
    parti[...] = r.reshape(NU, 16, E)
    ri_recv = []
    for n, d in enumerate(user_peers):
        ri_recv.append(send(parti.at[user_slot(*d)], ri.at[n], ri_s.at[n], ri_r.at[n], user_peer(*d)))
    add_a(0)
    add_a(2)
    for copy in loss_copies:
        copy.wait_recv()
    corelosses[c] = reduced_loss(2)
    core_copy = send(corelosses.at[c], corelosses.at[c], hop_s.at[3], hop_r.at[3], sibling)
    for copy in sent:
        copy.wait_send()
    for k in range(COLOURS):
        left(g.at[k, pl.ds(0, ROWS)], g_s.at[k])
        for d in range(N - 1):
            left(ra[k].at[d], ra_s.at[k, d])
    for n in range(len(near_items)):
        left(gi.at[0, 0], gi_s.at[n])
    add_b(1)
    add_b(0)
    core_copy.wait_recv()
    loss_ref[...] = jnp.broadcast_to(jnp.sum(corelosses[0] + corelosses[1], keepdims=True) / TOTAL, (8, 128))
    for copy in ri_recv:
        copy.wait_recv()
    total = parti[my_user_slot].astype(F32)
    for n in range(len(user_peers)):
        total = total + ri[n].astype(F32)
    gi_ref[...] = total
    add_b(2)


def hand_out(loss, ig, gu, gi, loss_out, ig_out, gu_out, gi_out):
    loss_out[0] = loss[0, 0]
    ig_out[...] = ig[...]
    gu_out[...] = gu[...]
    gi_out[...] = gi[...]


def shards(N, XL, past, cand, wu, wi, scale, shift, ids, slots):
    users, hist, depth = past.shape
    E = wu.shape[1]
    total = users * lax.axis_size("blk") * lax.axis_size("group")
    NU, NI, NS, QN = XL * N, XL * N * CORES, XL * N, (N // XL) * N
    feat = depth // (QN * CORES)
    hbm = pl.BlockSpec(memory_space=pltpu.HBM)
    smem = pl.BlockSpec(memory_space=pltpu.SMEM)
    vmem = pl.BlockSpec(memory_space=pltpu.VMEM)
    rows = depth // (N * N * N * CORES)
    CW = E // COLOURS

    def dma(*shape):
        return pltpu.SemaphoreType.DMA(shape)

    V = pltpu.VMEM
    scratch = [
        V((users * hist, depth), BF16), V((QN, users * hist, feat), BF16),
        V((users, depth), BF16),
        V((depth, E), BF16), V((depth, E), BF16),
        V((users * hist, E), F32), V((users, E), F32), V((users, E), F32), V((users, 128), F32),
        V((users, E), F32), V((users, 128), F32),
        V((NU, users, E), BF16), V((CORES, NS, users, E), BF16), V((NI, 1, 128), F32), V((NI, users, 128), F32),
        V((NU, 1, NU * users), F32), V((NU, 1, NU * users), F32),
        V((NI * users, NU * users), BF16),
        V((CORES, NS, users, E), BF16), V((NS, users, E), F32), V((NS, users, E), BF16),
        V((NS - 1, users, E), BF16),
        V((NU, users, E), BF16), V((NU - 1, users, E), BF16),
        V((COLOURS, 2 * users * hist, CW), BF16), V((CORES, NS, users, E), BF16),
        V((NI, users, feat), BF16), V((QN * feat, 2 * users * hist), BF16),
        V((COLOURS, N // XL, N, XL, N, rows, CW), BF16), V((N - 1, N, N, rows, CW), BF16),
        V((N - 1, N // XL, N, XL, rows, CW), BF16), V((N - 1, N // XL, XL, N, rows, CW), BF16),
        V((COLOURS, N * N, rows, CW), BF16), V((COLOURS, N * N - 1, rows, CW), BF16),
        V((NU, rows, E), BF16), V((NU - 1, rows, E), BF16),
        V((3, N, 8, 128), F32), V((CORES, 8, 128), F32),
        V((1, 1), F32), V((1, 1), F32), V((1, users), jnp.int32), V((1, users), jnp.int32),
        dma(8), dma(QN), dma(QN), dma(NI - 1), dma(NI - 1),
        dma(NI - 1), dma(NI - 1), dma(NU - 1), dma(NU - 1), dma(NU - 1), dma(NU - 1),
        dma(NS - 1), dma(NS - 1), dma(NU - 1), dma(NU - 1),
        dma(NS - 1), dma(NS - 1), dma(NU - 1), dma(NU - 1), dma(COLOURS), dma(COLOURS), dma(NS - 1), dma(NS - 1),
        dma(COLOURS, N - 1), dma(COLOURS, N - 1), dma(COLOURS, N * N - 1), dma(COLOURS, N * N - 1),
        dma(NU - 1), dma(NU - 1), dma(3, N - 1), dma(3, N - 1), dma(4), dma(4),
    ]
    outs = pl.pallas_call(
        functools.partial(tower_kernel, N, XL, total),
        name="two_tower",
        out_shape=(
            pltpu.VMEM((8, 128), F32),
            pltpu.VMEM((users, E), F32),
            pltpu.VMEM((rows, E), F32),
            pltpu.VMEM((rows, E), F32),
        ),
        in_specs=[hbm] * 8,
        out_specs=(vmem,) * 4,
        scratch_shapes=scratch,
        compiler_params=pltpu.CompilerParams(
            collective_id=0, has_side_effects=True, vmem_limit_bytes=60 * 1024 * 1024
        ),
    )(
        past.reshape(users * hist, depth), cand, wu, wi, scale.reshape(1, 1), shift.reshape(1, 1),
        ids.reshape(1, users), slots.reshape(1, users),
    )
    return pl.pallas_call(
        hand_out,
        name="hand_out",
        out_shape=(
            jax.ShapeDtypeStruct((1,), F32),
            jax.ShapeDtypeStruct((users, E), F32),
            jax.ShapeDtypeStruct((rows, E), F32),
            jax.ShapeDtypeStruct((rows, E), F32),
        ),
        in_specs=[vmem] * 4,
        out_specs=(smem, vmem, vmem, vmem),
        compiler_params=pltpu.CompilerParams(vmem_limit_bytes=4 * 1024 * 1024),
    )(*outs)


def solution(mesh):
    group = mesh.shape["group"]
    n = {128: 4, 16: 2}[mesh.size]
    both = ("blk", "group")
    return jax.shard_map(
        functools.partial(shards, n, group // n),
        mesh=mesh,
        in_specs=(P(both, None, None), P(both, None), P(), P(), P(), P(), P(both), P(both)),
        out_specs=(P(), P(both, None), P(both, None), P(both, None)),
        check_vma=False,
    )
```

```python
import functools

import jax
import jax.numpy as jnp
from jax import lax
from jax.experimental import pallas as pl
from jax.experimental.pallas import tpu as pltpu
from jax.sharding import PartitionSpec as P

EPS = 1e-06
MESH = pl.DeviceIdType.MESH
F32 = jnp.float32
BF16 = jnp.bfloat16
CORES = 2
COLOURS = 3


def dot(a, b):
    return jnp.dot(a, b, preferred_element_type=F32)


def dot_t(a, b):
    return lax.dot_general(a, b, (((0,), (0,)), ((), ())), preferred_element_type=F32)


def dot_nt(a, b):
    return lax.dot_general(a, b, (((1,), (1,)), ((), ())), preferred_element_type=F32)


def sigmoid(v):
    return 0.5 + 0.5 * jnp.tanh(0.5 * v)


def tower_kernel(
    N, XL, TOTAL,
    x_hbm, ci_hbm, wu_hbm, wi_hbm, scale_ref, shift_ref, ids_ref, slot_ref,
    loss_ref, ig_ref, gu_ref, gi_ref,
    xv, xs, civ, wuv, wiv, pre, pooled, gp, ulen, inorm, ilen,
    ua, ia, idrow, idbuf, slotbuf, tgtbuf, wt, pig, pigf, rigc, rig, pgu, rgu, g, gi, xi, xt,
    part, ra0, ra1, ra2, sa, rb, parti, ri, losses, corelosses, scale_s, shift_s, idv, slotv,
    lsem, xsem_s, xsem_r, xi_s, xi_r, id_s, id_r, slot_s, slot_r, tgt_s, tgt_r,
    ia_s, ia_r, ua_s, ua_r, ig_s, ig_r, ug_s, ug_r, g_s, g_r, gi_s, gi_r, gh_s, gh_r,
    ra_s, ra_r, rs_s, rs_r, ri_s, ri_r, lo_s, lo_r, hop_s, hop_r,
):
    USERS, E = pooled.shape
    HIST = xv.shape[0] // USERS
    FEAT = 128 if N == 4 else XL * N * 16
    QN = (N // XL) * N
    NU = XL * N
    NI = XL * N * CORES
    NS = XL * N
    CW = E // COLOURS
    XH = N // XL
    ROWS = USERS * HIST
    blk = lax.axis_index("blk")
    group = lax.axis_index("group")
    c = lax.rem(blk, CORES)
    z = lax.rem(blk // CORES, N)
    x = (blk // (CORES * N)) * XL + group // N
    y = lax.rem(group, N)
    odd = lax.rem(x, 2)
    pair_a = x + 1 - 2 * odd
    pair_b = lax.rem(x + N - 1 + 2 * odd, N)

    def device(px, py, pz, pc):
        return (((px // XL) * N + pz) * CORES + pc, lax.rem(px, XL) * N + py)

    def plus(v, d, n):
        return v if d == 0 else lax.rem(v + d, n)

    def minus(v, d, n):
        return v if d == 0 else lax.rem(v + n - d, n)

    def send(src, dst, ssem, rsem, to):
        copy = pltpu.make_async_remote_copy(
            src_ref=src, dst_ref=dst, send_sem=ssem, recv_sem=rsem, device_id=to, device_id_type=MESH
        )
        copy.start()
        sent.append(copy)
        return copy

    def arrived(dst, sem):
        pltpu.make_async_remote_copy(
            src_ref=dst, dst_ref=dst, send_sem=sem, recv_sem=sem, device_id=sibling, device_id_type=MESH
        ).wait_recv()

    def left(src, sem):
        pltpu.make_async_remote_copy(
            src_ref=src, dst_ref=src, send_sem=sem, recv_sem=sem, device_id=sibling, device_id_type=MESH
        ).wait_send()

    sent = []
    sibling = device(x, y, z, 1 - c)
    def ring(d):
        return min(d, N - d)

    span = range(N)
    user_peers = [(da, dy) for da in range(2) for dy in span if (da, dy) != (0, 0)]
    user_peers.sort(key=lambda p: -p[0] - ring(p[1]))
    near_items = [(db, dz, 0) for db in range(2) for dz in span if (db, dz) != (0, 0)]
    near_items.sort(key=lambda p: -p[0] - ring(p[1]))
    item_peers = near_items + [(db, dz, 1) for db in range(2) for dz in span]
    planes = [(di, dj) for di in span for dj in span if (di, dj) != (0, 0)]
    planes.sort(key=lambda p: -ring(p[0]) - ring(p[1]))
    feat_peers = [(dz, dc) for dc in range(CORES) for dz in span if (dz, dc) != (0, 0)]
    steps = sorted(range(1, N), key=lambda d: -ring(d))

    def user_peer(da, dy):
        return device(pair_a if da else x, plus(y, dy, N), z, c)

    def user_slot(da, dy):
        return (1 - odd if da else odd) * N + plus(y, dy, N)

    def item_slot(db, dz, dc):
        return dc * NS + db * N + dz

    def item_peer(db, dz, dc):
        return device(pair_b if db else x, y, plus(z, dz, N), plus(c, dc, CORES))

    def item_owner(db, dz, dc):
        return device(pair_b if db else x, y, minus(z, dz, N), plus(c, dc, CORES))

    def row_peer(dx, dy):
        return device(plus(x, dx, N), plus(y, dy, N), z, c)

    small = [
        pltpu.make_async_copy(a, b, lsem.at[4 + n])
        for n, (a, b) in enumerate(((ids_ref, idv), (slot_ref, slotv), (scale_ref, scale_s), (shift_ref, shift_s)))
    ]
    for load in small:
        load.start()
    load_ci = pltpu.make_async_copy(ci_hbm, civ, lsem.at[0])
    load_wi = pltpu.make_async_copy(wi_hbm, wiv, lsem.at[1])
    load_x = pltpu.make_async_copy(x_hbm, xv, lsem.at[2])
    load_wu = pltpu.make_async_copy(wu_hbm, wuv, lsem.at[3])
    for load in (load_ci, load_wi, load_x, load_wu):
        load.start()

    barrier = pltpu.get_barrier_semaphore()
    greeted = [row_peer(*d) for d in planes]
    greeted += [device(plus(x, dx, N), y, plus(z, dz, N), c) for dx in range(N) for dz in range(1, N)]
    greeted += [device(x, plus(y, dy, N), plus(z, dz, N), c) for dy in range(1, N) for dz in range(1, N)]
    greeted += [item_peer(*d) for d in item_peers if d[2]]
    for to in greeted:
        pl.semaphore_signal(barrier, inc=1, device_id=to, device_id_type=MESH)
    for load in small:
        load.wait()
    my_user_slot = user_slot(0, 0)
    rows = lax.broadcasted_iota(jnp.int32, (USERS, USERS), 0)
    lanes = lax.broadcasted_iota(jnp.int32, (USERS, USERS), 1)
    id_col = jnp.sum(jnp.where(rows == lanes, idv[...].astype(F32), 0.0), axis=1, keepdims=True)
    slot_col = jnp.sum(jnp.where(rows == lanes, slotv[...].astype(F32), 0.0), axis=1, keepdims=True)
    tile_rows = lax.broadcasted_iota(jnp.int32, (USERS, 128), 0)
    tile_lanes = lax.broadcasted_iota(jnp.int32, (USERS, 128), 1)
    idrow[0] = jnp.sum(jnp.where(tile_rows == tile_lanes, id_col, 0.0), axis=0, keepdims=True)
    wide_rows = lax.broadcasted_iota(jnp.int32, (USERS, NU * USERS), 0)
    wide_lanes = lax.broadcasted_iota(jnp.int32, (USERS, NU * USERS), 1)
    slotbuf[0] = jnp.sum(
        jnp.where(wide_lanes == wide_rows + my_user_slot * USERS, slot_col, 0.0), axis=0, keepdims=True
    )
    load_ci.wait()
    load_wi.wait()
    item_pre = dot(civ[...], wiv[...])
    item_len = jnp.sqrt(jnp.sum(item_pre * item_pre, axis=1, keepdims=True) + EPS)
    item_normed = item_pre / item_len
    inorm[...] = item_normed
    ilen[...] = jnp.broadcast_to(item_len, (USERS, 128))
    ia[0, 0] = item_normed.astype(BF16)
    pl.semaphore_wait(barrier, len(greeted))
    id_recv, slot_recv = [], []
    for n, d in enumerate(user_peers):
        slot_recv.append(send(slotbuf.at[0], slotbuf.at[n + 1], slot_s.at[n], slot_r.at[n], user_peer(*d)))
    for n, d in enumerate(item_peers):
        id_recv.append(send(idrow.at[0], idrow.at[item_slot(*d)], id_s.at[n], id_r.at[n], item_peer(*d)))
    ia_recv = []
    for n, d in enumerate(near_items):
        ia_recv.append(send(ia.at[0, 0], ia.at[0, item_slot(*d)], ia_s.at[n], ia_r.at[n], item_peer(*d)))
    load_x.wait()
    x_recv = []
    for q in range(QN):
        cols = pl.ds(pl.multiple_of((q * CORES + 1 - c) * FEAT, FEAT), FEAT)
        x_recv.append(send(xv.at[:, cols], xs.at[q], xsem_s.at[q], xsem_r.at[q], sibling))
    load_wu.wait()

    def forward(n, _):
        cols = pl.ds(pl.multiple_of(n * 256, 256), 256)
        pre[:, cols] = dot(xv[...], wuv[:, cols])
        return 0

    lax.fori_loop(0, E // 256, forward, 0)

    for copy in slot_recv + id_recv:
        copy.wait_recv()
    slots = slotbuf[0]
    for n in range(1, NU):
        slots = slots + slotbuf[n]
    wide = NU * USERS // 128
    found = jnp.zeros((1, NU * USERS), F32)
    for dc in range(CORES):
        for db in range(2):
            for dz in range(N):
                s = item_slot(db, dz, dc)
                col = jnp.sum(jnp.where(tile_rows == tile_lanes, idrow[s], 0.0), axis=1, keepdims=True)
                ids = jnp.broadcast_to(col, (USERS, 128))
                idbuf[s] = ids
                ob, og = item_owner(db, dz, dc)
                at = (tile_rows + (ob * (XL * N) + og) * USERS).astype(F32)
                hit = jnp.concatenate([at] * wide, axis=1) == slots
                found = found + jnp.sum(
                    jnp.where(hit, jnp.concatenate([ids] * wide, axis=1), 0.0), axis=0, keepdims=True
                )
    tgtbuf[0] = found
    tgt_recv = []
    for n, d in enumerate(user_peers):
        tgt_recv.append(send(tgtbuf.at[0], tgtbuf.at[n + 1], tgt_s.at[n], tgt_r.at[n], user_peer(*d)))

    def pool(n, _):
        u = n // COLOURS
        cols = pl.ds(pl.multiple_of(lax.rem(n, COLOURS) * CW, CW), CW)
        v = pre[pl.ds(pl.multiple_of(u * 8 * HIST, 8 * HIST), 8 * HIST), cols]
        act = v * sigmoid(v)
        pooled[pl.ds(pl.multiple_of(u * 8, 8), 8), cols] = jnp.sum(act.reshape(8, HIST, CW), axis=1) / HIST
        return 0

    lax.fori_loop(0, (USERS // 8) * COLOURS, pool, 0)
    mean = pooled[...]
    user_len = jnp.sqrt(jnp.sum(mean * mean, axis=1, keepdims=True) + EPS)
    user_normed = mean / user_len
    ulen[...] = jnp.broadcast_to(user_len, (USERS, 128))
    pooled[...] = user_normed
    ua[my_user_slot] = user_normed.astype(BF16)
    ua_recv = []
    for n, d in enumerate(user_peers):
        ua_recv.append(send(ua.at[my_user_slot], ua.at[my_user_slot], ua_s.at[n], ua_r.at[n], user_peer(*d)))

    xi_recv = []
    for n, (dz, dc) in enumerate(feat_peers):
        pz, pc = plus(z, dz, N), plus(c, dc, CORES)
        for h in range(XH):
            cols = pl.ds(pl.multiple_of(((h * N + pz) * CORES + pc) * FEAT, FEAT), FEAT)
            xi_recv.append(
                send(civ.at[:, cols], xi.at[h, dc * N + dz], xi_s.at[n, h], xi_r.at[n, h], item_peer(0, dz, dc))
            )
    for h in range(XH):
        xi[h, 0] = civ[:, pl.ds(pl.multiple_of(((h * N + z) * CORES + c) * FEAT, FEAT), FEAT)]
    for copy in ia_recv:
        copy.wait_recv()
    ia_hop = send(ia.at[0], ia.at[1], hop_s.at[0], hop_r.at[0], sibling)
    for copy in x_recv:
        copy.wait_recv()

    def turn(q, _):
        cols = pl.ds(pl.multiple_of((q * CORES + c) * FEAT, FEAT), FEAT)
        to = pl.ds(pl.multiple_of(q * FEAT, FEAT), FEAT)
        xt[to, 0:ROWS] = xv[:, cols].T
        xt[to, ROWS:2 * ROWS] = xs[q].T
        return 0

    lax.fori_loop(0, QN, turn, 0)
    for copy in tgt_recv:
        copy.wait_recv()
    targets = tgtbuf[0]
    for n in range(1, NU):
        targets = targets + tgtbuf[n]

    for copy in ua_recv:
        copy.wait_recv()
    ia_hop.wait_recv()
    scale = scale_s[0, 0]
    shift = shift_s[0, 0]
    users = ua[...].reshape(NU * USERS, E)
    loss = jnp.zeros((8, 128), F32)
    for n in range(NI // N):
        items = ia[n // 2, (n % 2) * N:(n % 2 + 1) * N].reshape(N * USERS, E)
        scores = dot_nt(items, users)
        ids = idbuf[n * N:(n + 1) * N].reshape(N * USERS, 128)
        sign = jnp.where(jnp.concatenate([ids] * wide, axis=1) == targets, 1.0, -1.0)
        margin = sign * (scale * scores + shift)
        e = jnp.exp(-jnp.abs(margin))
        terms = jnp.log1p(e) + jnp.maximum(-margin, 0.0)
        gate = jnp.where(margin >= 0.0, e, 1.0) / (1.0 + e)
        wt[n * N * USERS:(n + 1) * N * USERS, :] = (-scale * sign * gate).astype(BF16)
        terms = jnp.sum(terms.reshape(N * USERS // 8, 8, NU * USERS), axis=0)
        for j in range(wide):
            loss = loss + terms[:, j * 128:(j + 1) * 128]
    def reduce_loss(value, step, pos):
        losses[step, pos] = value
        copies = []
        for d in range(1, N):
            at = [x, y, z]
            at[step] = plus(pos, d, N)
            copies.append(
                send(losses.at[step, pos], losses.at[step, pos], lo_s.at[step, d - 1], lo_r.at[step, d - 1],
                     device(at[0], at[1], at[2], c))
            )
        return copies

    def reduced_loss(step):
        total = losses[step, 0]
        for d in range(1, N):
            total = total + losses[step, d]
        return total

    loss_copies = reduce_loss(loss, 0, x)
    pgu[...] = dot_t(wt[...], ia[...].reshape(NI * USERS, E)).astype(BF16).reshape(NU, USERS, E)
    ug_recv = []
    for n, d in enumerate(user_peers):
        ug_recv.append(send(pgu.at[user_slot(*d)], rgu.at[n], ug_s.at[n], ug_r.at[n], user_peer(*d)))
    pig[1] = dot(wt[NS * USERS:2 * NS * USERS, :], users).astype(BF16).reshape(NS, USERS, E)
    ig_hop = send(pig.at[1], rigc, hop_s.at[1], hop_r.at[1], sibling)
    pigf[...] = dot(wt[0:NS * USERS, :], users).reshape(NS, USERS, E)
    ig_hop.wait_recv()
    ig_recv = []
    for s in range(NS):
        pigf[s] = pigf[s] + rigc[s].astype(F32)
        if s > 0:
            pig[0, s] = pigf[s].astype(BF16)
    for n, d in enumerate(near_items):
        ig_recv.append(send(pig.at[0, item_slot(*d)], rig.at[n], ig_s.at[n], ig_r.at[n], item_owner(*d)))

    for copy in ug_recv:
        copy.wait_recv()
    grad_users = pgu[my_user_slot].astype(F32)
    for n in range(len(user_peers)):
        grad_users = grad_users + rgu[n].astype(F32)
    user_normed = pooled[...]
    radial = jnp.sum(user_normed * grad_users, axis=1, keepdims=True)
    gp[...] = (grad_users - user_normed * radial) / ulen[:, 0:1] / HIST

    pos = (x, y, z)

    def backward(m, _):
        k = jnp.where(m < 2, 1 - m, m)
        cols = pl.ds(pl.multiple_of(k * CW, CW), CW)

        def step(u, _):
            at = pl.ds(pl.multiple_of(u * 8 * HIST, 8 * HIST), 8 * HIST)
            v = pre[at, cols]
            s = sigmoid(v)
            outer = jnp.broadcast_to(gp[pl.ds(pl.multiple_of(u * 8, 8), 8), cols][:, None, :], (8, HIST, CW))
            g[k, at] = (outer.reshape(8 * HIST, CW) * s * (1.0 + v * (1.0 - s))).astype(BF16)
            to = pl.ds(pl.multiple_of(ROWS + u * 8 * HIST, 8 * HIST), 8 * HIST)
            pltpu.make_async_remote_copy(
                src_ref=g.at[k, at], dst_ref=g.at[k, to], send_sem=g_s.at[k, u], recv_sem=g_r.at[k, u],
                device_id=sibling, device_id_type=MESH,
            ).start()
            return 0

        lax.fori_loop(0, USERS // 8, step, 0)
        return 0

    def towards(axis, v):
        at = list(pos)
        at[axis] = v
        return device(at[0], at[1], at[2], c)

    def item_home():
        for copy in ig_recv:
            copy.wait_recv()
        item_grad = pigf[0]
        for n in range(len(near_items)):
            item_grad = item_grad + rig[n].astype(F32)
        ig_ref[...] = item_grad
        item_normed = inorm[...]
        radial = jnp.sum(item_normed * item_grad, axis=1, keepdims=True)
        gi[0, 0] = ((item_grad - item_normed * radial) / ilen[:, 0:1]).astype(BF16)
        gi_hand(0)
        for d in steps:
            pltpu.make_async_remote_copy(
                src_ref=gi.at[0, 0], dst_ref=gi.at[0, d], send_sem=gi_s.at[d], recv_sem=gi_r.at[d],
                device_id=item_peer(0, d, 0), device_id_type=MESH,
            ).start()

    def gi_hand(d):
        pltpu.make_async_remote_copy(
            src_ref=gi.at[0, d], dst_ref=gi.at[1, d], send_sem=gh_s.at[d], recv_sem=gh_r.at[d],
            device_id=sibling, device_id_type=MESH,
        ).start()

    def weight_grad(m, _):
        k = jnp.where(m < 2, 1 - m, m)
        pl.when(m == 1)(item_home)
        for u in range(USERS // 8):
            arrived(g.at[k, pl.ds(ROWS + u * 8 * HIST, 8 * HIST)], g_r.at[k, u])
        part[k] = dot(xt[...], g[k]).astype(BF16).reshape(XH, N, XL, N, 16, CW)
        for axis in range(COLOURS):

            @pl.when(k == axis)
            def _(axis=axis):
                for d in steps:
                    t = plus(pos[axis], d, N)
                    pltpu.make_async_remote_copy(
                        src_ref=slab(axis, t), dst_ref=ra[axis].at[d - 1], send_sem=ra_s.at[axis, d - 1],
                        recv_sem=ra_r.at[axis, d - 1], device_id=towards(axis, t), device_id_type=MESH,
                    ).start()

        return 0

    ra = (ra0, ra1, ra2)

    def slab(axis, t):
        if axis == 0:
            return part.at[0, t // XL, :, lax.rem(t, XL)]
        if axis == 1:
            return part.at[1, :, :, :, t]
        return part.at[2, :, t]

    lax.fori_loop(0, COLOURS, backward, 0)
    for copy in loss_copies:
        copy.wait_recv()
    loss_copies = reduce_loss(reduced_loss(0), 1, y)
    lax.fori_loop(0, COLOURS, weight_grad, 0)
    for copy in loss_copies:
        copy.wait_recv()
    loss_copies = reduce_loss(reduced_loss(1), 2, z)
    flight = {}

    def add_a(k):
        for d in range(N - 1):
            arrived(ra[k].at[d], ra_r.at[k, d])
        p1, p2 = pos[(k + 1) % 3], pos[(k + 2) % 3]
        flight[k] = []
        for n, (di, dj) in enumerate(planes + [(0, 0)]):
            i, j = plus(p1, di, N), plus(p2, dj, N)
            if k == 0:
                own, got = part.at[0, x // XL, j, lax.rem(x, XL), i], lambda d: ra0[d, j, i]
            elif k == 1:
                own, got = part.at[1, j // XL, i, lax.rem(j, XL), y], lambda d: ra1[d, j // XL, i, lax.rem(j, XL)]
            else:
                own, got = part.at[2, i // XL, z, lax.rem(i, XL), j], lambda d: ra2[d, i // XL, lax.rem(i, XL), j]
            total = own[...].astype(F32)
            for d in range(N - 1):
                total = total + got(d).astype(F32)
            sa[k, n] = total.astype(BF16)
            if (di, dj) != (0, 0):
                at = list(pos)
                at[(k + 1) % 3], at[(k + 2) % 3] = i, j
                to = device(at[0], at[1], at[2], c)
                flight[k].append(send(sa.at[k, n], rb.at[k, n], rs_s.at[k, n], rs_r.at[k, n], to))

    def add_b(k):
        for copy in flight[k]:
            copy.wait_recv()
        total = sa[k, len(planes)].astype(F32)
        for n in range(len(planes)):
            total = total + rb[k, n].astype(F32)
        gu_ref[:, k * CW:(k + 1) * CW] = total

    for d in reversed(steps):
        arrived(gi.at[0, d], gi_r.at[d])
        gi_hand(d)
    for copy in xi_recv:
        copy.wait_recv()
    for d in range(N):
        arrived(gi.at[1, d], gh_r.at[d])
    for h in range(XH):
        r = dot_t(xi[h].reshape(N * CORES * USERS, FEAT), gi[...].reshape(N * CORES * USERS, E)).astype(BF16)
        parti[h * XL:(h + 1) * XL] = r.reshape(XL, N, 16, E)
    ri_recv = []
    for n, (dx, dy) in enumerate(planes):
        tx, ty = plus(x, dx, N), plus(y, dy, N)
        ri_recv.append(send(parti.at[tx, ty], ri.at[n], ri_s.at[n], ri_r.at[n], row_peer(dx, dy)))
    add_a(1)
    add_a(0)
    add_a(2)
    for copy in loss_copies:
        copy.wait_recv()
    corelosses[c] = reduced_loss(2)
    core_copy = send(corelosses.at[c], corelosses.at[c], hop_s.at[3], hop_r.at[3], sibling)
    for copy in sent:
        copy.wait_send()
    for k in range(COLOURS):
        for u in range(USERS // 8):
            left(g.at[k, pl.ds(u * 8 * HIST, 8 * HIST)], g_s.at[k, u])
        for d in range(N - 1):
            left(ra[k].at[d], ra_s.at[k, d])
    for d in range(N):
        left(gi.at[0, d], gh_s.at[d])
        if d:
            left(gi.at[0, 0], gi_s.at[d])
    add_b(1)
    add_b(0)
    core_copy.wait_recv()
    loss_ref[...] = jnp.broadcast_to(jnp.sum(corelosses[0] + corelosses[1], keepdims=True) / TOTAL, (8, 128))
    for copy in ri_recv:
        copy.wait_recv()
    total = parti[x, y].astype(F32)
    for n in range(len(planes)):
        total = total + ri[n].astype(F32)
    gi_ref[...] = total
    add_b(2)


def hand_out(loss, ig, gu, gi, loss_out, ig_out, gu_out, gi_out):
    loss_out[0] = loss[0, 0]
    ig_out[...] = ig[...]
    gu_out[...] = gu[...]
    gi_out[...] = gi[...]


def shards(N, XL, past, cand, wu, wi, scale, shift, ids, slots):
    users, hist, depth = past.shape
    E = wu.shape[1]
    total = users * lax.axis_size("blk") * lax.axis_size("group")
    NU, NI, NS, QN = XL * N, XL * N * CORES, XL * N, (N // XL) * N
    feat = depth // (QN * CORES)
    hbm = pl.BlockSpec(memory_space=pltpu.HBM)
    smem = pl.BlockSpec(memory_space=pltpu.SMEM)
    vmem = pl.BlockSpec(memory_space=pltpu.VMEM)
    rows = depth // (N * N * N * CORES)
    CW = E // COLOURS

    def dma(*shape):
        return pltpu.SemaphoreType.DMA(shape)

    V = pltpu.VMEM
    scratch = [
        V((users * hist, depth), BF16), V((QN, users * hist, feat), BF16),
        V((users, depth), BF16),
        V((depth, E), BF16), V((depth, E), BF16),
        V((users * hist, E), F32), V((users, E), F32), V((users, E), F32), V((users, 128), F32),
        V((users, E), F32), V((users, 128), F32),
        V((NU, users, E), BF16), V((CORES, NS, users, E), BF16), V((NI, 1, 128), F32), V((NI, users, 128), F32),
        V((NU, 1, NU * users), F32), V((NU, 1, NU * users), F32),
        V((NI * users, NU * users), BF16),
        V((CORES, NS, users, E), BF16), V((NS, users, E), F32), V((NS, users, E), BF16),
        V((NS - 1, users, E), BF16),
        V((NU, users, E), BF16), V((NU - 1, users, E), BF16),
        V((COLOURS, 2 * users * hist, CW), BF16), V((CORES, N, users, E), BF16),
        V((N // XL, N * CORES, users, feat), BF16), V((QN * feat, 2 * users * hist), BF16),
        V((COLOURS, N // XL, N, XL, N, rows, CW), BF16), V((N - 1, N, N, rows, CW), BF16),
        V((N - 1, N // XL, N, XL, rows, CW), BF16), V((N - 1, N // XL, XL, N, rows, CW), BF16),
        V((COLOURS, N * N, rows, CW), BF16), V((COLOURS, N * N - 1, rows, CW), BF16),
        V((N, N, rows, E), BF16), V((N * N - 1, rows, E), BF16),
        V((3, N, 8, 128), F32), V((CORES, 8, 128), F32),
        V((1, 1), F32), V((1, 1), F32), V((1, users), jnp.int32), V((1, users), jnp.int32),
        dma(8), dma(QN), dma(QN), dma(N * CORES - 1, N // XL), dma(N * CORES - 1, N // XL),
        dma(NI - 1), dma(NI - 1), dma(NU - 1), dma(NU - 1), dma(NU - 1), dma(NU - 1),
        dma(NS - 1), dma(NS - 1), dma(NU - 1), dma(NU - 1),
        dma(NS - 1), dma(NS - 1), dma(NU - 1), dma(NU - 1), dma(COLOURS, users // 8), dma(COLOURS, users // 8), dma(N), dma(N), dma(N), dma(N),
        dma(COLOURS, N - 1), dma(COLOURS, N - 1), dma(COLOURS, N * N - 1), dma(COLOURS, N * N - 1),
        dma(N * N - 1), dma(N * N - 1), dma(3, N - 1), dma(3, N - 1), dma(4), dma(4),
    ]
    outs = pl.pallas_call(
        functools.partial(tower_kernel, N, XL, total),
        name="two_tower",
        out_shape=(
            pltpu.VMEM((8, 128), F32),
            pltpu.VMEM((users, E), F32),
            pltpu.VMEM((rows, E), F32),
            pltpu.VMEM((rows, E), F32),
        ),
        in_specs=[hbm] * 8,
        out_specs=(vmem,) * 4,
        scratch_shapes=scratch,
        compiler_params=pltpu.CompilerParams(
            collective_id=0, has_side_effects=True, vmem_limit_bytes=60 * 1024 * 1024
        ),
    )(
        past.reshape(users * hist, depth), cand, wu, wi, scale.reshape(1, 1), shift.reshape(1, 1),
        ids.reshape(1, users), slots.reshape(1, users),
    )
    return pl.pallas_call(
        hand_out,
        name="hand_out",
        out_shape=(
            jax.ShapeDtypeStruct((1,), F32),
            jax.ShapeDtypeStruct((users, E), F32),
            jax.ShapeDtypeStruct((rows, E), F32),
            jax.ShapeDtypeStruct((rows, E), F32),
        ),
        in_specs=[vmem] * 4,
        out_specs=(smem, vmem, vmem, vmem),
        compiler_params=pltpu.CompilerParams(vmem_limit_bytes=4 * 1024 * 1024),
    )(*outs)


def solution(mesh):
    group = mesh.shape["group"]
    n = {128: 4, 16: 2}[mesh.size]
    both = ("blk", "group")
    return jax.shard_map(
        functools.partial(shards, n, group // n),
        mesh=mesh,
        in_specs=(P(both, None, None), P(both, None), P(), P(), P(), P(), P(both), P(both)),
        out_specs=(P(), P(both, None), P(both, None), P(both, None)),
        check_vma=False,
    )
```

```python
import functools

import jax
import jax.numpy as jnp
from jax import lax
from jax.experimental import pallas as pl
from jax.experimental.pallas import tpu as pltpu
from jax.sharding import PartitionSpec as P

EPS = 1e-06
MESH = pl.DeviceIdType.MESH
F32 = jnp.float32
BF16 = jnp.bfloat16
CORES = 2
COLOURS = 3


def dot(a, b):
    return jnp.dot(a, b, preferred_element_type=F32)


def dot_t(a, b):
    return lax.dot_general(a, b, (((0,), (0,)), ((), ())), preferred_element_type=F32)


def dot_nt(a, b):
    return lax.dot_general(a, b, (((1,), (1,)), ((), ())), preferred_element_type=F32)


def sigmoid(v):
    return 0.5 + 0.5 * jnp.tanh(0.5 * v)


def tower_kernel(
    N, XL, TOTAL,
    x_hbm, ci_hbm, wu_hbm, wi_hbm, scale_ref, shift_ref, ids_ref, slot_ref,
    loss_ref, ig_ref, gu_ref, gi_ref,
    xv, xs, civ, wuv, wiv, pre, pooled, gp, ulen, inorm, ilen,
    ua, ia, idrow, idbuf, slotbuf, tgtbuf, wt, pig, pigf, rigc, rig, pgu, rgu, g, gi, xi, xt,
    part, ra0, ra1, ra2, sa, rb, parti, ri, si, rj, losses, corelosses, scale_s, shift_s, idv, slotv,
    lsem, xsem_s, xsem_r, xi_s, xi_r, id_s, id_r, slot_s, slot_r, tgt_s, tgt_r,
    ia_s, ia_r, ua_s, ua_r, ig_s, ig_r, ug_s, ug_r, g_s, g_r, gi_s, gi_r, gh_s, gh_r,
    ra_s, ra_r, rs_s, rs_r, ri_s, ri_r, rj_s, rj_r, lo_s, lo_r, hop_s, hop_r,
):
    USERS, E = pooled.shape
    HIST = xv.shape[0] // USERS
    FEAT = 128 if N == 4 else XL * N * 16
    QN = (N // XL) * N
    NU = XL * N
    NI = XL * N * CORES
    NS = XL * N
    CW = E // COLOURS
    XH = N // XL
    ROWS = USERS * HIST
    blk = lax.axis_index("blk")
    group = lax.axis_index("group")
    c = lax.rem(blk, CORES)
    z = lax.rem(blk // CORES, N)
    x = (blk // (CORES * N)) * XL + group // N
    y = lax.rem(group, N)
    odd = lax.rem(x, 2)
    pair_a = x + 1 - 2 * odd
    pair_b = lax.rem(x + N - 1 + 2 * odd, N)

    def device(px, py, pz, pc):
        return (((px // XL) * N + pz) * CORES + pc, lax.rem(px, XL) * N + py)

    def plus(v, d, n):
        return v if d == 0 else lax.rem(v + d, n)

    def minus(v, d, n):
        return v if d == 0 else lax.rem(v + n - d, n)

    def send(src, dst, ssem, rsem, to):
        copy = pltpu.make_async_remote_copy(
            src_ref=src, dst_ref=dst, send_sem=ssem, recv_sem=rsem, device_id=to, device_id_type=MESH
        )
        copy.start()
        sent.append(copy)
        return copy

    def arrived(dst, sem):
        pltpu.make_async_remote_copy(
            src_ref=dst, dst_ref=dst, send_sem=sem, recv_sem=sem, device_id=sibling, device_id_type=MESH
        ).wait_recv()

    def left(src, sem):
        pltpu.make_async_remote_copy(
            src_ref=src, dst_ref=src, send_sem=sem, recv_sem=sem, device_id=sibling, device_id_type=MESH
        ).wait_send()

    sent = []
    sibling = device(x, y, z, 1 - c)
    def ring(d):
        return min(d, N - d)

    span = range(N)
    user_peers = [(da, dy) for da in range(2) for dy in span if (da, dy) != (0, 0)]
    user_peers.sort(key=lambda p: -p[0] - ring(p[1]))
    near_items = [(db, dz, 0) for db in range(2) for dz in span if (db, dz) != (0, 0)]
    near_items.sort(key=lambda p: -p[0] - ring(p[1]))
    item_peers = near_items + [(db, dz, 1) for db in range(2) for dz in span]
    planes = [(di, dj) for di in span for dj in span if (di, dj) != (0, 0)]
    planes.sort(key=lambda p: -ring(p[0]) - ring(p[1]))
    feat_peers = [(dz, dc) for dc in range(CORES) for dz in span if (dz, dc) != (0, 0)]
    steps = sorted(range(1, N), key=lambda d: -ring(d))

    def user_peer(da, dy):
        return device(pair_a if da else x, plus(y, dy, N), z, c)

    def user_slot(da, dy):
        return (1 - odd if da else odd) * N + plus(y, dy, N)

    def item_slot(db, dz, dc):
        return dc * NS + db * N + dz

    def item_peer(db, dz, dc):
        return device(pair_b if db else x, y, plus(z, dz, N), plus(c, dc, CORES))

    def item_owner(db, dz, dc):
        return device(pair_b if db else x, y, minus(z, dz, N), plus(c, dc, CORES))

    def row_peer(dx, dy):
        return device(plus(x, dx, N), plus(y, dy, N), z, c)

    small = [
        pltpu.make_async_copy(a, b, lsem.at[4 + n])
        for n, (a, b) in enumerate(((ids_ref, idv), (slot_ref, slotv), (scale_ref, scale_s), (shift_ref, shift_s)))
    ]
    for load in small:
        load.start()
    load_ci = pltpu.make_async_copy(ci_hbm, civ, lsem.at[0])
    load_wi = pltpu.make_async_copy(wi_hbm, wiv, lsem.at[1])
    load_x = pltpu.make_async_copy(x_hbm, xv, lsem.at[2])
    load_wu = pltpu.make_async_copy(wu_hbm, wuv, lsem.at[3])
    for load in (load_ci, load_wi, load_x, load_wu):
        load.start()

    barrier = pltpu.get_barrier_semaphore()
    greeted = [row_peer(*d) for d in planes]
    greeted += [device(plus(x, dx, N), y, plus(z, dz, N), c) for dx in range(N) for dz in range(1, N)]
    greeted += [device(x, plus(y, dy, N), plus(z, dz, N), c) for dy in range(1, N) for dz in range(1, N)]
    greeted += [item_peer(*d) for d in item_peers if d[2]]
    for to in greeted:
        pl.semaphore_signal(barrier, inc=1, device_id=to, device_id_type=MESH)
    for load in small:
        load.wait()
    my_user_slot = user_slot(0, 0)
    rows = lax.broadcasted_iota(jnp.int32, (USERS, USERS), 0)
    lanes = lax.broadcasted_iota(jnp.int32, (USERS, USERS), 1)
    id_col = jnp.sum(jnp.where(rows == lanes, idv[...].astype(F32), 0.0), axis=1, keepdims=True)
    slot_col = jnp.sum(jnp.where(rows == lanes, slotv[...].astype(F32), 0.0), axis=1, keepdims=True)
    tile_rows = lax.broadcasted_iota(jnp.int32, (USERS, 128), 0)
    tile_lanes = lax.broadcasted_iota(jnp.int32, (USERS, 128), 1)
    idrow[0] = jnp.sum(jnp.where(tile_rows == tile_lanes, id_col, 0.0), axis=0, keepdims=True)
    wide_rows = lax.broadcasted_iota(jnp.int32, (USERS, NU * USERS), 0)
    wide_lanes = lax.broadcasted_iota(jnp.int32, (USERS, NU * USERS), 1)
    slotbuf[0] = jnp.sum(
        jnp.where(wide_lanes == wide_rows + my_user_slot * USERS, slot_col, 0.0), axis=0, keepdims=True
    )
    load_ci.wait()
    load_wi.wait()
    item_pre = dot(civ[...], wiv[...])
    item_len = jnp.sqrt(jnp.sum(item_pre * item_pre, axis=1, keepdims=True) + EPS)
    item_normed = item_pre / item_len
    inorm[...] = item_normed
    ilen[...] = jnp.broadcast_to(item_len, (USERS, 128))
    ia[0, 0] = item_normed.astype(BF16)
    pl.semaphore_wait(barrier, len(greeted))
    id_recv, slot_recv = [], []
    for n, d in enumerate(user_peers):
        slot_recv.append(send(slotbuf.at[0], slotbuf.at[n + 1], slot_s.at[n], slot_r.at[n], user_peer(*d)))
    for n, d in enumerate(item_peers):
        id_recv.append(send(idrow.at[0], idrow.at[item_slot(*d)], id_s.at[n], id_r.at[n], item_peer(*d)))
    ia_recv = []
    for n, d in enumerate(near_items):
        ia_recv.append(send(ia.at[0, 0], ia.at[0, item_slot(*d)], ia_s.at[n], ia_r.at[n], item_peer(*d)))
    load_x.wait()
    x_recv = []
    for q in range(QN):
        cols = pl.ds(pl.multiple_of((q * CORES + 1 - c) * FEAT, FEAT), FEAT)
        x_recv.append(send(xv.at[:, cols], xs.at[q], xsem_s.at[q], xsem_r.at[q], sibling))
    load_wu.wait()

    def forward(n, _):
        cols = pl.ds(pl.multiple_of(n * 256, 256), 256)
        pre[:, cols] = dot(xv[...], wuv[:, cols])
        return 0

    lax.fori_loop(0, E // 256, forward, 0)

    for copy in slot_recv + id_recv:
        copy.wait_recv()
    slots = slotbuf[0]
    for n in range(1, NU):
        slots = slots + slotbuf[n]
    wide = NU * USERS // 128
    found = jnp.zeros((1, NU * USERS), F32)
    for dc in range(CORES):
        for db in range(2):
            for dz in range(N):
                s = item_slot(db, dz, dc)
                col = jnp.sum(jnp.where(tile_rows == tile_lanes, idrow[s], 0.0), axis=1, keepdims=True)
                ids = jnp.broadcast_to(col, (USERS, 128))
                idbuf[s] = ids
                ob, og = item_owner(db, dz, dc)
                at = (tile_rows + (ob * (XL * N) + og) * USERS).astype(F32)
                hit = jnp.concatenate([at] * wide, axis=1) == slots
                found = found + jnp.sum(
                    jnp.where(hit, jnp.concatenate([ids] * wide, axis=1), 0.0), axis=0, keepdims=True
                )
    tgtbuf[0] = found
    tgt_recv = []
    for n, d in enumerate(user_peers):
        tgt_recv.append(send(tgtbuf.at[0], tgtbuf.at[n + 1], tgt_s.at[n], tgt_r.at[n], user_peer(*d)))

    def pool(n, _):
        u = n // COLOURS
        cols = pl.ds(pl.multiple_of(lax.rem(n, COLOURS) * CW, CW), CW)
        v = pre[pl.ds(pl.multiple_of(u * 8 * HIST, 8 * HIST), 8 * HIST), cols]
        act = v * sigmoid(v)
        pooled[pl.ds(pl.multiple_of(u * 8, 8), 8), cols] = jnp.sum(act.reshape(8, HIST, CW), axis=1) / HIST
        return 0

    lax.fori_loop(0, (USERS // 8) * COLOURS, pool, 0)
    mean = pooled[...]
    user_len = jnp.sqrt(jnp.sum(mean * mean, axis=1, keepdims=True) + EPS)
    user_normed = mean / user_len
    ulen[...] = jnp.broadcast_to(user_len, (USERS, 128))
    pooled[...] = user_normed
    ua[my_user_slot] = user_normed.astype(BF16)
    ua_recv = []
    for n, d in enumerate(user_peers):
        ua_recv.append(send(ua.at[my_user_slot], ua.at[my_user_slot], ua_s.at[n], ua_r.at[n], user_peer(*d)))

    xi_recv = []
    for n, (dz, dc) in enumerate(feat_peers):
        pz, pc = plus(z, dz, N), plus(c, dc, CORES)
        for h in range(XH):
            cols = pl.ds(pl.multiple_of(((h * N + pz) * CORES + pc) * FEAT, FEAT), FEAT)
            xi_recv.append(
                send(civ.at[:, cols], xi.at[h, dc * N + dz], xi_s.at[n, h], xi_r.at[n, h], item_peer(0, dz, dc))
            )
    for h in range(XH):
        xi[h, 0] = civ[:, pl.ds(pl.multiple_of(((h * N + z) * CORES + c) * FEAT, FEAT), FEAT)]
    for copy in ia_recv:
        copy.wait_recv()
    ia_hop = send(ia.at[0], ia.at[1], hop_s.at[0], hop_r.at[0], sibling)
    for copy in x_recv:
        copy.wait_recv()

    def turn(q, _):
        cols = pl.ds(pl.multiple_of((q * CORES + c) * FEAT, FEAT), FEAT)
        to = pl.ds(pl.multiple_of(q * FEAT, FEAT), FEAT)
        xt[to, 0:ROWS] = xv[:, cols].T
        xt[to, ROWS:2 * ROWS] = xs[q].T
        return 0

    lax.fori_loop(0, QN, turn, 0)
    for copy in tgt_recv:
        copy.wait_recv()
    targets = tgtbuf[0]
    for n in range(1, NU):
        targets = targets + tgtbuf[n]

    for copy in ua_recv:
        copy.wait_recv()
    ia_hop.wait_recv()
    scale = scale_s[0, 0]
    shift = shift_s[0, 0]
    users = ua[...].reshape(NU * USERS, E)
    loss = jnp.zeros((8, 128), F32)
    for n in range(NI // N):
        items = ia[n // 2, (n % 2) * N:(n % 2 + 1) * N].reshape(N * USERS, E)
        scores = dot_nt(items, users)
        ids = idbuf[n * N:(n + 1) * N].reshape(N * USERS, 128)
        sign = jnp.where(jnp.concatenate([ids] * wide, axis=1) == targets, 1.0, -1.0)
        margin = sign * (scale * scores + shift)
        e = jnp.exp(-jnp.abs(margin))
        terms = jnp.log1p(e) + jnp.maximum(-margin, 0.0)
        gate = jnp.where(margin >= 0.0, e, 1.0) / (1.0 + e)
        wt[n * N * USERS:(n + 1) * N * USERS, :] = (-scale * sign * gate).astype(BF16)
        terms = jnp.sum(terms.reshape(N * USERS // 8, 8, NU * USERS), axis=0)
        for j in range(wide):
            loss = loss + terms[:, j * 128:(j + 1) * 128]
    def reduce_loss(value, step, pos):
        losses[step, pos] = value
        copies = []
        for d in range(1, N):
            at = [x, y, z]
            at[step] = plus(pos, d, N)
            copies.append(
                send(losses.at[step, pos], losses.at[step, pos], lo_s.at[step, d - 1], lo_r.at[step, d - 1],
                     device(at[0], at[1], at[2], c))
            )
        return copies

    def reduced_loss(step):
        total = losses[step, 0]
        for d in range(1, N):
            total = total + losses[step, d]
        return total

    loss_copies = reduce_loss(loss, 0, x)
    pgu[...] = dot_t(wt[...], ia[...].reshape(NI * USERS, E)).astype(BF16).reshape(NU, USERS, E)
    ug_recv = []
    for n, d in enumerate(user_peers):
        ug_recv.append(send(pgu.at[user_slot(*d)], rgu.at[n], ug_s.at[n], ug_r.at[n], user_peer(*d)))
    pig[1] = dot(wt[NS * USERS:2 * NS * USERS, :], users).astype(BF16).reshape(NS, USERS, E)
    ig_hop = send(pig.at[1], rigc, hop_s.at[1], hop_r.at[1], sibling)
    pigf[...] = dot(wt[0:NS * USERS, :], users).reshape(NS, USERS, E)
    ig_hop.wait_recv()
    ig_recv = []
    for s in range(NS):
        pigf[s] = pigf[s] + rigc[s].astype(F32)
        if s > 0:
            pig[0, s] = pigf[s].astype(BF16)
    for n, d in enumerate(near_items):
        ig_recv.append(send(pig.at[0, item_slot(*d)], rig.at[n], ig_s.at[n], ig_r.at[n], item_owner(*d)))

    for copy in ug_recv:
        copy.wait_recv()
    grad_users = pgu[my_user_slot].astype(F32)
    for n in range(len(user_peers)):
        grad_users = grad_users + rgu[n].astype(F32)
    user_normed = pooled[...]
    radial = jnp.sum(user_normed * grad_users, axis=1, keepdims=True)
    gp[...] = (grad_users - user_normed * radial) / ulen[:, 0:1] / HIST

    pos = (x, y, z)

    def backward(m, _):
        k = jnp.where(m < 2, 1 - m, m)
        cols = pl.ds(pl.multiple_of(k * CW, CW), CW)

        def step(u, _):
            at = pl.ds(pl.multiple_of(u * 8 * HIST, 8 * HIST), 8 * HIST)
            v = pre[at, cols]
            s = sigmoid(v)
            outer = jnp.broadcast_to(gp[pl.ds(pl.multiple_of(u * 8, 8), 8), cols][:, None, :], (8, HIST, CW))
            g[k, at] = (outer.reshape(8 * HIST, CW) * s * (1.0 + v * (1.0 - s))).astype(BF16)
            to = pl.ds(pl.multiple_of(ROWS + u * 8 * HIST, 8 * HIST), 8 * HIST)
            pltpu.make_async_remote_copy(
                src_ref=g.at[k, at], dst_ref=g.at[k, to], send_sem=g_s.at[k, u], recv_sem=g_r.at[k, u],
                device_id=sibling, device_id_type=MESH,
            ).start()
            return 0

        lax.fori_loop(0, USERS // 8, step, 0)
        return 0

    def towards(axis, v):
        at = list(pos)
        at[axis] = v
        return device(at[0], at[1], at[2], c)

    def item_home():
        for copy in ig_recv:
            copy.wait_recv()
        item_grad = pigf[0]
        for n in range(len(near_items)):
            item_grad = item_grad + rig[n].astype(F32)
        ig_ref[...] = item_grad
        item_normed = inorm[...]
        radial = jnp.sum(item_normed * item_grad, axis=1, keepdims=True)
        gi[0, 0] = ((item_grad - item_normed * radial) / ilen[:, 0:1]).astype(BF16)
        gi_hand(0)
        for d in steps:
            pltpu.make_async_remote_copy(
                src_ref=gi.at[0, 0], dst_ref=gi.at[0, d], send_sem=gi_s.at[d], recv_sem=gi_r.at[d],
                device_id=item_peer(0, d, 0), device_id_type=MESH,
            ).start()

    def gi_hand(d):
        pltpu.make_async_remote_copy(
            src_ref=gi.at[0, d], dst_ref=gi.at[1, d], send_sem=gh_s.at[d], recv_sem=gh_r.at[d],
            device_id=sibling, device_id_type=MESH,
        ).start()

    def weight_grad(m, _):
        k = jnp.where(m < 2, 1 - m, m)
        pl.when(m == 1)(item_home)
        for u in range(USERS // 8):
            arrived(g.at[k, pl.ds(ROWS + u * 8 * HIST, 8 * HIST)], g_r.at[k, u])
        part[k] = dot(xt[...], g[k]).astype(BF16).reshape(XH, N, XL, N, 16, CW)
        for axis in range(COLOURS):

            @pl.when(k == axis)
            def _(axis=axis):
                for d in steps:
                    t = plus(pos[axis], d, N)
                    pltpu.make_async_remote_copy(
                        src_ref=slab(axis, t), dst_ref=ra[axis].at[d - 1], send_sem=ra_s.at[axis, d - 1],
                        recv_sem=ra_r.at[axis, d - 1], device_id=towards(axis, t), device_id_type=MESH,
                    ).start()

        return 0

    ra = (ra0, ra1, ra2)

    def slab(axis, t):
        if axis == 0:
            return part.at[0, t // XL, :, lax.rem(t, XL)]
        if axis == 1:
            return part.at[1, :, :, :, t]
        return part.at[2, :, t]

    lax.fori_loop(0, COLOURS, backward, 0)
    for copy in loss_copies:
        copy.wait_recv()
    loss_copies = reduce_loss(reduced_loss(0), 1, y)
    lax.fori_loop(0, COLOURS, weight_grad, 0)
    for copy in loss_copies:
        copy.wait_recv()
    loss_copies = reduce_loss(reduced_loss(1), 2, z)
    flight = {}

    def add_a(k):
        for d in range(N - 1):
            arrived(ra[k].at[d], ra_r.at[k, d])
        p1, p2 = pos[(k + 1) % 3], pos[(k + 2) % 3]
        flight[k] = []
        for n, (di, dj) in enumerate(planes + [(0, 0)]):
            i, j = plus(p1, di, N), plus(p2, dj, N)
            if k == 0:
                own, got = part.at[0, x // XL, j, lax.rem(x, XL), i], lambda d: ra0[d, j, i]
            elif k == 1:
                own, got = part.at[1, j // XL, i, lax.rem(j, XL), y], lambda d: ra1[d, j // XL, i, lax.rem(j, XL)]
            else:
                own, got = part.at[2, i // XL, z, lax.rem(i, XL), j], lambda d: ra2[d, i // XL, lax.rem(i, XL), j]
            total = own[...].astype(F32)
            for d in range(N - 1):
                total = total + got(d).astype(F32)
            sa[k, n] = total.astype(BF16)
            if (di, dj) != (0, 0):
                at = list(pos)
                at[(k + 1) % 3], at[(k + 2) % 3] = i, j
                to = device(at[0], at[1], at[2], c)
                flight[k].append(send(sa.at[k, n], rb.at[k, n], rs_s.at[k, n], rs_r.at[k, n], to))

    def add_b(k):
        for copy in flight[k]:
            copy.wait_recv()
        total = sa[k, len(planes)].astype(F32)
        for n in range(len(planes)):
            total = total + rb[k, n].astype(F32)
        gu_ref[:, k * CW:(k + 1) * CW] = total

    for d in reversed(steps):
        arrived(gi.at[0, d], gi_r.at[d])
        gi_hand(d)
    for copy in xi_recv:
        copy.wait_recv()
    for d in range(N):
        arrived(gi.at[1, d], gh_r.at[d])
    for h in range(XH):
        r = dot_t(xi[h].reshape(N * CORES * USERS, FEAT), gi[...].reshape(N * CORES * USERS, E)).astype(BF16)
        parti[h * XL:(h + 1) * XL] = r.reshape(XL, N, 16, E)
    left_half, right_half = pl.ds(0, E // 2), pl.ds(E // 2, E // 2)
    ri_recv = []
    for d in steps:
        t = plus(x, d, N)
        src = parti.at[t, :, :, left_half]
        ri_recv.append(send(src, ri.at[0, d - 1], ri_s.at[0, d - 1], ri_r.at[0, d - 1], towards(0, t)))
        t = plus(y, d, N)
        src = parti.at[:, t, :, right_half]
        ri_recv.append(send(src, ri.at[1, d - 1], ri_s.at[1, d - 1], ri_r.at[1, d - 1], towards(1, t)))
    add_a(1)
    add_a(0)
    add_a(2)
    for copy in ri_recv:
        copy.wait_recv()
    for n in range(N):
        total = parti[x, n, :, 0:E // 2].astype(F32)
        for d in range(N - 1):
            total = total + ri[0, d, n].astype(F32)
        si[0, n] = total.astype(BF16)
        total = parti[n, y, :, E // 2:E].astype(F32)
        for d in range(N - 1):
            total = total + ri[1, d, n].astype(F32)
        si[1, n] = total.astype(BF16)
    ri_recv = []
    for h in range(2):
        for d in steps:
            t = plus(pos[1 - h], d, N)
            ri_recv.append(send(si.at[h, t], rj.at[h, d - 1], rj_s.at[h, d - 1], rj_r.at[h, d - 1], towards(1 - h, t)))
    for copy in loss_copies:
        copy.wait_recv()
    corelosses[c] = reduced_loss(2)
    core_copy = send(corelosses.at[c], corelosses.at[c], hop_s.at[3], hop_r.at[3], sibling)
    for copy in sent:
        copy.wait_send()
    for k in range(COLOURS):
        for u in range(USERS // 8):
            left(g.at[k, pl.ds(u * 8 * HIST, 8 * HIST)], g_s.at[k, u])
        for d in range(N - 1):
            left(ra[k].at[d], ra_s.at[k, d])
    for d in range(N):
        left(gi.at[0, d], gh_s.at[d])
        if d:
            left(gi.at[0, 0], gi_s.at[d])
    add_b(1)
    add_b(0)
    core_copy.wait_recv()
    loss_ref[...] = jnp.broadcast_to(jnp.sum(corelosses[0] + corelosses[1], keepdims=True) / TOTAL, (8, 128))
    for copy in ri_recv:
        copy.wait_recv()
    for h in range(2):
        total = si[h, pos[1 - h]].astype(F32)
        for d in range(N - 1):
            total = total + rj[h, d].astype(F32)
        gi_ref[:, h * (E // 2):(h + 1) * (E // 2)] = total
    add_b(2)


def hand_out(loss, ig, gu, gi, loss_out, ig_out, gu_out, gi_out):
    loss_out[0] = loss[0, 0]
    ig_out[...] = ig[...]
    gu_out[...] = gu[...]
    gi_out[...] = gi[...]


def shards(N, XL, past, cand, wu, wi, scale, shift, ids, slots):
    users, hist, depth = past.shape
    E = wu.shape[1]
    total = users * lax.axis_size("blk") * lax.axis_size("group")
    NU, NI, NS, QN = XL * N, XL * N * CORES, XL * N, (N // XL) * N
    feat = depth // (QN * CORES)
    hbm = pl.BlockSpec(memory_space=pltpu.HBM)
    smem = pl.BlockSpec(memory_space=pltpu.SMEM)
    vmem = pl.BlockSpec(memory_space=pltpu.VMEM)
    rows = depth // (N * N * N * CORES)
    CW = E // COLOURS

    def dma(*shape):
        return pltpu.SemaphoreType.DMA(shape)

    V = pltpu.VMEM
    scratch = [
        V((users * hist, depth), BF16), V((QN, users * hist, feat), BF16),
        V((users, depth), BF16),
        V((depth, E), BF16), V((depth, E), BF16),
        V((users * hist, E), F32), V((users, E), F32), V((users, E), F32), V((users, 128), F32),
        V((users, E), F32), V((users, 128), F32),
        V((NU, users, E), BF16), V((CORES, NS, users, E), BF16), V((NI, 1, 128), F32), V((NI, users, 128), F32),
        V((NU, 1, NU * users), F32), V((NU, 1, NU * users), F32),
        V((NI * users, NU * users), BF16),
        V((CORES, NS, users, E), BF16), V((NS, users, E), F32), V((NS, users, E), BF16),
        V((NS - 1, users, E), BF16),
        V((NU, users, E), BF16), V((NU - 1, users, E), BF16),
        V((COLOURS, 2 * users * hist, CW), BF16), V((CORES, N, users, E), BF16),
        V((N // XL, N * CORES, users, feat), BF16), V((QN * feat, 2 * users * hist), BF16),
        V((COLOURS, N // XL, N, XL, N, rows, CW), BF16), V((N - 1, N, N, rows, CW), BF16),
        V((N - 1, N // XL, N, XL, rows, CW), BF16), V((N - 1, N // XL, XL, N, rows, CW), BF16),
        V((COLOURS, N * N, rows, CW), BF16), V((COLOURS, N * N - 1, rows, CW), BF16),
        V((N, N, rows, E), BF16), V((2, N - 1, N, rows, E // 2), BF16),
        V((2, N, rows, E // 2), BF16), V((2, N - 1, rows, E // 2), BF16),
        V((3, N, 8, 128), F32), V((CORES, 8, 128), F32),
        V((1, 1), F32), V((1, 1), F32), V((1, users), jnp.int32), V((1, users), jnp.int32),
        dma(8), dma(QN), dma(QN), dma(N * CORES - 1, N // XL), dma(N * CORES - 1, N // XL),
        dma(NI - 1), dma(NI - 1), dma(NU - 1), dma(NU - 1), dma(NU - 1), dma(NU - 1),
        dma(NS - 1), dma(NS - 1), dma(NU - 1), dma(NU - 1),
        dma(NS - 1), dma(NS - 1), dma(NU - 1), dma(NU - 1), dma(COLOURS, users // 8), dma(COLOURS, users // 8), dma(N), dma(N), dma(N), dma(N),
        dma(COLOURS, N - 1), dma(COLOURS, N - 1), dma(COLOURS, N * N - 1), dma(COLOURS, N * N - 1),
        dma(2, N - 1), dma(2, N - 1), dma(2, N - 1), dma(2, N - 1), dma(3, N - 1), dma(3, N - 1), dma(4), dma(4),
    ]
    outs = pl.pallas_call(
        functools.partial(tower_kernel, N, XL, total),
        name="two_tower",
        out_shape=(
            pltpu.VMEM((8, 128), F32),
            pltpu.VMEM((users, E), F32),
            pltpu.VMEM((rows, E), F32),
            pltpu.VMEM((rows, E), F32),
        ),
        in_specs=[hbm] * 8,
        out_specs=(vmem,) * 4,
        scratch_shapes=scratch,
        compiler_params=pltpu.CompilerParams(
            collective_id=0, has_side_effects=True, vmem_limit_bytes=60 * 1024 * 1024
        ),
    )(
        past.reshape(users * hist, depth), cand, wu, wi, scale.reshape(1, 1), shift.reshape(1, 1),
        ids.reshape(1, users), slots.reshape(1, users),
    )
    return pl.pallas_call(
        hand_out,
        name="hand_out",
        out_shape=(
            jax.ShapeDtypeStruct((1,), F32),
            jax.ShapeDtypeStruct((users, E), F32),
            jax.ShapeDtypeStruct((rows, E), F32),
            jax.ShapeDtypeStruct((rows, E), F32),
        ),
        in_specs=[vmem] * 4,
        out_specs=(smem, vmem, vmem, vmem),
        compiler_params=pltpu.CompilerParams(vmem_limit_bytes=4 * 1024 * 1024),
    )(*outs)


def solution(mesh):
    group = mesh.shape["group"]
    n = {128: 4, 16: 2}[mesh.size]
    both = ("blk", "group")
    return jax.shard_map(
        functools.partial(shards, n, group // n),
        mesh=mesh,
        in_specs=(P(both, None, None), P(both, None), P(), P(), P(), P(), P(both), P(both)),
        out_specs=(P(), P(both, None), P(both, None), P(both, None)),
        check_vma=False,
    )
```

```python
import functools

import jax
import jax.numpy as jnp
from jax import lax
from jax.experimental import pallas as pl
from jax.experimental.pallas import tpu as pltpu
from jax.sharding import PartitionSpec as P

EPS = 1e-06
MESH = pl.DeviceIdType.MESH
F32 = jnp.float32
BF16 = jnp.bfloat16
CORES = 2
COLOURS = 3


def dot(a, b):
    return jnp.dot(a, b, preferred_element_type=F32)


def dot_t(a, b):
    return lax.dot_general(a, b, (((0,), (0,)), ((), ())), preferred_element_type=F32)


def dot_nt(a, b):
    return lax.dot_general(a, b, (((1,), (1,)), ((), ())), preferred_element_type=F32)


def sigmoid(v):
    return 0.5 + 0.5 * jnp.tanh(0.5 * v)


def tower_kernel(
    N, XL, TOTAL,
    x_hbm, ci_hbm, wu_hbm, wi_hbm, scale_ref, shift_ref, ids_ref, slot_ref,
    loss_ref, ig_ref, gu_ref, gi_ref,
    xv, xs, civ, wuv, wiv, pre, pooled, gp, ulen, inorm, ilen,
    ua, ia, idrow, idbuf, slotbuf, tgtbuf, wt, pig, pigf, rigc, rig, pgu, rgu, g, gi, xi, xt,
    part, ra0, ra1, ra2, sa, rb, parti, ri, si, rj, losses, corelosses, scale_s, shift_s, idv, slotv,
    lsem, xsem_s, xsem_r, xi_s, xi_r, id_s, id_r, slot_s, slot_r, tgt_s, tgt_r,
    ia_s, ia_r, ua_s, ua_r, ig_s, ig_r, ug_s, ug_r, g_s, g_r, gi_s, gi_r, gh_s, gh_r,
    ra_s, ra_r, rs_s, rs_r, ri_s, ri_r, rj_s, rj_r, lo_s, lo_r, hop_s, hop_r,
):
    USERS, E = pooled.shape
    HIST = xv.shape[0] // USERS
    FEAT = 128 if N == 4 else XL * N * 16
    QN = (N // XL) * N
    NU = XL * N
    NI = XL * N * CORES
    NS = XL * N
    CW = E // COLOURS
    XH = N // XL
    ROWS = USERS * HIST
    blk = lax.axis_index("blk")
    group = lax.axis_index("group")
    c = lax.rem(blk, CORES)
    z = lax.rem(blk // CORES, N)
    x = (blk // (CORES * N)) * XL + group // N
    y = lax.rem(group, N)
    odd = lax.rem(x, 2)
    pair_a = x + 1 - 2 * odd
    pair_b = lax.rem(x + N - 1 + 2 * odd, N)

    def device(px, py, pz, pc):
        return (((px // XL) * N + pz) * CORES + pc, lax.rem(px, XL) * N + py)

    def plus(v, d, n):
        return v if d == 0 else lax.rem(v + d, n)

    def minus(v, d, n):
        return v if d == 0 else lax.rem(v + n - d, n)

    def send(src, dst, ssem, rsem, to):
        copy = pltpu.make_async_remote_copy(
            src_ref=src, dst_ref=dst, send_sem=ssem, recv_sem=rsem, device_id=to, device_id_type=MESH
        )
        copy.start()
        sent.append(copy)
        return copy

    def arrived(dst, sem):
        pltpu.make_async_remote_copy(
            src_ref=dst, dst_ref=dst, send_sem=sem, recv_sem=sem, device_id=sibling, device_id_type=MESH
        ).wait_recv()

    def left(src, sem):
        pltpu.make_async_remote_copy(
            src_ref=src, dst_ref=src, send_sem=sem, recv_sem=sem, device_id=sibling, device_id_type=MESH
        ).wait_send()

    sent = []
    sibling = device(x, y, z, 1 - c)
    def ring(d):
        return min(d, N - d)

    span = range(N)
    user_peers = [(da, dy) for da in range(2) for dy in span if (da, dy) != (0, 0)]
    user_peers.sort(key=lambda p: -p[0] - ring(p[1]))
    near_items = [(db, dz, 0) for db in range(2) for dz in span if (db, dz) != (0, 0)]
    near_items.sort(key=lambda p: -p[0] - ring(p[1]))
    item_peers = near_items + [(db, dz, 1) for db in range(2) for dz in span]
    planes = [(di, dj) for di in span for dj in span if (di, dj) != (0, 0)]
    planes.sort(key=lambda p: -ring(p[0]) - ring(p[1]))
    feat_peers = [(dz, dc) for dc in range(CORES) for dz in span if (dz, dc) != (0, 0)]
    steps = sorted(range(1, N), key=lambda d: -ring(d))

    def user_peer(da, dy):
        return device(pair_a if da else x, plus(y, dy, N), z, c)

    def user_slot(da, dy):
        return (1 - odd if da else odd) * N + plus(y, dy, N)

    def item_slot(db, dz, dc):
        return dc * NS + db * N + dz

    def item_peer(db, dz, dc):
        return device(pair_b if db else x, y, plus(z, dz, N), plus(c, dc, CORES))

    def item_owner(db, dz, dc):
        return device(pair_b if db else x, y, minus(z, dz, N), plus(c, dc, CORES))

    def row_peer(dx, dy):
        return device(plus(x, dx, N), plus(y, dy, N), z, c)

    small = [
        pltpu.make_async_copy(a, b, lsem.at[4 + n])
        for n, (a, b) in enumerate(((ids_ref, idv), (slot_ref, slotv), (scale_ref, scale_s), (shift_ref, shift_s)))
    ]
    for load in small:
        load.start()
    load_ci = pltpu.make_async_copy(ci_hbm, civ, lsem.at[0])
    load_wi = pltpu.make_async_copy(wi_hbm, wiv, lsem.at[1])
    load_x = pltpu.make_async_copy(x_hbm, xv, lsem.at[2])
    load_wu = pltpu.make_async_copy(wu_hbm, wuv, lsem.at[3])
    for load in (load_ci, load_wi, load_x, load_wu):
        load.start()

    barrier = pltpu.get_barrier_semaphore()
    greeted = [row_peer(*d) for d in planes]
    greeted += [device(plus(x, dx, N), y, plus(z, dz, N), c) for dx in range(N) for dz in range(1, N)]
    greeted += [device(x, plus(y, dy, N), plus(z, dz, N), c) for dy in range(1, N) for dz in range(1, N)]
    greeted += [item_peer(*d) for d in item_peers if d[2]]
    for to in greeted:
        pl.semaphore_signal(barrier, inc=1, device_id=to, device_id_type=MESH)
    for load in small:
        load.wait()
    my_user_slot = user_slot(0, 0)
    rows = lax.broadcasted_iota(jnp.int32, (USERS, USERS), 0)
    lanes = lax.broadcasted_iota(jnp.int32, (USERS, USERS), 1)
    id_col = jnp.sum(jnp.where(rows == lanes, idv[...].astype(F32), 0.0), axis=1, keepdims=True)
    slot_col = jnp.sum(jnp.where(rows == lanes, slotv[...].astype(F32), 0.0), axis=1, keepdims=True)
    tile_rows = lax.broadcasted_iota(jnp.int32, (USERS, 128), 0)
    tile_lanes = lax.broadcasted_iota(jnp.int32, (USERS, 128), 1)
    idrow[0] = jnp.sum(jnp.where(tile_rows == tile_lanes, id_col, 0.0), axis=0, keepdims=True)
    wide_rows = lax.broadcasted_iota(jnp.int32, (USERS, NU * USERS), 0)
    wide_lanes = lax.broadcasted_iota(jnp.int32, (USERS, NU * USERS), 1)
    slotbuf[0] = jnp.sum(
        jnp.where(wide_lanes == wide_rows + my_user_slot * USERS, slot_col, 0.0), axis=0, keepdims=True
    )
    load_ci.wait()
    load_wi.wait()
    item_pre = dot(civ[...], wiv[...])
    item_len = jnp.sqrt(jnp.sum(item_pre * item_pre, axis=1, keepdims=True) + EPS)
    item_normed = item_pre / item_len
    inorm[...] = item_normed
    ilen[...] = jnp.broadcast_to(item_len, (USERS, 128))
    ia[0, 0] = item_normed.astype(BF16)
    pl.semaphore_wait(barrier, len(greeted))
    id_recv, slot_recv = [], []
    for n, d in enumerate(user_peers):
        slot_recv.append(send(slotbuf.at[0], slotbuf.at[n + 1], slot_s.at[n], slot_r.at[n], user_peer(*d)))
    for n, d in enumerate(item_peers):
        id_recv.append(send(idrow.at[0], idrow.at[item_slot(*d)], id_s.at[n], id_r.at[n], item_peer(*d)))
    ia_recv = []
    for n, d in enumerate(near_items):
        ia_recv.append(send(ia.at[0, 0], ia.at[0, item_slot(*d)], ia_s.at[n], ia_r.at[n], item_peer(*d)))
    load_x.wait()
    x_recv = []
    for q in range(QN):
        cols = pl.ds(pl.multiple_of((q * CORES + 1 - c) * FEAT, FEAT), FEAT)
        x_recv.append(send(xv.at[:, cols], xs.at[q], xsem_s.at[q], xsem_r.at[q], sibling))
    load_wu.wait()

    def pool(n, u):
        cols = pl.ds(pl.multiple_of(n * CW, CW), CW)
        v = pre[pl.ds(pl.multiple_of(u * 8 * HIST, 8 * HIST), 8 * HIST), cols]
        act = v * sigmoid(v)
        pooled[pl.ds(pl.multiple_of(u * 8, 8), 8), cols] = jnp.sum(act.reshape(8, HIST, CW), axis=1) / HIST

    def forward(n, _):
        for u in range(USERS // 8):
            pool(jnp.maximum(n - 1, 0), u)
        cols = pl.ds(pl.multiple_of(n * CW, CW), CW)
        pre[:, cols] = dot(xv[...], wuv[:, cols])
        return 0

    lax.fori_loop(0, COLOURS, forward, 0)
    def pool_last(u, _):
        pool(COLOURS - 1, u)
        return 0

    lax.fori_loop(0, USERS // 8, pool_last, 0)
    mean = pooled[...]
    user_len = jnp.sqrt(jnp.sum(mean * mean, axis=1, keepdims=True) + EPS)
    user_normed = mean / user_len
    ulen[...] = jnp.broadcast_to(user_len, (USERS, 128))
    pooled[...] = user_normed
    ua[my_user_slot] = user_normed.astype(BF16)
    ua_recv = []
    for n, d in enumerate(user_peers):
        ua_recv.append(send(ua.at[my_user_slot], ua.at[my_user_slot], ua_s.at[n], ua_r.at[n], user_peer(*d)))

    for copy in slot_recv + id_recv:
        copy.wait_recv()
    slots = slotbuf[0]
    for n in range(1, NU):
        slots = slots + slotbuf[n]
    wide = NU * USERS // 128
    found = jnp.zeros((1, NU * USERS), F32)
    for dc in range(CORES):
        for db in range(2):
            for dz in range(N):
                s = item_slot(db, dz, dc)
                col = jnp.sum(jnp.where(tile_rows == tile_lanes, idrow[s], 0.0), axis=1, keepdims=True)
                ids = jnp.broadcast_to(col, (USERS, 128))
                idbuf[s] = ids
                ob, og = item_owner(db, dz, dc)
                at = (tile_rows + (ob * (XL * N) + og) * USERS).astype(F32)
                hit = jnp.concatenate([at] * wide, axis=1) == slots
                found = found + jnp.sum(
                    jnp.where(hit, jnp.concatenate([ids] * wide, axis=1), 0.0), axis=0, keepdims=True
                )
    tgtbuf[0] = found
    tgt_recv = []
    for n, d in enumerate(user_peers):
        tgt_recv.append(send(tgtbuf.at[0], tgtbuf.at[n + 1], tgt_s.at[n], tgt_r.at[n], user_peer(*d)))

    xi_recv = []
    for n, (dz, dc) in enumerate(feat_peers):
        pz, pc = plus(z, dz, N), plus(c, dc, CORES)
        for h in range(XH):
            cols = pl.ds(pl.multiple_of(((h * N + pz) * CORES + pc) * FEAT, FEAT), FEAT)
            xi_recv.append(
                send(civ.at[:, cols], xi.at[h, dc * N + dz], xi_s.at[n, h], xi_r.at[n, h], item_peer(0, dz, dc))
            )
    for h in range(XH):
        xi[h, 0] = civ[:, pl.ds(pl.multiple_of(((h * N + z) * CORES + c) * FEAT, FEAT), FEAT)]
    for copy in ia_recv:
        copy.wait_recv()
    ia_hop = send(ia.at[0], ia.at[1], hop_s.at[0], hop_r.at[0], sibling)
    for copy in x_recv:
        copy.wait_recv()

    def turn(q, _):
        cols = pl.ds(pl.multiple_of((q * CORES + c) * FEAT, FEAT), FEAT)
        to = pl.ds(pl.multiple_of(q * FEAT, FEAT), FEAT)
        xt[to, 0:ROWS] = xv[:, cols].T
        xt[to, ROWS:2 * ROWS] = xs[q].T
        return 0

    lax.fori_loop(0, QN, turn, 0)
    for copy in tgt_recv:
        copy.wait_recv()
    targets = tgtbuf[0]
    for n in range(1, NU):
        targets = targets + tgtbuf[n]

    for copy in ua_recv:
        copy.wait_recv()
    ia_hop.wait_recv()
    scale = scale_s[0, 0]
    shift = shift_s[0, 0]
    users = ua[...].reshape(NU * USERS, E)
    loss = jnp.zeros((8, 128), F32)
    for n in range(NI // N):
        items = ia[n // 2, (n % 2) * N:(n % 2 + 1) * N].reshape(N * USERS, E)
        scores = dot_nt(items, users)
        ids = idbuf[n * N:(n + 1) * N].reshape(N * USERS, 128)
        sign = jnp.where(jnp.concatenate([ids] * wide, axis=1) == targets, 1.0, -1.0)
        margin = sign * (scale * scores + shift)
        e = jnp.exp(-jnp.abs(margin))
        terms = jnp.log1p(e) + jnp.maximum(-margin, 0.0)
        gate = jnp.where(margin >= 0.0, e, 1.0) / (1.0 + e)
        wt[n * N * USERS:(n + 1) * N * USERS, :] = (-scale * sign * gate).astype(BF16)
        terms = jnp.sum(terms.reshape(N * USERS // 8, 8, NU * USERS), axis=0)
        for j in range(wide):
            loss = loss + terms[:, j * 128:(j + 1) * 128]
    def reduce_loss(value, step, pos):
        losses[step, pos] = value
        copies = []
        for d in range(1, N):
            at = [x, y, z]
            at[step] = plus(pos, d, N)
            copies.append(
                send(losses.at[step, pos], losses.at[step, pos], lo_s.at[step, d - 1], lo_r.at[step, d - 1],
                     device(at[0], at[1], at[2], c))
            )
        return copies

    def reduced_loss(step):
        total = losses[step, 0]
        for d in range(1, N):
            total = total + losses[step, d]
        return total

    loss_copies = reduce_loss(loss, 0, x)
    pgu[...] = dot_t(wt[...], ia[...].reshape(NI * USERS, E)).astype(BF16).reshape(NU, USERS, E)
    ug_recv = []
    for n, d in enumerate(user_peers):
        ug_recv.append(send(pgu.at[user_slot(*d)], rgu.at[n], ug_s.at[n], ug_r.at[n], user_peer(*d)))
    pig[1] = dot(wt[NS * USERS:2 * NS * USERS, :], users).astype(BF16).reshape(NS, USERS, E)
    ig_hop = send(pig.at[1], rigc, hop_s.at[1], hop_r.at[1], sibling)
    pigf[...] = dot(wt[0:NS * USERS, :], users).reshape(NS, USERS, E)
    ig_hop.wait_recv()
    ig_recv = []
    for s in range(NS):
        pigf[s] = pigf[s] + rigc[s].astype(F32)
        if s > 0:
            pig[0, s] = pigf[s].astype(BF16)
    for n, d in enumerate(near_items):
        ig_recv.append(send(pig.at[0, item_slot(*d)], rig.at[n], ig_s.at[n], ig_r.at[n], item_owner(*d)))

    for copy in ug_recv:
        copy.wait_recv()
    grad_users = pgu[my_user_slot].astype(F32)
    for n in range(len(user_peers)):
        grad_users = grad_users + rgu[n].astype(F32)
    user_normed = pooled[...]
    radial = jnp.sum(user_normed * grad_users, axis=1, keepdims=True)
    gp[...] = (grad_users - user_normed * radial) / ulen[:, 0:1] / HIST

    pos = (x, y, z)

    def backward(m, _):
        k = jnp.where(m < 2, 1 - m, m)
        cols = pl.ds(pl.multiple_of(k * CW, CW), CW)

        def step(u, _):
            at = pl.ds(pl.multiple_of(u * 8 * HIST, 8 * HIST), 8 * HIST)
            v = pre[at, cols]
            s = sigmoid(v)
            outer = jnp.broadcast_to(gp[pl.ds(pl.multiple_of(u * 8, 8), 8), cols][:, None, :], (8, HIST, CW))
            g[k, at] = (outer.reshape(8 * HIST, CW) * s * (1.0 + v * (1.0 - s))).astype(BF16)
            to = pl.ds(pl.multiple_of(ROWS + u * 8 * HIST, 8 * HIST), 8 * HIST)
            pltpu.make_async_remote_copy(
                src_ref=g.at[k, at], dst_ref=g.at[k, to], send_sem=g_s.at[k, u], recv_sem=g_r.at[k, u],
                device_id=sibling, device_id_type=MESH,
            ).start()
            return 0

        lax.fori_loop(0, USERS // 8, step, 0)
        return 0

    def towards(axis, v):
        at = list(pos)
        at[axis] = v
        return device(at[0], at[1], at[2], c)

    def item_home():
        for copy in ig_recv:
            copy.wait_recv()
        item_grad = pigf[0]
        for n in range(len(near_items)):
            item_grad = item_grad + rig[n].astype(F32)
        ig_ref[...] = item_grad
        item_normed = inorm[...]
        radial = jnp.sum(item_normed * item_grad, axis=1, keepdims=True)
        gi[0, 0] = ((item_grad - item_normed * radial) / ilen[:, 0:1]).astype(BF16)
        gi_hand(0)
        for d in steps:
            pltpu.make_async_remote_copy(
                src_ref=gi.at[0, 0], dst_ref=gi.at[0, d], send_sem=gi_s.at[d], recv_sem=gi_r.at[d],
                device_id=item_peer(0, d, 0), device_id_type=MESH,
            ).start()

    def gi_hand(d):
        pltpu.make_async_remote_copy(
            src_ref=gi.at[0, d], dst_ref=gi.at[1, d], send_sem=gh_s.at[d], recv_sem=gh_r.at[d],
            device_id=sibling, device_id_type=MESH,
        ).start()

    def weight_grad(m, _):
        k = jnp.where(m < 2, 1 - m, m)
        pl.when(m == 1)(item_home)
        for u in range(USERS // 8):
            arrived(g.at[k, pl.ds(ROWS + u * 8 * HIST, 8 * HIST)], g_r.at[k, u])
        part[k] = dot(xt[...], g[k]).astype(BF16).reshape(XH, N, XL, N, 16, CW)
        for axis in range(COLOURS):

            @pl.when(k == axis)
            def _(axis=axis):
                for d in steps:
                    t = plus(pos[axis], d, N)
                    pltpu.make_async_remote_copy(
                        src_ref=slab(axis, t), dst_ref=ra[axis].at[d - 1], send_sem=ra_s.at[axis, d - 1],
                        recv_sem=ra_r.at[axis, d - 1], device_id=towards(axis, t), device_id_type=MESH,
                    ).start()

        return 0

    ra = (ra0, ra1, ra2)

    def slab(axis, t):
        if axis == 0:
            return part.at[0, t // XL, :, lax.rem(t, XL)]
        if axis == 1:
            return part.at[1, :, :, :, t]
        return part.at[2, :, t]

    lax.fori_loop(0, COLOURS, backward, 0)
    for copy in loss_copies:
        copy.wait_recv()
    loss_copies = reduce_loss(reduced_loss(0), 1, y)
    lax.fori_loop(0, COLOURS, weight_grad, 0)
    for copy in loss_copies:
        copy.wait_recv()
    loss_copies = reduce_loss(reduced_loss(1), 2, z)
    flight = {}

    def add_a(k):
        for d in range(N - 1):
            arrived(ra[k].at[d], ra_r.at[k, d])
        p1, p2 = pos[(k + 1) % 3], pos[(k + 2) % 3]
        flight[k] = []
        for n, (di, dj) in enumerate(planes + [(0, 0)]):
            i, j = plus(p1, di, N), plus(p2, dj, N)
            if k == 0:
                own, got = part.at[0, x // XL, j, lax.rem(x, XL), i], lambda d: ra0[d, j, i]
            elif k == 1:
                own, got = part.at[1, j // XL, i, lax.rem(j, XL), y], lambda d: ra1[d, j // XL, i, lax.rem(j, XL)]
            else:
                own, got = part.at[2, i // XL, z, lax.rem(i, XL), j], lambda d: ra2[d, i // XL, lax.rem(i, XL), j]
            total = own[...].astype(F32)
            for d in range(N - 1):
                total = total + got(d).astype(F32)
            sa[k, n] = total.astype(BF16)
            if (di, dj) != (0, 0):
                at = list(pos)
                at[(k + 1) % 3], at[(k + 2) % 3] = i, j
                to = device(at[0], at[1], at[2], c)
                flight[k].append(send(sa.at[k, n], rb.at[k, n], rs_s.at[k, n], rs_r.at[k, n], to))

    def add_b(k):
        for copy in flight[k]:
            copy.wait_recv()
        total = sa[k, len(planes)].astype(F32)
        for n in range(len(planes)):
            total = total + rb[k, n].astype(F32)
        gu_ref[:, k * CW:(k + 1) * CW] = total

    for d in reversed(steps):
        arrived(gi.at[0, d], gi_r.at[d])
        gi_hand(d)
    for copy in xi_recv:
        copy.wait_recv()
    for d in range(N):
        arrived(gi.at[1, d], gh_r.at[d])
    for h in range(XH):
        r = dot_t(xi[h].reshape(N * CORES * USERS, FEAT), gi[...].reshape(N * CORES * USERS, E)).astype(BF16)
        parti[h * XL:(h + 1) * XL] = r.reshape(XL, N, 16, E)
    left_half, right_half = pl.ds(0, E // 2), pl.ds(E // 2, E // 2)
    ri_recv = []
    for d in steps:
        t = plus(x, d, N)
        src = parti.at[t, :, :, left_half]
        ri_recv.append(send(src, ri.at[0, d - 1], ri_s.at[0, d - 1], ri_r.at[0, d - 1], towards(0, t)))
        t = plus(y, d, N)
        src = parti.at[:, t, :, right_half]
        ri_recv.append(send(src, ri.at[1, d - 1], ri_s.at[1, d - 1], ri_r.at[1, d - 1], towards(1, t)))
    add_a(1)
    add_a(0)
    add_a(2)
    for copy in ri_recv:
        copy.wait_recv()
    for n in range(N):
        total = parti[x, n, :, 0:E // 2].astype(F32)
        for d in range(N - 1):
            total = total + ri[0, d, n].astype(F32)
        si[0, n] = total.astype(BF16)
        total = parti[n, y, :, E // 2:E].astype(F32)
        for d in range(N - 1):
            total = total + ri[1, d, n].astype(F32)
        si[1, n] = total.astype(BF16)
    ri_recv = []
    for h in range(2):
        for d in steps:
            t = plus(pos[1 - h], d, N)
            ri_recv.append(send(si.at[h, t], rj.at[h, d - 1], rj_s.at[h, d - 1], rj_r.at[h, d - 1], towards(1 - h, t)))
    for copy in loss_copies:
        copy.wait_recv()
    corelosses[c] = reduced_loss(2)
    core_copy = send(corelosses.at[c], corelosses.at[c], hop_s.at[3], hop_r.at[3], sibling)
    for copy in sent:
        copy.wait_send()
    for k in range(COLOURS):
        for u in range(USERS // 8):
            left(g.at[k, pl.ds(u * 8 * HIST, 8 * HIST)], g_s.at[k, u])
        for d in range(N - 1):
            left(ra[k].at[d], ra_s.at[k, d])
    for d in range(N):
        left(gi.at[0, d], gh_s.at[d])
        if d:
            left(gi.at[0, 0], gi_s.at[d])
    add_b(1)
    add_b(0)
    core_copy.wait_recv()
    loss_ref[...] = jnp.broadcast_to(jnp.sum(corelosses[0] + corelosses[1], keepdims=True) / TOTAL, (8, 128))
    for copy in ri_recv:
        copy.wait_recv()
    for h in range(2):
        total = si[h, pos[1 - h]].astype(F32)
        for d in range(N - 1):
            total = total + rj[h, d].astype(F32)
        gi_ref[:, h * (E // 2):(h + 1) * (E // 2)] = total
    add_b(2)


def hand_out(loss, ig, gu, gi, loss_out, ig_out, gu_out, gi_out):
    loss_out[0] = loss[0, 0]
    ig_out[...] = ig[...]
    gu_out[...] = gu[...]
    gi_out[...] = gi[...]


def shards(N, XL, past, cand, wu, wi, scale, shift, ids, slots):
    users, hist, depth = past.shape
    E = wu.shape[1]
    total = users * lax.axis_size("blk") * lax.axis_size("group")
    NU, NI, NS, QN = XL * N, XL * N * CORES, XL * N, (N // XL) * N
    feat = depth // (QN * CORES)
    hbm = pl.BlockSpec(memory_space=pltpu.HBM)
    smem = pl.BlockSpec(memory_space=pltpu.SMEM)
    vmem = pl.BlockSpec(memory_space=pltpu.VMEM)
    rows = depth // (N * N * N * CORES)
    CW = E // COLOURS

    def dma(*shape):
        return pltpu.SemaphoreType.DMA(shape)

    V = pltpu.VMEM
    scratch = [
        V((users * hist, depth), BF16), V((QN, users * hist, feat), BF16),
        V((users, depth), BF16),
        V((depth, E), BF16), V((depth, E), BF16),
        V((users * hist, E), F32), V((users, E), F32), V((users, E), F32), V((users, 128), F32),
        V((users, E), F32), V((users, 128), F32),
        V((NU, users, E), BF16), V((CORES, NS, users, E), BF16), V((NI, 1, 128), F32), V((NI, users, 128), F32),
        V((NU, 1, NU * users), F32), V((NU, 1, NU * users), F32),
        V((NI * users, NU * users), BF16),
        V((CORES, NS, users, E), BF16), V((NS, users, E), F32), V((NS, users, E), BF16),
        V((NS - 1, users, E), BF16),
        V((NU, users, E), BF16), V((NU - 1, users, E), BF16),
        V((COLOURS, 2 * users * hist, CW), BF16), V((CORES, N, users, E), BF16),
        V((N // XL, N * CORES, users, feat), BF16), V((QN * feat, 2 * users * hist), BF16),
        V((COLOURS, N // XL, N, XL, N, rows, CW), BF16), V((N - 1, N, N, rows, CW), BF16),
        V((N - 1, N // XL, N, XL, rows, CW), BF16), V((N - 1, N // XL, XL, N, rows, CW), BF16),
        V((COLOURS, N * N, rows, CW), BF16), V((COLOURS, N * N - 1, rows, CW), BF16),
        V((N, N, rows, E), BF16), V((2, N - 1, N, rows, E // 2), BF16),
        V((2, N, rows, E // 2), BF16), V((2, N - 1, rows, E // 2), BF16),
        V((3, N, 8, 128), F32), V((CORES, 8, 128), F32),
        V((1, 1), F32), V((1, 1), F32), V((1, users), jnp.int32), V((1, users), jnp.int32),
        dma(8), dma(QN), dma(QN), dma(N * CORES - 1, N // XL), dma(N * CORES - 1, N // XL),
        dma(NI - 1), dma(NI - 1), dma(NU - 1), dma(NU - 1), dma(NU - 1), dma(NU - 1),
        dma(NS - 1), dma(NS - 1), dma(NU - 1), dma(NU - 1),
        dma(NS - 1), dma(NS - 1), dma(NU - 1), dma(NU - 1), dma(COLOURS, users // 8), dma(COLOURS, users // 8), dma(N), dma(N), dma(N), dma(N),
        dma(COLOURS, N - 1), dma(COLOURS, N - 1), dma(COLOURS, N * N - 1), dma(COLOURS, N * N - 1),
        dma(2, N - 1), dma(2, N - 1), dma(2, N - 1), dma(2, N - 1), dma(3, N - 1), dma(3, N - 1), dma(4), dma(4),
    ]
    outs = pl.pallas_call(
        functools.partial(tower_kernel, N, XL, total),
        name="two_tower",
        out_shape=(
            pltpu.VMEM((8, 128), F32),
            pltpu.VMEM((users, E), F32),
            pltpu.VMEM((rows, E), F32),
            pltpu.VMEM((rows, E), F32),
        ),
        in_specs=[hbm] * 8,
        out_specs=(vmem,) * 4,
        scratch_shapes=scratch,
        compiler_params=pltpu.CompilerParams(
            collective_id=0, has_side_effects=True, vmem_limit_bytes=60 * 1024 * 1024
        ),
    )(
        past.reshape(users * hist, depth), cand, wu, wi, scale.reshape(1, 1), shift.reshape(1, 1),
        ids.reshape(1, users), slots.reshape(1, users),
    )
    return pl.pallas_call(
        hand_out,
        name="hand_out",
        out_shape=(
            jax.ShapeDtypeStruct((1,), F32),
            jax.ShapeDtypeStruct((users, E), F32),
            jax.ShapeDtypeStruct((rows, E), F32),
            jax.ShapeDtypeStruct((rows, E), F32),
        ),
        in_specs=[vmem] * 4,
        out_specs=(smem, vmem, vmem, vmem),
        compiler_params=pltpu.CompilerParams(vmem_limit_bytes=4 * 1024 * 1024),
    )(*outs)


def solution(mesh):
    group = mesh.shape["group"]
    n = {128: 4, 16: 2}[mesh.size]
    both = ("blk", "group")
    return jax.shard_map(
        functools.partial(shards, n, group // n),
        mesh=mesh,
        in_specs=(P(both, None, None), P(both, None), P(), P(), P(), P(), P(both), P(both)),
        out_specs=(P(), P(both, None), P(both, None), P(both, None)),
        check_vma=False,
    )
```

```python
import functools

import jax
import jax.numpy as jnp
from jax import lax
from jax.experimental import pallas as pl
from jax.experimental.pallas import tpu as pltpu
from jax.sharding import PartitionSpec as P

EPS = 1e-06
MESH = pl.DeviceIdType.MESH
F32 = jnp.float32
BF16 = jnp.bfloat16
CORES = 2
COLOURS = 3


def dot(a, b):
    return jnp.dot(a, b, preferred_element_type=F32)


def dot_t(a, b):
    return lax.dot_general(a, b, (((0,), (0,)), ((), ())), preferred_element_type=F32)


def dot_nt(a, b):
    return lax.dot_general(a, b, (((1,), (1,)), ((), ())), preferred_element_type=F32)


def sigmoid(v):
    return 0.5 + 0.5 * jnp.tanh(0.5 * v)


def tower_kernel(
    N, XL, TOTAL,
    x_hbm, ci_hbm, wu_hbm, wi_hbm, scale_ref, shift_ref, ids_ref, slot_ref,
    loss_ref, ig_ref, gu_ref, gi_ref,
    xv, xs, civ, wuv, wiv, pre, pooled, gp, ulen, inorm, ilen,
    ua, ia, idrow, idbuf, slotbuf, tgtbuf, sc, wt, pig, pigf, rigc, rig, pgu, rgu, g, gi, xi, xt,
    part, ra0, ra1, ra2, sa, rb, parti, ri, si, rj, losses, corelosses, scale_s, shift_s, idv, slotv,
    lsem, xsem_s, xsem_r, xi_s, xi_r, id_s, id_r, slot_s, slot_r, tgt_s, tgt_r,
    ia_s, ia_r, ua_s, ua_r, ig_s, ig_r, ug_s, ug_r, g_s, g_r, gi_s, gi_r, gh_s, gh_r,
    ra_s, ra_r, rs_s, rs_r, ri_s, ri_r, rj_s, rj_r, lo_s, lo_r, hop_s, hop_r,
):
    USERS, E = pooled.shape
    HIST = xv.shape[0] // USERS
    FEAT = 128 if N == 4 else XL * N * 16
    QN = (N // XL) * N
    NU = XL * N
    NI = XL * N * CORES
    NS = XL * N
    CW = E // COLOURS
    XH = N // XL
    ROWS = USERS * HIST
    blk = lax.axis_index("blk")
    group = lax.axis_index("group")
    c = lax.rem(blk, CORES)
    z = lax.rem(blk // CORES, N)
    x = (blk // (CORES * N)) * XL + group // N
    y = lax.rem(group, N)
    odd = lax.rem(x, 2)
    pair_a = x + 1 - 2 * odd
    pair_b = lax.rem(x + N - 1 + 2 * odd, N)

    def device(px, py, pz, pc):
        return (((px // XL) * N + pz) * CORES + pc, lax.rem(px, XL) * N + py)

    def plus(v, d, n):
        return v if d == 0 else lax.rem(v + d, n)

    def minus(v, d, n):
        return v if d == 0 else lax.rem(v + n - d, n)

    def send(src, dst, ssem, rsem, to):
        copy = pltpu.make_async_remote_copy(
            src_ref=src, dst_ref=dst, send_sem=ssem, recv_sem=rsem, device_id=to, device_id_type=MESH
        )
        copy.start()
        sent.append(copy)
        return copy

    def arrived(dst, sem):
        pltpu.make_async_remote_copy(
            src_ref=dst, dst_ref=dst, send_sem=sem, recv_sem=sem, device_id=sibling, device_id_type=MESH
        ).wait_recv()

    def left(src, sem):
        pltpu.make_async_remote_copy(
            src_ref=src, dst_ref=src, send_sem=sem, recv_sem=sem, device_id=sibling, device_id_type=MESH
        ).wait_send()

    sent = []
    sibling = device(x, y, z, 1 - c)
    def ring(d):
        return min(d, N - d)

    span = range(N)
    user_peers = [(da, dy) for da in range(2) for dy in span if (da, dy) != (0, 0)]
    user_peers.sort(key=lambda p: -p[0] - ring(p[1]))
    near_items = [(db, dz, 0) for db in range(2) for dz in span if (db, dz) != (0, 0)]
    near_items.sort(key=lambda p: -p[0] - ring(p[1]))
    item_peers = near_items + [(db, dz, 1) for db in range(2) for dz in span]
    planes = [(di, dj) for di in span for dj in span if (di, dj) != (0, 0)]
    planes.sort(key=lambda p: -ring(p[0]) - ring(p[1]))
    feat_peers = [(dz, dc) for dc in range(CORES) for dz in span if (dz, dc) != (0, 0)]
    steps = sorted(range(1, N), key=lambda d: -ring(d))

    def user_peer(da, dy):
        return device(pair_a if da else x, plus(y, dy, N), z, c)

    def user_slot(da, dy):
        return (1 - odd if da else odd) * N + plus(y, dy, N)

    def item_slot(db, dz, dc):
        return dc * NS + db * N + dz

    def item_peer(db, dz, dc):
        return device(pair_b if db else x, y, plus(z, dz, N), plus(c, dc, CORES))

    def item_owner(db, dz, dc):
        return device(pair_b if db else x, y, minus(z, dz, N), plus(c, dc, CORES))

    def row_peer(dx, dy):
        return device(plus(x, dx, N), plus(y, dy, N), z, c)

    small = [
        pltpu.make_async_copy(a, b, lsem.at[4 + n])
        for n, (a, b) in enumerate(((ids_ref, idv), (slot_ref, slotv), (scale_ref, scale_s), (shift_ref, shift_s)))
    ]
    for load in small:
        load.start()
    load_ci = pltpu.make_async_copy(ci_hbm, civ, lsem.at[0])
    load_wi = pltpu.make_async_copy(wi_hbm, wiv, lsem.at[1])
    load_x = pltpu.make_async_copy(x_hbm, xv, lsem.at[2])
    load_wu = pltpu.make_async_copy(wu_hbm, wuv, lsem.at[3])
    for load in (load_ci, load_wi, load_x, load_wu):
        load.start()

    barrier = pltpu.get_barrier_semaphore()
    greeted = [row_peer(*d) for d in planes]
    greeted += [device(plus(x, dx, N), y, plus(z, dz, N), c) for dx in range(N) for dz in range(1, N)]
    greeted += [device(x, plus(y, dy, N), plus(z, dz, N), c) for dy in range(1, N) for dz in range(1, N)]
    greeted += [item_peer(*d) for d in item_peers if d[2]]
    for to in greeted:
        pl.semaphore_signal(barrier, inc=1, device_id=to, device_id_type=MESH)
    for load in small:
        load.wait()
    my_user_slot = user_slot(0, 0)
    rows = lax.broadcasted_iota(jnp.int32, (USERS, USERS), 0)
    lanes = lax.broadcasted_iota(jnp.int32, (USERS, USERS), 1)
    id_col = jnp.sum(jnp.where(rows == lanes, idv[...].astype(F32), 0.0), axis=1, keepdims=True)
    slot_col = jnp.sum(jnp.where(rows == lanes, slotv[...].astype(F32), 0.0), axis=1, keepdims=True)
    tile_rows = lax.broadcasted_iota(jnp.int32, (USERS, 128), 0)
    tile_lanes = lax.broadcasted_iota(jnp.int32, (USERS, 128), 1)
    idrow[0] = jnp.sum(jnp.where(tile_rows == tile_lanes, id_col, 0.0), axis=0, keepdims=True)
    wide_rows = lax.broadcasted_iota(jnp.int32, (USERS, NU * USERS), 0)
    wide_lanes = lax.broadcasted_iota(jnp.int32, (USERS, NU * USERS), 1)
    slotbuf[0] = jnp.sum(
        jnp.where(wide_lanes == wide_rows + my_user_slot * USERS, slot_col, 0.0), axis=0, keepdims=True
    )
    load_ci.wait()
    load_wi.wait()
    item_pre = dot(civ[...], wiv[...])
    item_len = jnp.sqrt(jnp.sum(item_pre * item_pre, axis=1, keepdims=True) + EPS)
    item_normed = item_pre / item_len
    inorm[...] = item_normed
    ilen[...] = jnp.broadcast_to(item_len, (USERS, 128))
    ia[0, 0] = item_normed.astype(BF16)
    pl.semaphore_wait(barrier, len(greeted))
    id_recv, slot_recv = [], []
    for n, d in enumerate(user_peers):
        slot_recv.append(send(slotbuf.at[0], slotbuf.at[n + 1], slot_s.at[n], slot_r.at[n], user_peer(*d)))
    for n, d in enumerate(item_peers):
        id_recv.append(send(idrow.at[0], idrow.at[item_slot(*d)], id_s.at[n], id_r.at[n], item_peer(*d)))
    ia_recv = []
    for n, d in enumerate(near_items):
        ia_recv.append(send(ia.at[0, 0], ia.at[0, item_slot(*d)], ia_s.at[n], ia_r.at[n], item_peer(*d)))
    load_x.wait()
    x_recv = []
    for q in range(QN):
        cols = pl.ds(pl.multiple_of((q * CORES + 1 - c) * FEAT, FEAT), FEAT)
        x_recv.append(send(xv.at[:, cols], xs.at[q], xsem_s.at[q], xsem_r.at[q], sibling))
    load_wu.wait()

    def pool(n, u):
        cols = pl.ds(pl.multiple_of(n * CW, CW), CW)
        v = pre[pl.ds(pl.multiple_of(u * 8 * HIST, 8 * HIST), 8 * HIST), cols]
        act = v * sigmoid(v)
        pooled[pl.ds(pl.multiple_of(u * 8, 8), 8), cols] = jnp.sum(act.reshape(8, HIST, CW), axis=1) / HIST

    def forward(n, _):
        for u in range(USERS // 8):
            pool(jnp.maximum(n - 1, 0), u)
        cols = pl.ds(pl.multiple_of(n * CW, CW), CW)
        pre[:, cols] = dot(xv[...], wuv[:, cols])
        return 0

    lax.fori_loop(0, COLOURS, forward, 0)
    def pool_last(u, _):
        pool(COLOURS - 1, u)
        return 0

    lax.fori_loop(0, USERS // 8, pool_last, 0)
    mean = pooled[...]
    user_len = jnp.sqrt(jnp.sum(mean * mean, axis=1, keepdims=True) + EPS)
    user_normed = mean / user_len
    ulen[...] = jnp.broadcast_to(user_len, (USERS, 128))
    pooled[...] = user_normed
    ua[my_user_slot] = user_normed.astype(BF16)
    ua_recv = []
    for n, d in enumerate(user_peers):
        ua_recv.append(send(ua.at[my_user_slot], ua.at[my_user_slot], ua_s.at[n], ua_r.at[n], user_peer(*d)))

    for copy in slot_recv + id_recv:
        copy.wait_recv()
    slots = slotbuf[0]
    for n in range(1, NU):
        slots = slots + slotbuf[n]
    wide = NU * USERS // 128
    found = jnp.zeros((1, NU * USERS), F32)
    for dc in range(CORES):
        for db in range(2):
            for dz in range(N):
                s = item_slot(db, dz, dc)
                col = jnp.sum(jnp.where(tile_rows == tile_lanes, idrow[s], 0.0), axis=1, keepdims=True)
                ids = jnp.broadcast_to(col, (USERS, 128))
                idbuf[s] = ids
                ob, og = item_owner(db, dz, dc)
                at = (tile_rows + (ob * (XL * N) + og) * USERS).astype(F32)
                hit = jnp.concatenate([at] * wide, axis=1) == slots
                found = found + jnp.sum(
                    jnp.where(hit, jnp.concatenate([ids] * wide, axis=1), 0.0), axis=0, keepdims=True
                )
    tgtbuf[0] = found
    tgt_recv = []
    for n, d in enumerate(user_peers):
        tgt_recv.append(send(tgtbuf.at[0], tgtbuf.at[n + 1], tgt_s.at[n], tgt_r.at[n], user_peer(*d)))

    xi_recv = []
    for n, (dz, dc) in enumerate(feat_peers):
        pz, pc = plus(z, dz, N), plus(c, dc, CORES)
        for h in range(XH):
            cols = pl.ds(pl.multiple_of(((h * N + pz) * CORES + pc) * FEAT, FEAT), FEAT)
            xi_recv.append(
                send(civ.at[:, cols], xi.at[h, dc * N + dz], xi_s.at[n, h], xi_r.at[n, h], item_peer(0, dz, dc))
            )
    for h in range(XH):
        xi[h, 0] = civ[:, pl.ds(pl.multiple_of(((h * N + z) * CORES + c) * FEAT, FEAT), FEAT)]
    for copy in ia_recv:
        copy.wait_recv()
    ia_hop = send(ia.at[0], ia.at[1], hop_s.at[0], hop_r.at[0], sibling)
    for copy in x_recv:
        copy.wait_recv()

    def turn(q, _):
        cols = pl.ds(pl.multiple_of((q * CORES + c) * FEAT, FEAT), FEAT)
        to = pl.ds(pl.multiple_of(q * FEAT, FEAT), FEAT)
        xt[to, 0:ROWS] = xv[:, cols].T
        xt[to, ROWS:2 * ROWS] = xs[q].T
        return 0

    lax.fori_loop(0, QN, turn, 0)
    for copy in ua_recv:
        copy.wait_recv()
    ia_hop.wait_recv()
    users = ua[...].reshape(NU * USERS, E)
    for n in range(NI // N):
        items = ia[n // 2, (n % 2) * N:(n % 2 + 1) * N].reshape(N * USERS, E)
        sc[n * N * USERS:(n + 1) * N * USERS, :] = dot_nt(items, users)
    for copy in tgt_recv:
        copy.wait_recv()
    targets = tgtbuf[0]
    for n in range(1, NU):
        targets = targets + tgtbuf[n]

    scale = scale_s[0, 0]
    shift = shift_s[0, 0]
    loss = jnp.zeros((8, 128), F32)
    for n in range(NI // N):
        scores = sc[n * N * USERS:(n + 1) * N * USERS, :]
        ids = idbuf[n * N:(n + 1) * N].reshape(N * USERS, 128)
        sign = jnp.where(jnp.concatenate([ids] * wide, axis=1) == targets, 1.0, -1.0)
        margin = sign * (scale * scores + shift)
        e = jnp.exp(-jnp.abs(margin))
        terms = jnp.log1p(e) + jnp.maximum(-margin, 0.0)
        gate = jnp.where(margin >= 0.0, e, 1.0) / (1.0 + e)
        wt[n * N * USERS:(n + 1) * N * USERS, :] = (-scale * sign * gate).astype(BF16)
        terms = jnp.sum(terms.reshape(N * USERS // 8, 8, NU * USERS), axis=0)
        for j in range(wide):
            loss = loss + terms[:, j * 128:(j + 1) * 128]
    def reduce_loss(value, step, pos):
        losses[step, pos] = value
        copies = []
        for d in range(1, N):
            at = [x, y, z]
            at[step] = plus(pos, d, N)
            copies.append(
                send(losses.at[step, pos], losses.at[step, pos], lo_s.at[step, d - 1], lo_r.at[step, d - 1],
                     device(at[0], at[1], at[2], c))
            )
        return copies

    def reduced_loss(step):
        total = losses[step, 0]
        for d in range(1, N):
            total = total + losses[step, d]
        return total

    loss_copies = reduce_loss(loss, 0, x)
    pgu[...] = dot_t(wt[...], ia[...].reshape(NI * USERS, E)).astype(BF16).reshape(NU, USERS, E)
    ug_recv = []
    for n, d in enumerate(user_peers):
        ug_recv.append(send(pgu.at[user_slot(*d)], rgu.at[n], ug_s.at[n], ug_r.at[n], user_peer(*d)))
    pig[1] = dot(wt[NS * USERS:2 * NS * USERS, :], users).astype(BF16).reshape(NS, USERS, E)
    ig_hop = send(pig.at[1], rigc, hop_s.at[1], hop_r.at[1], sibling)
    pigf[...] = dot(wt[0:NS * USERS, :], users).reshape(NS, USERS, E)
    ig_hop.wait_recv()
    ig_recv = []
    for s in range(NS):
        pigf[s] = pigf[s] + rigc[s].astype(F32)
        if s > 0:
            pig[0, s] = pigf[s].astype(BF16)
    for n, d in enumerate(near_items):
        ig_recv.append(send(pig.at[0, item_slot(*d)], rig.at[n], ig_s.at[n], ig_r.at[n], item_owner(*d)))

    for copy in ug_recv:
        copy.wait_recv()
    grad_users = pgu[my_user_slot].astype(F32)
    for n in range(len(user_peers)):
        grad_users = grad_users + rgu[n].astype(F32)
    user_normed = pooled[...]
    radial = jnp.sum(user_normed * grad_users, axis=1, keepdims=True)
    gp[...] = (grad_users - user_normed * radial) / ulen[:, 0:1] / HIST

    pos = (x, y, z)

    def backward(m, _):
        k = jnp.where(m < 2, 1 - m, m)
        cols = pl.ds(pl.multiple_of(k * CW, CW), CW)

        def step(u, _):
            at = pl.ds(pl.multiple_of(u * 8 * HIST, 8 * HIST), 8 * HIST)
            v = pre[at, cols]
            s = sigmoid(v)
            outer = jnp.broadcast_to(gp[pl.ds(pl.multiple_of(u * 8, 8), 8), cols][:, None, :], (8, HIST, CW))
            g[k, at] = (outer.reshape(8 * HIST, CW) * s * (1.0 + v * (1.0 - s))).astype(BF16)
            to = pl.ds(pl.multiple_of(ROWS + u * 8 * HIST, 8 * HIST), 8 * HIST)
            pltpu.make_async_remote_copy(
                src_ref=g.at[k, at], dst_ref=g.at[k, to], send_sem=g_s.at[k, u], recv_sem=g_r.at[k, u],
                device_id=sibling, device_id_type=MESH,
            ).start()
            return 0

        lax.fori_loop(0, USERS // 8, step, 0)
        return 0

    def towards(axis, v):
        at = list(pos)
        at[axis] = v
        return device(at[0], at[1], at[2], c)

    def item_home():
        for copy in ig_recv:
            copy.wait_recv()
        item_grad = pigf[0]
        for n in range(len(near_items)):
            item_grad = item_grad + rig[n].astype(F32)
        ig_ref[...] = item_grad
        item_normed = inorm[...]
        radial = jnp.sum(item_normed * item_grad, axis=1, keepdims=True)
        gi[0, 0] = ((item_grad - item_normed * radial) / ilen[:, 0:1]).astype(BF16)
        gi_hand(0)
        for d in steps:
            pltpu.make_async_remote_copy(
                src_ref=gi.at[0, 0], dst_ref=gi.at[0, d], send_sem=gi_s.at[d], recv_sem=gi_r.at[d],
                device_id=item_peer(0, d, 0), device_id_type=MESH,
            ).start()

    def gi_hand(d):
        pltpu.make_async_remote_copy(
            src_ref=gi.at[0, d], dst_ref=gi.at[1, d], send_sem=gh_s.at[d], recv_sem=gh_r.at[d],
            device_id=sibling, device_id_type=MESH,
        ).start()

    def weight_grad(m, _):
        k = jnp.where(m < 2, 1 - m, m)
        pl.when(m == 1)(item_home)
        for u in range(USERS // 8):
            arrived(g.at[k, pl.ds(ROWS + u * 8 * HIST, 8 * HIST)], g_r.at[k, u])
        part[k] = dot(xt[...], g[k]).astype(BF16).reshape(XH, N, XL, N, 16, CW)
        for axis in range(COLOURS):

            @pl.when(k == axis)
            def _(axis=axis):
                for d in steps:
                    t = plus(pos[axis], d, N)
                    pltpu.make_async_remote_copy(
                        src_ref=slab(axis, t), dst_ref=ra[axis].at[d - 1], send_sem=ra_s.at[axis, d - 1],
                        recv_sem=ra_r.at[axis, d - 1], device_id=towards(axis, t), device_id_type=MESH,
                    ).start()

        return 0

    ra = (ra0, ra1, ra2)

    def slab(axis, t):
        if axis == 0:
            return part.at[0, t // XL, :, lax.rem(t, XL)]
        if axis == 1:
            return part.at[1, :, :, :, t]
        return part.at[2, :, t]

    lax.fori_loop(0, COLOURS, backward, 0)
    for copy in loss_copies:
        copy.wait_recv()
    loss_copies = reduce_loss(reduced_loss(0), 1, y)
    lax.fori_loop(0, COLOURS, weight_grad, 0)
    for copy in loss_copies:
        copy.wait_recv()
    loss_copies = reduce_loss(reduced_loss(1), 2, z)
    flight = {}

    def add_a(k):
        for d in range(N - 1):
            arrived(ra[k].at[d], ra_r.at[k, d])
        p1, p2 = pos[(k + 1) % 3], pos[(k + 2) % 3]
        flight[k] = []
        for n, (di, dj) in enumerate(planes + [(0, 0)]):
            i, j = plus(p1, di, N), plus(p2, dj, N)
            if k == 0:
                own, got = part.at[0, x // XL, j, lax.rem(x, XL), i], lambda d: ra0[d, j, i]
            elif k == 1:
                own, got = part.at[1, j // XL, i, lax.rem(j, XL), y], lambda d: ra1[d, j // XL, i, lax.rem(j, XL)]
            else:
                own, got = part.at[2, i // XL, z, lax.rem(i, XL), j], lambda d: ra2[d, i // XL, lax.rem(i, XL), j]
            total = own[...].astype(F32)
            for d in range(N - 1):
                total = total + got(d).astype(F32)
            sa[k, n] = total.astype(BF16)
            if (di, dj) != (0, 0):
                at = list(pos)
                at[(k + 1) % 3], at[(k + 2) % 3] = i, j
                to = device(at[0], at[1], at[2], c)
                flight[k].append(send(sa.at[k, n], rb.at[k, n], rs_s.at[k, n], rs_r.at[k, n], to))

    def add_b(k):
        for copy in flight[k]:
            copy.wait_recv()
        total = sa[k, len(planes)].astype(F32)
        for n in range(len(planes)):
            total = total + rb[k, n].astype(F32)
        gu_ref[:, k * CW:(k + 1) * CW] = total

    for d in reversed(steps):
        arrived(gi.at[0, d], gi_r.at[d])
        gi_hand(d)
    for copy in xi_recv:
        copy.wait_recv()
    for d in range(N):
        arrived(gi.at[1, d], gh_r.at[d])
    for h in range(XH):
        r = dot_t(xi[h].reshape(N * CORES * USERS, FEAT), gi[...].reshape(N * CORES * USERS, E)).astype(BF16)
        parti[h * XL:(h + 1) * XL] = r.reshape(XL, N, 16, E)
    left_half, right_half = pl.ds(0, E // 2), pl.ds(E // 2, E // 2)
    ri_recv = []
    for d in steps:
        t = plus(x, d, N)
        src = parti.at[t, :, :, left_half]
        ri_recv.append(send(src, ri.at[0, d - 1], ri_s.at[0, d - 1], ri_r.at[0, d - 1], towards(0, t)))
        t = plus(y, d, N)
        src = parti.at[:, t, :, right_half]
        ri_recv.append(send(src, ri.at[1, d - 1], ri_s.at[1, d - 1], ri_r.at[1, d - 1], towards(1, t)))
    add_a(1)
    add_a(0)
    add_a(2)
    for copy in ri_recv:
        copy.wait_recv()
    for n in range(N):
        total = parti[x, n, :, 0:E // 2].astype(F32)
        for d in range(N - 1):
            total = total + ri[0, d, n].astype(F32)
        si[0, n] = total.astype(BF16)
        total = parti[n, y, :, E // 2:E].astype(F32)
        for d in range(N - 1):
            total = total + ri[1, d, n].astype(F32)
        si[1, n] = total.astype(BF16)
    ri_recv = []
    for h in range(2):
        for d in steps:
            t = plus(pos[1 - h], d, N)
            ri_recv.append(send(si.at[h, t], rj.at[h, d - 1], rj_s.at[h, d - 1], rj_r.at[h, d - 1], towards(1 - h, t)))
    for copy in loss_copies:
        copy.wait_recv()
    corelosses[c] = reduced_loss(2)
    core_copy = send(corelosses.at[c], corelosses.at[c], hop_s.at[3], hop_r.at[3], sibling)
    for copy in sent:
        copy.wait_send()
    for k in range(COLOURS):
        for u in range(USERS // 8):
            left(g.at[k, pl.ds(u * 8 * HIST, 8 * HIST)], g_s.at[k, u])
        for d in range(N - 1):
            left(ra[k].at[d], ra_s.at[k, d])
    for d in range(N):
        left(gi.at[0, d], gh_s.at[d])
        if d:
            left(gi.at[0, 0], gi_s.at[d])
    add_b(1)
    add_b(0)
    core_copy.wait_recv()
    loss_ref[...] = jnp.broadcast_to(jnp.sum(corelosses[0] + corelosses[1], keepdims=True) / TOTAL, (8, 128))
    for copy in ri_recv:
        copy.wait_recv()
    for h in range(2):
        total = si[h, pos[1 - h]].astype(F32)
        for d in range(N - 1):
            total = total + rj[h, d].astype(F32)
        gi_ref[:, h * (E // 2):(h + 1) * (E // 2)] = total
    add_b(2)


def hand_out(loss, ig, gu, gi, loss_out, ig_out, gu_out, gi_out):
    loss_out[0] = loss[0, 0]
    ig_out[...] = ig[...]
    gu_out[...] = gu[...]
    gi_out[...] = gi[...]


def shards(N, XL, past, cand, wu, wi, scale, shift, ids, slots):
    users, hist, depth = past.shape
    E = wu.shape[1]
    total = users * lax.axis_size("blk") * lax.axis_size("group")
    NU, NI, NS, QN = XL * N, XL * N * CORES, XL * N, (N // XL) * N
    feat = depth // (QN * CORES)
    hbm = pl.BlockSpec(memory_space=pltpu.HBM)
    smem = pl.BlockSpec(memory_space=pltpu.SMEM)
    vmem = pl.BlockSpec(memory_space=pltpu.VMEM)
    rows = depth // (N * N * N * CORES)
    CW = E // COLOURS

    def dma(*shape):
        return pltpu.SemaphoreType.DMA(shape)

    V = pltpu.VMEM
    scratch = [
        V((users * hist, depth), BF16), V((QN, users * hist, feat), BF16),
        V((users, depth), BF16),
        V((depth, E), BF16), V((depth, E), BF16),
        V((users * hist, E), F32), V((users, E), F32), V((users, E), F32), V((users, 128), F32),
        V((users, E), F32), V((users, 128), F32),
        V((NU, users, E), BF16), V((CORES, NS, users, E), BF16), V((NI, 1, 128), F32), V((NI, users, 128), F32),
        V((NU, 1, NU * users), F32), V((NU, 1, NU * users), F32),
        V((NI * users, NU * users), F32), V((NI * users, NU * users), BF16),
        V((CORES, NS, users, E), BF16), V((NS, users, E), F32), V((NS, users, E), BF16),
        V((NS - 1, users, E), BF16),
        V((NU, users, E), BF16), V((NU - 1, users, E), BF16),
        V((COLOURS, 2 * users * hist, CW), BF16), V((CORES, N, users, E), BF16),
        V((N // XL, N * CORES, users, feat), BF16), V((QN * feat, 2 * users * hist), BF16),
        V((COLOURS, N // XL, N, XL, N, rows, CW), BF16), V((N - 1, N, N, rows, CW), BF16),
        V((N - 1, N // XL, N, XL, rows, CW), BF16), V((N - 1, N // XL, XL, N, rows, CW), BF16),
        V((COLOURS, N * N, rows, CW), BF16), V((COLOURS, N * N - 1, rows, CW), BF16),
        V((N, N, rows, E), BF16), V((2, N - 1, N, rows, E // 2), BF16),
        V((2, N, rows, E // 2), BF16), V((2, N - 1, rows, E // 2), BF16),
        V((3, N, 8, 128), F32), V((CORES, 8, 128), F32),
        V((1, 1), F32), V((1, 1), F32), V((1, users), jnp.int32), V((1, users), jnp.int32),
        dma(8), dma(QN), dma(QN), dma(N * CORES - 1, N // XL), dma(N * CORES - 1, N // XL),
        dma(NI - 1), dma(NI - 1), dma(NU - 1), dma(NU - 1), dma(NU - 1), dma(NU - 1),
        dma(NS - 1), dma(NS - 1), dma(NU - 1), dma(NU - 1),
        dma(NS - 1), dma(NS - 1), dma(NU - 1), dma(NU - 1), dma(COLOURS, users // 8), dma(COLOURS, users // 8), dma(N), dma(N), dma(N), dma(N),
        dma(COLOURS, N - 1), dma(COLOURS, N - 1), dma(COLOURS, N * N - 1), dma(COLOURS, N * N - 1),
        dma(2, N - 1), dma(2, N - 1), dma(2, N - 1), dma(2, N - 1), dma(3, N - 1), dma(3, N - 1), dma(4), dma(4),
    ]
    outs = pl.pallas_call(
        functools.partial(tower_kernel, N, XL, total),
        name="two_tower",
        out_shape=(
            pltpu.VMEM((8, 128), F32),
            pltpu.VMEM((users, E), F32),
            pltpu.VMEM((rows, E), F32),
            pltpu.VMEM((rows, E), F32),
        ),
        in_specs=[hbm] * 8,
        out_specs=(vmem,) * 4,
        scratch_shapes=scratch,
        compiler_params=pltpu.CompilerParams(
            collective_id=0, has_side_effects=True, vmem_limit_bytes=60 * 1024 * 1024
        ),
    )(
        past.reshape(users * hist, depth), cand, wu, wi, scale.reshape(1, 1), shift.reshape(1, 1),
        ids.reshape(1, users), slots.reshape(1, users),
    )
    return pl.pallas_call(
        hand_out,
        name="hand_out",
        out_shape=(
            jax.ShapeDtypeStruct((1,), F32),
            jax.ShapeDtypeStruct((users, E), F32),
            jax.ShapeDtypeStruct((rows, E), F32),
            jax.ShapeDtypeStruct((rows, E), F32),
        ),
        in_specs=[vmem] * 4,
        out_specs=(smem, vmem, vmem, vmem),
        compiler_params=pltpu.CompilerParams(vmem_limit_bytes=4 * 1024 * 1024),
    )(*outs)


def solution(mesh):
    group = mesh.shape["group"]
    n = {128: 4, 16: 2}[mesh.size]
    both = ("blk", "group")
    return jax.shard_map(
        functools.partial(shards, n, group // n),
        mesh=mesh,
        in_specs=(P(both, None, None), P(both, None), P(), P(), P(), P(), P(both), P(both)),
        out_specs=(P(), P(both, None), P(both, None), P(both, None)),
        check_vma=False,
    )
```
